32 devices in a mesh: seq: 8 (over y, x, core), head: 4 (over z).
Axes of the slice: x: 2, y: 2, z: 4, core: 2. Of those that a mesh axis runs over, the one named last changes fastest.
Arguments:
- token_ids: int32 [6144], replicated, may hold values from 0 to 31999
- completion: int32 [6144], replicated, may hold values from 0 to 1, as said below
- decay_rate: float32 [1, 4], P(None, 'head'), may hold values from 0 to 0.05
- w_mixer: bfloat16 [1, 1024, 6144], P(None, 'seq', 'head'), may hold values from -0.1875 to 0.1875
- w_output: bfloat16 [1, 2048, 1024], P(None, 'head', 'seq'), may hold values from -0.125 to 0.125
- w_expand: bfloat16 [1, 1024, 4096], P(None, 'seq', 'head'), may hold values from -0.1875 to 0.1875
- w_contract: bfloat16 [1, 2048, 1024], P(None, 'head', 'seq'), may hold values from -0.125 to 0.125
- norm_gains: bfloat16 [3, 1024], P(None, 'seq'), may hold values from 0.5 to 1.5
- embedding: bfloat16 [32000, 1024], P('seq'), may hold values from -0.375 to 0.375
- mom_mixer: float32 [1, 1024, 6144], P(None, 'seq', 'head'), may hold values from -0.0010764359 to 0.0010764359
- var_mixer: float32 [1, 1024, 6144], P(None, 'seq', 'head'), may hold values from 2.5431315e-09 to 1.0172526e-08
- mom_output: float32 [1, 2048, 1024], P(None, 'head', 'seq'), may hold values from -0.0010764359 to 0.0010764359
- var_output: float32 [1, 2048, 1024], P(None, 'head', 'seq'), may hold values from 2.5431315e-09 to 1.0172526e-08
- mom_expand: float32 [1, 1024, 4096], P(None, 'seq', 'head'), may hold values from -0.0010764359 to 0.0010764359
- var_expand: float32 [1, 1024, 4096], P(None, 'seq', 'head'), may hold values from 2.5431315e-09 to 1.0172526e-08
- mom_contract: float32 [1, 2048, 1024], P(None, 'head', 'seq'), may hold values from -0.0010764359 to 0.0010764359
- var_contract: float32 [1, 2048, 1024], P(None, 'head', 'seq'), may hold values from 2.5431315e-09 to 1.0172526e-08
- mom_gains: float32 [3, 1024], P(None, 'seq'), may hold values from -0.0010764359 to 0.0010764359
- var_gains: float32 [3, 1024], P(None, 'seq'), may hold values from 2.5431315e-09 to 1.0172526e-08
- mom_embed: float32 [32000, 1024], P('seq', 'head'), may hold values from -0.0010764359 to 0.0010764359
- var_embed: float32 [32000, 1024], P('seq', 'head'), may hold values from 2.5431315e-09 to 1.0172526e-08
Outputs:
- mean_loss: float32 [], replicated
- trust_square_sums: float32 [8, 2], replicated
- new_mom_mixer: float32 [1, 1024, 6144], P(None, 'seq', 'head')
- new_var_mixer: float32 [1, 1024, 6144], P(None, 'seq', 'head')
- new_w_mixer: float32 [1, 1024, 6144], P(None, 'seq', 'head')
- new_mom_output: float32 [1, 2048, 1024], P(None, 'head', 'seq')
- new_var_output: float32 [1, 2048, 1024], P(None, 'head', 'seq')
- new_w_output: float32 [1, 2048, 1024], P(None, 'head', 'seq')
- new_mom_expand: float32 [1, 1024, 4096], P(None, 'seq', 'head')
- new_var_expand: float32 [1, 1024, 4096], P(None, 'seq', 'head')
- new_w_expand: float32 [1, 1024, 4096], P(None, 'seq', 'head')
- new_mom_contract: float32 [1, 2048, 1024], P(None, 'head', 'seq')
- new_var_contract: float32 [1, 2048, 1024], P(None, 'head', 'seq')
- new_w_contract: float32 [1, 2048, 1024], P(None, 'head', 'seq')
- new_mom_gains: float32 [3, 1024], P(None, 'seq')
- new_var_gains: float32 [3, 1024], P(None, 'seq')
- new_w_gains: float32 [3, 1024], P(None, 'seq')
- new_mom_embed: float32 [32000, 1024], P('seq', 'head')
- new_var_embed: float32 [32000, 1024], P('seq', 'head')
- new_w_embed: float32 [32000, 1024], P('seq', 'head')
The draws below stay inside these ranges and needn't reach their ends.
Inputs may be any that keep to these rules, and one draw needn't show every extreme that they name: `completion`: each span of 768 tokens (one index of seq) holds at most 384 ones, and one span holds exactly 384.
All inputs are finite; a program needn't handle non-finite values.
Results may differ from the reference program's by a relative error of at most 0.018.
Values may be sent and summed in bfloat16 or wider, within the bound.
A program may use at most 192 MiB of HBM per device.

```python
import math
import jax
import jax.numpy as jnp
import numpy as np
from jax import lax

D = 1024
HEADS = 4
KD = 256
VD = 512
FF = 2048
V = 32000
LAYERS = 1
STEP = 10
TOK_DEV = 768
TOKENS = 6144


def head_order(sub_key):
    return jax.random.permutation(sub_key, HEADS)


def draw_decay_rate(key, part):
    key_perm, key_slow, key_fast = jax.random.split(key, 3)
    orders = jax.vmap(head_order)(jax.random.split(key_perm, LAYERS))
    slow_count = 2
    slow_rate = jnp.exp(jax.random.uniform(key_slow, (LAYERS, HEADS), jnp.float32, jnp.log(0.3), jnp.log(2.0))) / TOKENS
    fast_rate = jnp.exp(jax.random.uniform(key_fast, (LAYERS, HEADS), jnp.float32, jnp.log(1.0 / 50.0), jnp.log(1.0 / 30.0)))
    return jnp.where(orders < slow_count, slow_rate, fast_rate).astype(jnp.float32)


def draw_completion(key, part):
    spans_n = TOKENS // TOK_DEV
    capacity = TOK_DEV // 2
    key_count, key_full, key_score = jax.random.split(key, 3)
    counts = jax.random.randint(key_count, (spans_n,), 0, capacity + 1)
    forced = jax.random.randint(key_full, (), 0, spans_n)
    counts = jnp.where(jnp.arange(spans_n) == forced, capacity, counts)
    scores = jax.random.randint(key_score, (spans_n, TOK_DEV), 0, 524288) * TOK_DEV + jnp.arange(TOK_DEV)[None, :]
    ranks = jnp.argsort(jnp.argsort(scores, axis=1, stable=True), axis=1, stable=True)
    return (ranks < counts[:, None]).astype(jnp.int32).reshape(TOKENS)


def draw_embedding(key, part):
    key_entry, key_shard = jax.random.split(jax.random.fold_in(key, 71), 2)
    shard_count = TOKENS // TOK_DEV
    shard_rows = V // shard_count
    shard_no = jnp.arange(V) // shard_rows
    rough = jnp.exp(jax.random.uniform(key_shard, (shard_count,), jnp.float32, jnp.log(0.8), jnp.log(1.25)))
    picked = jnp.sum(jnp.where(shard_no[:, None] == jnp.arange(shard_count)[None, :], rough[None, :], 0.0), axis=1)
    rise = jnp.exp(jnp.log(3.0) * shard_no.astype(jnp.float32) / max(shard_count - 1, 1))
    row_scale = 0.8 * D ** (-0.5) * rise * picked
    entries = jnp.clip(jax.random.normal(key_entry, (V, D), jnp.float32), -4.0, 4.0)
    return (entries * row_scale[:, None]).astype(jnp.bfloat16)


def set_ends(values, key, low, high):
    spot = [jax.random.randint(jax.random.fold_in(key, axis), (), 0, length) for axis, length in enumerate(values.shape)]
    widest = values.shape.index(max(values.shape))
    neighbour = spot[:widest] + [(spot[widest] + 1) % values.shape[widest]] + spot[widest + 1:]
    return values.at[tuple(spot)].set(low).at[tuple(neighbour)].set(high)


def block_levels(stream_key, shape, cuts, least, top_value):
    def one(axis_at, blocks):
        steps = jax.random.uniform(jax.random.fold_in(jax.random.fold_in(stream_key, 6), axis_at), (blocks,), jnp.float32, least / len(cuts), top_value / len(cuts))
        return jnp.repeat(jnp.exp(steps), shape[axis_at] // blocks).reshape((-1,) + (1,) * (len(shape) - axis_at - 1))

    factor_of = one(*cuts[0])
    for cut in cuts[1:]:
        factor_of = factor_of * one(*cut)
    return factor_of


def rank_table(count, lean):
    weights = [(1 << 20) // math.isqrt(grade ** lean) + 1 for grade in range(1, count + 1)]
    spread = 1 + sum(weights) // (1 << 30)
    return np.cumsum(np.array([max(1, weight // spread) for weight in weights]))


def ranked_ids(stream_key, dims, count, skew):
    table = rank_table(count, skew)
    pick = jax.random.randint(jax.random.fold_in(stream_key, 1), dims, 0, int(table[count - 1]))
    grade = jnp.searchsorted(jnp.asarray(table, jnp.int32), pick, side="right")
    return jax.random.permutation(jax.random.fold_in(stream_key, 2), count)[grade].astype(jnp.int32)


def bell_draw(own_key, extent, deviation, limit, cuts=(), held_as=jnp.bfloat16):
    drawn = jax.random.normal(own_key, extent, jnp.float32) * deviation
    if len(cuts) > 0:
        drawn = block_levels(own_key, extent, cuts, -0.22, 0.18) * drawn
    return jnp.clip(drawn, min=-limit, max=limit).astype(held_as)


def setup_inputs(seed: int = 0) -> dict:
    keys = jax.random.split(jax.random.key(seed), 22)
    token_ids = set_ends(ranked_ids(keys[0], (TOKENS,), V, 2), jax.random.fold_in(keys[0], 3), 0, V - 1).astype(jnp.int32)
    completion = draw_completion(jax.random.fold_in(keys[21], 71), 0)
    decay_rate = draw_decay_rate(jax.random.fold_in(keys[21], 71), 0)
    w_mixer = bell_draw(keys[3], (LAYERS, D, HEADS * (2 * KD + 2 * VD)), D ** -0.5, 0.1875, ((1, 8), (2, 4)))
    w_output = bell_draw(keys[4], (LAYERS, HEADS * VD, D), (HEADS * VD) ** -0.5, 0.125, ((1, 4), (2, 8)))
    w_expand = bell_draw(keys[5], (LAYERS, D, 2 * FF), D ** -0.5, 0.1875, ((1, 8), (2, 4)))
    w_contract = bell_draw(keys[6], (LAYERS, FF, D), FF ** -0.5, 0.125, ((1, 4), (2, 8)))
    norm_gains = jnp.clip(1.0 + 0.1 * jax.random.normal(keys[7], (2 * LAYERS + 1, D), jnp.float32), 0.5, 1.5).astype(jnp.bfloat16)
    embedding = draw_embedding(jax.random.fold_in(keys[21], 71), 0)
    mom_mixer = bell_draw(keys[9], (LAYERS, D, HEADS * (2 * KD + 2 * VD)), (0.44 / (D * TOKENS) ** 0.5), 0.0010764359, ((1, 8), (2, 4)), jnp.float32)
    var_mixer = jnp.clip(jnp.exp(math.log(1.017252593271678e-08) - 1.3862944 * jax.random.uniform(keys[10], (LAYERS, D, HEADS * (2 * KD + 2 * VD)), jnp.float32) ** block_levels(keys[10], (LAYERS, D, HEADS * (2 * KD + 2 * VD)), ((1, 8), (2, 4)), -0.2, 0.2)), 2.543131483179195e-09, 1.017252593271678e-08)
    mom_output = bell_draw(keys[11], (LAYERS, HEADS * VD, D), (0.44 / (D * TOKENS) ** 0.5), 0.0010764359, ((1, 4), (2, 8)), jnp.float32)
    var_output = jnp.clip(jnp.exp(math.log(1.017252593271678e-08) - 1.3862944 * jax.random.uniform(keys[12], (LAYERS, HEADS * VD, D), jnp.float32) ** block_levels(keys[12], (LAYERS, HEADS * VD, D), ((1, 4), (2, 8)), -0.2, 0.2)), 2.543131483179195e-09, 1.017252593271678e-08)
    mom_expand = bell_draw(keys[13], (LAYERS, D, 2 * FF), (0.44 / (D * TOKENS) ** 0.5), 0.0010764359, ((1, 8), (2, 4)), jnp.float32)
    var_expand = jnp.clip(jnp.exp(math.log(1.017252593271678e-08) - 1.3862944 * jax.random.uniform(keys[14], (LAYERS, D, 2 * FF), jnp.float32) ** block_levels(keys[14], (LAYERS, D, 2 * FF), ((1, 8), (2, 4)), -0.2, 0.2)), 2.543131483179195e-09, 1.017252593271678e-08)
    mom_contract = bell_draw(keys[15], (LAYERS, FF, D), (0.44 / (D * TOKENS) ** 0.5), 0.0010764359, ((1, 4), (2, 8)), jnp.float32)
    var_contract = jnp.clip(jnp.exp(math.log(1.017252593271678e-08) - 1.3862944 * jax.random.uniform(keys[16], (LAYERS, FF, D), jnp.float32) ** block_levels(keys[16], (LAYERS, FF, D), ((1, 4), (2, 8)), -0.2, 0.2)), 2.543131483179195e-09, 1.017252593271678e-08)
    mom_gains = bell_draw(keys[17], (2 * LAYERS + 1, D), (0.44 / (D * TOKENS) ** 0.5), 0.0010764359, ((1, 8),), jnp.float32)
    var_gains = jnp.clip(jnp.exp(math.log(1.017252593271678e-08) - 1.3862944 * jax.random.uniform(keys[18], (2 * LAYERS + 1, D), jnp.float32) ** block_levels(keys[18], (2 * LAYERS + 1, D), ((1, 8),), -0.2, 0.2)), 2.543131483179195e-09, 1.017252593271678e-08)
    mom_embed = bell_draw(keys[19], (V, D), (0.44 / (D * TOKENS) ** 0.5), 0.0010764359, ((0, 8), (1, 4)), jnp.float32)
    var_embed = jnp.clip(jnp.exp(math.log(1.017252593271678e-08) - 1.3862944 * jax.random.uniform(keys[20], (V, D), jnp.float32) ** block_levels(keys[20], (V, D), ((0, 8), (1, 4)), -0.2, 0.2)), 2.543131483179195e-09, 1.017252593271678e-08)
    return dict(token_ids=token_ids, completion=completion, decay_rate=decay_rate, w_mixer=w_mixer, w_output=w_output, w_expand=w_expand, w_contract=w_contract, norm_gains=norm_gains, embedding=embedding, mom_mixer=mom_mixer, var_mixer=var_mixer, mom_output=mom_output, var_output=var_output, mom_expand=mom_expand, var_expand=var_expand, mom_contract=mom_contract, var_contract=var_contract, mom_gains=mom_gains, var_gains=var_gains, mom_embed=mom_embed, var_embed=var_embed)


EXACT_MATMUL = lax.Precision.HIGHEST
NORM_EPS = 1e-05
BETA_ONE = 0.9
BETA_TWO = 0.999
ADAM_EPS = 1e-08
DECAY_WT = 0.01
LEARN_RATE = 0.2
TRUST_EPSILON = 1e-06

@jax.custom_vjp
def low(v):
    return lax.optimization_barrier(v.astype(jnp.bfloat16)).astype(jnp.float32)

@jax.custom_vjp
def low_back(v):
    return v

def low_keep(v):
    return (low(v), None)

def low_pass(kept, grad):
    return (grad,)

def back_keep(v):
    return (v, None)

def back_low(kept, grad):
    return (low(grad),)
low.defvjp(low_keep, low_pass)
low_back.defvjp(back_keep, back_low)

def layer_norm(values, gain_row):
    centred = values - lax.optimization_barrier(jnp.mean(values, axis=-1, keepdims=True))
    spread_sq = lax.optimization_barrier(jnp.mean(centred * centred, axis=-1, keepdims=True))
    return centred * lax.rsqrt(spread_sq + NORM_EPS) * gain_row

def rotary_tables(positions, width_in):
    halfway = width_in // 2
    frequency = jnp.exp(-jnp.log(10000.0) * jnp.arange(halfway).astype(jnp.float32) / halfway)
    phases = positions.astype(jnp.float32)[:, None] * frequency[None, :]
    return (jnp.cos(phases), jnp.sin(phases))

def rotate(values, cosines, sines):
    halfway = values.shape[-1] // 2
    leading = values[..., :halfway]
    trailing = values[..., halfway:]
    return jnp.concatenate([leading * cosines - trailing * sines, leading * sines + trailing * cosines], axis=-1)

def gate_norm(gate_pre, retained):
    scaled = retained * lax.rsqrt(lax.optimization_barrier(jnp.mean(retained * retained, axis=-1, keepdims=True)) + NORM_EPS)
    return gate_pre * jax.nn.sigmoid(gate_pre) * scaled

def gelu_gate(gate_part, up_part):
    return jax.nn.gelu(gate_part) * up_part

def retention(query_all, keys_all, values_all, rates):
    span_len = TOK_DEV
    blocks = query_all.shape[0] // span_len
    head_count = rates.shape[0]
    steps_in = jnp.arange(span_len).astype(jnp.float32)
    offsets = steps_in[:, None] - steps_in[None, :]
    within = jnp.where(offsets[None] >= 0, jnp.exp(-rates[:, None, None] * jnp.maximum(offsets, 0.0)[None]), 0.0)
    tail_decay = jnp.exp(-rates[None, :] * (span_len - 1.0 - steps_in)[:, None])
    lead_decay = jnp.exp(-rates[None, :] * (steps_in + 1.0)[:, None])
    block_decay = jnp.exp(-rates * span_len)

    def block_step(carried_state, inputs):
        query_tile, keys_blk, value_tile = inputs
        scores = low_back(jnp.einsum('shk,thk->hst', query_tile, keys_blk, precision=EXACT_MATMUL))
        weights_blk = low(scores * within)
        inner_part = low_back(jnp.einsum('hst,thv->shv', weights_blk, value_tile, precision=EXACT_MATMUL))
        cross_part = low_back(jnp.einsum('fdr,drz->fdz', query_tile, low(carried_state), precision=EXACT_MATMUL))
        mixed_out = inner_part + lead_decay[:, :, None] * cross_part
        weighted_values = low(keys_blk * tail_decay[:, :, None])
        weight_update = low_back(jnp.einsum('dqr,dqs->qrs', weighted_values, value_tile, precision=EXACT_MATMUL))
        return (block_decay[:, None, None] * carried_state + weight_update, mixed_out)
    zero_state = jnp.zeros((head_count, KD, VD), jnp.float32)
    shaped = (query_all.reshape(blocks, span_len, head_count, KD), keys_all.reshape(blocks, span_len, head_count, KD), values_all.reshape(blocks, span_len, head_count, VD))
    _, mixed_out = lax.scan(jax.checkpoint(block_step), zero_state, shaped)
    return mixed_out.reshape(blocks * span_len, head_count, VD)

def layer_forward(residual, mixer, output, expand, contract, gain_a, gain_b, rates, cosines, sines):
    tokens_in = residual.shape[0]
    head_count = rates.shape[0]
    normed = low(layer_norm(residual, gain_a))
    proj = jnp.dot(normed, mixer, precision=EXACT_MATMUL, preferred_element_type=jnp.float32)
    proj = proj.reshape(tokens_in, head_count, 2 * KD + 2 * VD)
    q_pre = low_back(proj[:, :, :KD])
    k_pre = low_back(proj[:, :, KD:2 * KD])
    v_pre = low_back(proj[:, :, 2 * KD:2 * KD + VD])
    gate_pre = low_back(proj[:, :, 2 * KD + VD:])
    query_all = low(rotate(q_pre, cosines[:, None, :], sines[:, None, :]))
    keys_all = low(rotate(k_pre, cosines[:, None, :], sines[:, None, :]) * KD ** (-0.5))
    values_all = low(v_pre)
    retained = retention(query_all, keys_all, values_all, rates)
    gated_out = low(gate_norm(gate_pre, retained)).reshape(tokens_in, head_count * VD)
    residual_mid = residual + low_back(jnp.dot(gated_out, output, precision=EXACT_MATMUL, preferred_element_type=jnp.float32))
    normed_b = low(layer_norm(residual_mid, gain_b))
    gate_up = jnp.dot(normed_b, expand, precision=EXACT_MATMUL, preferred_element_type=jnp.float32)
    gate_up = gate_up.reshape(tokens_in, head_count, 2, FF // head_count)
    hidden = low(gelu_gate(low_back(gate_up[:, :, 0]), low_back(gate_up[:, :, 1]))).reshape(tokens_in, FF)
    return residual_mid + low_back(jnp.dot(hidden, contract, precision=EXACT_MATMUL, preferred_element_type=jnp.float32))

def take_rows(frame_rows, places):
    return jnp.take(frame_rows, places, axis=0)

def forward_loss(mixer, output, expand, contract, gains, table, token_ids, completion, rates):
    residual = jnp.take(table, token_ids, axis=0)
    cosines, sines = rotary_tables(jnp.arange(TOKENS), KD)
    for layer_no in range(LAYERS):
        residual = jax.checkpoint(layer_forward)(residual, mixer[layer_no], output[layer_no], expand[layer_no], contract[layer_no], gains[2 * layer_no], gains[2 * layer_no + 1], rates[layer_no], cosines, sines)
    final_norm = low(layer_norm(residual, gains[2 * LAYERS]))
    spans_n = TOKENS // TOK_DEV
    capacity = TOK_DEV // 2
    mask_grid = completion.reshape(spans_n, TOK_DEV)
    slot_grid = jnp.where(mask_grid == 1, jnp.cumsum(mask_grid, axis=1) - 1, -1)
    matches = slot_grid[:, None, :] == jnp.arange(capacity)[None, :, None]
    places = lax.optimization_barrier(jnp.sum(jnp.where(matches, jnp.arange(TOK_DEV)[None, None, :], 0), axis=-1)).astype(jnp.int32)
    present = jnp.any(matches, axis=-1)
    next_ids = jnp.roll(token_ids, -1).reshape(spans_n, TOK_DEV)
    live = (completion * (jnp.arange(TOKENS) < TOKENS - 1)).reshape(spans_n, TOK_DEV)
    targets = lax.optimization_barrier(jnp.sum(jnp.where(matches, next_ids[:, None, :], 0), axis=-1)).astype(jnp.int32)
    row_weight = lax.optimization_barrier(jnp.sum(jnp.where(matches, live[:, None, :], 0), axis=-1)).astype(jnp.float32)
    count_live = jnp.sum(live).astype(jnp.float32)
    final_grid = final_norm.reshape(spans_n, TOK_DEV, D)
    chosen = jax.vmap(take_rows)(final_grid, places) * present[:, :, None].astype(jnp.float32)

    def span_loss(pieces):
        row_block, goal_ids, weight_row = pieces
        logits = low_back(jnp.dot(row_block, table.T, precision=EXACT_MATMUL, preferred_element_type=jnp.float32))
        peak = lax.optimization_barrier(jnp.max(logits, axis=-1, keepdims=True))
        log_total = peak[:, 0] + jnp.log(lax.optimization_barrier(jnp.sum(jnp.exp(logits - peak), axis=-1)))
        target_logit = jnp.take_along_axis(logits, goal_ids[:, None].astype(jnp.int32), axis=1)[:, 0]
        return jnp.sum(weight_row * (log_total - target_logit))
    per_span = lax.map(jax.checkpoint(span_loss), (chosen, targets, row_weight))
    return jnp.sum(per_span) / count_live

def lamb_parts(weight, moment, second, grad):
    new_moment = BETA_ONE * moment + (1.0 - BETA_ONE) * grad
    new_second = BETA_TWO * second + (1.0 - BETA_TWO) * grad * grad
    moment_hat = new_moment / (1.0 - BETA_ONE ** STEP)
    second_hat = new_second / (1.0 - BETA_TWO ** STEP)
    ratio = moment_hat / (jnp.sqrt(second_hat) + ADAM_EPS) + DECAY_WT * weight
    return (new_moment, new_second, ratio)

def reference(token_ids, completion, decay_rate, w_mixer, w_output, w_expand, w_contract, norm_gains, embedding, mom_mixer, var_mixer, mom_output, var_output, mom_expand, var_expand, mom_contract, var_contract, mom_gains, var_gains, mom_embed, var_embed):
    mixer = w_mixer.astype(jnp.float32)
    output = w_output.astype(jnp.float32)
    expand = w_expand.astype(jnp.float32)
    contract = w_contract.astype(jnp.float32)
    gains = norm_gains.astype(jnp.float32)
    table = embedding.astype(jnp.float32)

    def objective(mixer_in, output_in, expand_in, contract_in, gains_in, table_in):
        return forward_loss(mixer_in, output_in, expand_in, contract_in, gains_in, table_in, token_ids, completion, decay_rate)
    scalar_loss, pullback = jax.vjp(objective, mixer, output, expand, contract, gains, table)
    grad_mixer, grad_output, grad_expand, grad_contract, grad_gains, grad_table = pullback(jnp.ones_like(scalar_loss))
    part_mixer = lamb_parts(mixer, mom_mixer, var_mixer, grad_mixer)
    part_output = lamb_parts(output, mom_output, var_output, grad_output)
    part_expand = lamb_parts(expand, mom_expand, var_expand, grad_expand)
    part_contract = lamb_parts(contract, mom_contract, var_contract, grad_contract)
    shard_gains = lamb_parts(gains, mom_gains, var_gains, grad_gains)
    shard_table = lamb_parts(table, mom_embed, var_embed, grad_table)
    layered_w = (mixer, output, expand, contract)
    layered_ratio_rows = (part_mixer[2], part_output[2], part_expand[2], part_contract[2])
    wsq_layers = jnp.stack([lax.optimization_barrier(jnp.sum(group_entry * group_entry, axis=(1, 2))) for group_entry in layered_w], axis=1).reshape(-1)
    layer_ratio_squares = jnp.stack([lax.optimization_barrier(jnp.sum(group_entry * group_entry, axis=(1, 2))) for group_entry in layered_ratio_rows], axis=1).reshape(-1)
    weight_squares = jnp.concatenate([wsq_layers, jnp.sum(table * table)[None], lax.optimization_barrier(jnp.sum(gains * gains, axis=1))])
    ratio_squares = jnp.concatenate([layer_ratio_squares, jnp.sum(shard_table[2] * shard_table[2])[None], lax.optimization_barrier(jnp.sum(shard_gains[2] * shard_gains[2], axis=1))])
    trust_ratio = jnp.sqrt(weight_squares) * lax.rsqrt(ratio_squares + TRUST_EPSILON)
    trust_layers = trust_ratio[:4 * LAYERS].reshape(LAYERS, 4)
    new_w_mixer = mixer - LEARN_RATE * trust_layers[:, 0][:, None, None] * part_mixer[2]
    new_w_output = output - LEARN_RATE * trust_layers[:, 1][:, None, None] * part_output[2]
    new_w_expand = expand - LEARN_RATE * trust_layers[:, 2][:, None, None] * part_expand[2]
    new_w_contract = contract - LEARN_RATE * trust_layers[:, 3][:, None, None] * part_contract[2]
    new_w_embed = table - LEARN_RATE * trust_ratio[4 * LAYERS] * shard_table[2]
    new_w_gains = gains - LEARN_RATE * trust_ratio[4 * LAYERS + 1:][:, None] * shard_gains[2]
    trust_square_sums = jnp.stack([weight_squares, ratio_squares], axis=1)
    return (scalar_loss, trust_square_sums, part_mixer[0], part_mixer[1], new_w_mixer, part_output[0], part_output[1], new_w_output, part_expand[0], part_expand[1], new_w_expand, part_contract[0], part_contract[1], new_w_contract, shard_gains[0], shard_gains[1], new_w_gains, shard_table[0], shard_table[1], new_w_embed)
```

```python
import functools
import jax
import jax.numpy as jnp
from jax import lax
from jax.experimental import pallas as pl
from jax.experimental.pallas import tpu as pltpu
from jax.sharding import PartitionSpec as P

MESH = pl.DeviceIdType.MESH
ANY = pl.BlockSpec(memory_space=pl.ANY)
WHOLE = pl.BlockSpec(memory_space=pltpu.VMEM)


def greet(targets):
    barrier = pltpu.get_barrier_semaphore()
    for target in targets:
        pl.semaphore_signal(barrier, inc=1, device_id=target, device_id_type=MESH)
    pl.semaphore_wait(barrier, len(targets))


def push(src, dst, sends, recvs, at, target):
    copy = pltpu.make_async_remote_copy(
        src_ref=src,
        dst_ref=dst,
        send_sem=sends.at[at],
        recv_sem=recvs.at[at],
        device_id=target,
        device_id_type=MESH,
    )
    copy.start()
    return copy


def call(body, outs, in_specs, out_specs, scratch, cid, args, sent=0, name=None):
    return pl.pallas_call(
        body,
        out_shape=outs,
        in_specs=in_specs,
        out_specs=out_specs,
        scratch_shapes=scratch,
        compiler_params=pltpu.CompilerParams(
            collective_id=cid, has_side_effects=True, vmem_limit_bytes=48 * 2**20
        ),
        cost_estimate=pl.CostEstimate(flops=0, bytes_accessed=sent * 40 + 2**20, transcendentals=0),
        name=name,
    )(*args)


def z_ag(x, H, cid):
    def body(x_ref, o_ref, sends, recvs, own):
        h = lax.axis_index("head")
        peers = [{"head": lax.rem(h + k, H)} for k in range(1, H)]
        mine = pltpu.make_async_copy(x_ref, o_ref.at[h], own)
        mine.start()
        greet(peers)
        copies = [push(x_ref, o_ref.at[h], sends, recvs, k, peers[k]) for k in range(H - 1)]
        for copy in copies:
            copy.wait()
        mine.wait()

    return call(
        body,
        jax.ShapeDtypeStruct((H,) + x.shape, x.dtype),
        [ANY],
        ANY,
        [pltpu.SemaphoreType.DMA((H - 1,)), pltpu.SemaphoreType.DMA((H - 1,)), pltpu.SemaphoreType.DMA],
        cid,
        (x,),
        sent=x.size * 2 * (H - 1),
        name="z_ag",
    )


def z_rs(x, H, cid):
    R, C = x.shape[1:]

    def body(x_ref, o_ref, held, sends, recvs, own):
        h = lax.axis_index("head")
        peers = [{"head": lax.rem(h + k, H)} for k in range(1, H)]
        mine = pltpu.make_async_copy(x_ref.at[h], held.at[0], own)
        mine.start()
        greet(peers)
        copies = [
            push(x_ref.at[lax.rem(h + k, H)], held.at[k], sends, recvs, k - 1, peers[k - 1])
            for k in range(1, H)
        ]
        mine.wait()
        for copy in copies:
            copy.wait()
        step = min(R, 32)

        def rows(i, carry):
            at = pl.ds(pl.multiple_of(i * step, step), step)
            total = held[0, at, :].astype(jnp.float32)
            for k in range(1, H):
                total = total + held[k, at, :].astype(jnp.float32)
            o_ref[at, :] = total
            return carry

        lax.fori_loop(0, R // step, rows, 0)

    return call(
        body,
        jax.ShapeDtypeStruct((R, C), jnp.float32),
        [ANY],
        WHOLE,
        [
            pltpu.VMEM((H, R, C), x.dtype),
            pltpu.SemaphoreType.DMA((H - 1,)),
            pltpu.SemaphoreType.DMA((H - 1,)),
            pltpu.SemaphoreType.DMA,
        ],
        cid,
        (x,),
        sent=R * C * 2 * (H - 1),
        name="z_rs",
    )


def p_ag(x, S, cid):
    N = S // 2

    def body(x_ref, o_ref, sends, recvs, fsends, frecvs, own):
        s = lax.axis_index("seq")
        sib = {"seq": s + 1 - 2 * lax.rem(s, 2)}
        peers = [{"seq": lax.rem(s + 2 * k, S)} for k in range(1, N)]
        mine = pltpu.make_async_copy(x_ref, o_ref.at[s], own)
        mine.start()
        greet(peers + [sib])
        copies = [push(x_ref, o_ref.at[s], sends, recvs, k, peers[k]) for k in range(N - 1)]
        copies.append(push(x_ref, o_ref.at[s], sends, recvs, N - 1, sib))
        passed = []
        for k in range(1, N):
            copies[k - 1].wait_recv()
            source = lax.rem(s - 2 * k + 2 * S, S)
            passed.append(push(o_ref.at[source], o_ref.at[source], fsends, frecvs, k - 1, sib))
        copies[N - 1].wait_recv()
        for copy in copies:
            copy.wait_send()
        for copy in passed:
            copy.wait()
        mine.wait()

    return call(
        body,
        jax.ShapeDtypeStruct((S,) + x.shape, x.dtype),
        [ANY],
        ANY,
        [
            pltpu.SemaphoreType.DMA((N,)),
            pltpu.SemaphoreType.DMA((N,)),
            pltpu.SemaphoreType.DMA((N - 1,)),
            pltpu.SemaphoreType.DMA((N - 1,)),
            pltpu.SemaphoreType.DMA,
        ],
        cid,
        (x,),
        sent=x.size * 2 * N,
        name="p_ag",
    )


def p_rs(x, S, cid):
    N = S // 2
    R, C = x.shape[1:]
    step = min(R, 32)

    def body(x_ref, o_ref, sib_held, own_held, out_held, held, sends, recvs, csends, crecvs, own):
        s = lax.axis_index("seq")
        parity = lax.rem(s, 2)
        sib = {"seq": s + 1 - 2 * parity}
        peers = [{"seq": lax.rem(s + 2 * k, S)} for k in range(1, N)]
        mine = []
        for k in range(N):
            owner = lax.rem(s + 2 * k, S)
            mine.append(pltpu.make_async_copy(x_ref.at[owner], own_held.at[k], own.at[k]))
            mine[-1].start()
        greet(peers + [sib])
        order = list(range(1, N)) + [0]
        swaps = {}
        for k in order:
            owner = lax.rem(s + 2 * k, S) + 1 - 2 * parity
            swaps[k] = push(x_ref.at[owner], sib_held.at[k], csends, crecvs, k, sib)
        copies = []
        for k in order:
            mine[k].wait()
            swaps[k].wait_recv()

            def rows(i, carry, k=k):
                at = pl.ds(pl.multiple_of(i * step, step), step)
                total = own_held[k, at, :].astype(jnp.float32) + sib_held[k, at, :].astype(jnp.float32)
                if k == 0:
                    o_ref[at, :] = total
                else:
                    out_held[k - 1, at, :] = total.astype(x.dtype)
                return carry

            lax.fori_loop(0, R // step, rows, 0)
            if k > 0:
                copies.append(push(out_held.at[k - 1], held.at[k - 1], sends, recvs, k - 1, peers[k - 1]))
        for copy in copies:
            copy.wait()
        for k in order:
            swaps[k].wait_send()

        def total_rows(i, carry):
            at = pl.ds(pl.multiple_of(i * step, step), step)
            total = o_ref[at, :]
            for k in range(N - 1):
                total = total + held[k, at, :].astype(jnp.float32)
            o_ref[at, :] = total
            return carry

        lax.fori_loop(0, R // step, total_rows, 0)

    return call(
        body,
        jax.ShapeDtypeStruct((R, C), jnp.float32),
        [ANY],
        WHOLE,
        [
            pltpu.VMEM((N, R, C), x.dtype),
            pltpu.VMEM((N, R, C), x.dtype),
            pltpu.VMEM((N - 1, R, C), x.dtype),
            pltpu.VMEM((N - 1, R, C), x.dtype),
            pltpu.SemaphoreType.DMA((N - 1,)),
            pltpu.SemaphoreType.DMA((N - 1,)),
            pltpu.SemaphoreType.DMA((N,)),
            pltpu.SemaphoreType.DMA((N,)),
            pltpu.SemaphoreType.DMA((N,)),
        ],
        cid,
        (x,),
        sent=R * C * 2 * N,
        name="p_rs",
    )


def all_sum(x, S, H, cid):
    def body(x_ref, o_ref, first, middle, second, sends, recvs, zsends, zrecvs):
        s, h = lax.axis_index("seq"), lax.axis_index("head")
        peers = [{"seq": lax.rem(s + k, S)} for k in range(1, S)]
        heads = [{"head": lax.rem(h + k, H)} for k in range(1, H)]
        greet(peers + heads)
        copies = [push(x_ref, first.at[s], sends, recvs, k, peers[k]) for k in range(S - 1)]
        first[s] = x_ref[...]
        for copy in copies:
            copy.wait()
        total = first[0]
        for k in range(1, S):
            total = total + first[k]
        middle[...] = total
        copies = [push(middle, second.at[h], zsends, zrecvs, k, heads[k]) for k in range(H - 1)]
        second[h] = total
        for copy in copies:
            copy.wait()
        total = second[0]
        for k in range(1, H):
            total = total + second[k]
        o_ref[...] = total

    return call(
        body,
        jax.ShapeDtypeStruct(x.shape, x.dtype),
        [WHOLE],
        WHOLE,
        [
            pltpu.VMEM((S,) + x.shape, x.dtype),
            pltpu.VMEM(x.shape, x.dtype),
            pltpu.VMEM((H,) + x.shape, x.dtype),
            pltpu.SemaphoreType.DMA((S - 1,)),
            pltpu.SemaphoreType.DMA((S - 1,)),
            pltpu.SemaphoreType.DMA((H - 1,)),
            pltpu.SemaphoreType.DMA((H - 1,)),
        ],
        cid,
        (x,),
        sent=x.size * 4 * (S + H),
        name="all_sum",
    )


KD = 256
VD = 512
STEP = 10

NORM_EPS = 1e-05
BETA_ONE = 0.9
BETA_TWO = 0.999
ADAM_EPS = 1e-08
DECAY_WT = 0.01
LEARN_RATE = 0.2
TRUST_EPSILON = 1e-06


def contract_dims(left_side, right_side, left_dim, right_dim):
    return lax.dot_general(
        left_side,
        right_side,
        (((left_dim,), (right_dim,)), ((), ())),
        preferred_element_type=jnp.float32,
    )


def matmul(left_side, right_side):
    return jnp.dot(left_side, right_side, preferred_element_type=jnp.float32)


def centre(values):
    centred = values - jnp.mean(values, axis=-1, keepdims=True)
    return centred * lax.rsqrt(jnp.mean(centred * centred, axis=-1, keepdims=True) + NORM_EPS)


def row_scale(values):
    centred = values - jnp.mean(values, axis=-1, keepdims=True)
    return lax.rsqrt(jnp.mean(centred * centred, axis=-1, keepdims=True) + NORM_EPS)


def norm_back(values, gain_row, grad):
    hat, scale = centre(values), row_scale(values)
    scaled = grad * gain_row
    mean_one = jnp.mean(scaled, axis=-1, keepdims=True)
    mean_two = jnp.mean(scaled * hat, axis=-1, keepdims=True)
    return scale * (scaled - mean_one - hat * mean_two), jnp.sum(grad * hat, axis=0)


def rotary_tables(positions):
    halfway = KD // 2
    frequency = jnp.exp(-jnp.log(10000.0) * jnp.arange(halfway).astype(jnp.float32) / halfway)
    phases = positions.astype(jnp.float32)[:, None] * frequency[None, :]
    return (jnp.cos(phases), jnp.sin(phases))


def rotate(values, cosines, sines):
    halfway = values.shape[-1] // 2
    leading = values[..., :halfway]
    trailing = values[..., halfway:]
    return jnp.concatenate(
        [leading * cosines - trailing * sines, leading * sines + trailing * cosines], axis=-1
    )


def rotate_back(grads, cosines, sines):
    return rotate(grads, cosines, -sines)


def gate_norm(gate_pre, retained):
    scaled = retained * lax.rsqrt(jnp.mean(retained * retained, axis=-1, keepdims=True) + NORM_EPS)
    return gate_pre * jax.nn.sigmoid(gate_pre) * scaled


def gelu_gate(gate_part, up_part):
    return jax.nn.gelu(gate_part) * up_part


def lamb_parts(weight, moment, second, grad):
    new_moment = BETA_ONE * moment + (1.0 - BETA_ONE) * grad
    new_second = BETA_TWO * second + (1.0 - BETA_TWO) * grad * grad
    moment_hat = new_moment / (1.0 - BETA_ONE**STEP)
    second_hat = new_second / (1.0 - BETA_TWO**STEP)
    ratio = moment_hat / (jnp.sqrt(second_hat) + ADAM_EPS) + DECAY_WT * weight
    return (new_moment, new_second, ratio)


def shift(value, axis, by):
    count = lax.axis_size(axis)
    return lax.ppermute(value, axis, [(i, (i + by) % count) for i in range(count)])


def head_gather(value):
    return [value] + [shift(value, "head", k) for k in range(1, lax.axis_size("head"))]


def head_sum(pieces_of):
    count, mine = lax.axis_size("head"), lax.axis_index("head")
    total = pieces_of(mine).astype(jnp.float32)
    for k in range(1, count):
        piece = pieces_of(lax.rem(mine + k, count)).astype(jnp.bfloat16)
        total = total + shift(piece, "head", k).astype(jnp.float32)
    return total


def in_order(pieces):
    count, mine = len(pieces), lax.axis_index("head")
    rows = pieces[0].shape[0]
    whole = jnp.zeros((count * rows,) + pieces[0].shape[1:], pieces[0].dtype)
    for k, piece in enumerate(pieces):
        at = lax.rem(mine - k + count, count) * rows
        whole = lax.dynamic_update_slice_in_dim(whole, piece, at, 0)
    return whole


def local(
    token_ids,
    completion,
    decay_rate,
    w_mixer,
    w_output,
    w_expand,
    w_contract,
    norm_gains,
    embedding,
    mom_mixer,
    var_mixer,
    mom_output,
    var_output,
    mom_expand,
    var_expand,
    mom_contract,
    var_contract,
    mom_gains,
    var_gains,
    mom_embed,
    var_embed,
):
    bf, f32 = jnp.bfloat16, jnp.float32
    s, h = lax.axis_index("seq"), lax.axis_index("head")
    S, H = lax.axis_size("seq"), lax.axis_size("head")
    total_tokens = token_ids.shape[0]
    span = total_tokens // S
    vocab_part, width = embedding.shape
    quarter = width // H
    cap = span // 2
    own = cap // H
    rows_own = span // H
    assert w_mixer.shape[0] == 1
    token_start = s * span
    vocab_start = s * vocab_part

    mixer = lax.all_gather(w_mixer[0], "seq", axis=0, tiled=True)
    output = lax.all_gather(w_output[0], "seq", axis=1, tiled=True)
    expand = lax.all_gather(w_expand[0], "seq", axis=0, tiled=True)
    contract = lax.all_gather(w_contract[0], "seq", axis=1, tiled=True)
    small = jnp.concatenate([norm_gains.astype(f32), mom_gains, var_gains], axis=0)
    small = jnp.concatenate([small, jnp.zeros((16 - small.shape[0], small.shape[1]), f32)], axis=0)
    small_all = p_ag(small, S, 1).transpose(1, 0, 2).reshape(16, width)
    gains, mom_gains_all, var_gains_all = small_all[:3], small_all[3:6], small_all[6:9]

    ids_grid = token_ids.reshape(S, H, rows_own)
    ids_own = lax.dynamic_index_in_dim(ids_grid, h, 1, keepdims=False)
    chosen = ids_own.reshape(-1) - vocab_start
    inside = (chosen >= 0) & (chosen < vocab_part)
    found = jnp.take(embedding, jnp.clip(chosen, 0, vocab_part - 1), axis=0)
    found = jnp.where(inside[:, None], found, jnp.zeros((), bf))
    rows = p_rs(found.reshape(S, rows_own, width), S, 2).astype(bf)
    x0 = in_order(head_gather(rows))

    mask_own = lax.dynamic_slice_in_dim(completion, token_start, span)
    slot_of = jnp.where(mask_own == 1, jnp.cumsum(mask_own) - 1, -1)
    picker = (slot_of[None, :] == jnp.arange(cap)[:, None]).astype(bf)
    place = jnp.sum(
        jnp.where(slot_of[None, :] == jnp.arange(cap)[:, None], jnp.arange(span)[None, :], 0), axis=1
    )
    mask_grid = completion.reshape(S, span)
    next_ids = jnp.roll(token_ids, -1).reshape(S, span)
    live = (completion * (jnp.arange(total_tokens) < total_tokens - 1)).reshape(S, span)
    slot_grid = jnp.where(mask_grid == 1, jnp.cumsum(mask_grid, axis=1) - 1, -1)
    matches = slot_grid[:, None, :] == jnp.arange(cap)[None, :, None]
    targets = jnp.sum(jnp.where(matches, next_ids[:, None, :], 0), axis=-1)
    row_weights = jnp.sum(jnp.where(matches, live[:, None, :], 0), axis=-1).astype(f32)
    count_live = jnp.sum(live).astype(f32)

    def of_quarter(grid, head):
        return lax.dynamic_index_in_dim(grid.reshape(S, H, own), head, 1, keepdims=False).reshape(-1)

    rate = decay_rate[0, 0]
    steps_in = jnp.arange(span).astype(f32)
    offsets = place[:, None].astype(f32) - steps_in[None, :]
    within = jnp.where(offsets >= 0, jnp.exp(-rate * jnp.maximum(offsets, 0.0)), 0.0)
    tail_decay = jnp.exp(-rate * (span - 1.0 - steps_in))[:, None]
    lead_decay = jnp.exp(-rate * (place.astype(f32) + 1.0))[:, None]
    cosines, sines = rotary_tables(token_start + jnp.arange(span))
    cosines_q, sines_q = rotary_tables(token_start + place)

    def state_sum(update, cid, backward):
        everyone = p_ag(update.astype(bf), S, cid)
        position = jnp.arange(S)
        gap = position - s - 1 if backward else s - 1 - position
        factor = jnp.where(gap >= 0, jnp.exp(-rate * span * jnp.maximum(gap, 0).astype(f32)), 0.0)
        return jnp.sum(everyone.astype(f32) * factor[:, None, None], axis=0).astype(bf)

    hat0 = centre(x0.astype(f32))
    normed = (hat0 * gains[0]).astype(bf)
    proj_kv = matmul(normed, mixer[:, KD : 2 * KD + VD])
    keys = (rotate(proj_kv[:, :KD], cosines, sines) * KD ** (-0.5)).astype(bf)
    values = proj_kv[:, KD:].astype(bf)
    weighted = (keys.astype(f32) * tail_decay).astype(bf)
    update = contract_dims(weighted, values, 0, 0)
    state = state_sum(update, 3, False)
    normed_q = matmul(picker, normed).astype(bf)
    query = rotate(matmul(normed_q, mixer[:, :KD]), cosines_q, sines_q).astype(bf)
    gate_pre = matmul(normed_q, mixer[:, 2 * KD + VD :])
    scores = contract_dims(query, keys, 1, 1)
    weights_blk = (scores * within).astype(bf)
    inner_part = matmul(weights_blk, values)
    retained = inner_part + lead_decay * matmul(query, state)
    gated = gate_norm(gate_pre, retained).astype(bf)

    def own_rows(value):
        return lambda head: lax.dynamic_slice_in_dim(value, head * own, own, 0)

    picker_own = own_rows(picker)(h)
    x0_own = matmul(picker_own, x0)
    x1 = x0_own + head_sum(own_rows(matmul(gated, output)))
    normed_b_own = (centre(x1) * gains[1]).astype(bf)
    normed_b = in_order(head_gather(normed_b_own))
    gate_up = matmul(normed_b, expand)
    width_ff = gate_up.shape[1] // 2
    hidden = gelu_gate(gate_up[:, :width_ff], gate_up[:, width_ff:]).astype(bf)
    x2 = x1 + head_sum(own_rows(matmul(hidden, contract)))
    final_own = (centre(x2) * gains[2]).astype(bf)

    final_rows = p_ag(final_own, S, 4).reshape(S * own, width)
    logits = contract_dims(final_rows, embedding, 1, 1)
    peak = jnp.max(logits, axis=-1)
    exp_total = jnp.sum(jnp.exp(logits - peak[:, None]), axis=-1)
    stats = p_ag(jnp.stack([peak, exp_total]).reshape(-1, 128), S, 5).reshape(S, 2, S * own)
    peak_all = jnp.max(stats[:, 0], axis=0)
    total_all = jnp.sum(stats[:, 1] * jnp.exp(stats[:, 0] - peak_all), axis=0)
    log_total = peak_all + jnp.log(total_all)

    def logits_grad(logits, log_total, head):
        scale = of_quarter(row_weights, head) / count_live
        local_target = of_quarter(targets, head) - vocab_start
        hit = jnp.arange(vocab_part)[None, :] == local_target[:, None]
        grads = jnp.exp(logits - log_total[:, None]) - hit.astype(f32)
        return (grads * scale[:, None]).astype(bf), hit, scale

    grad_logits, hit, scale_row = logits_grad(logits, log_total, h)
    target_logit = jnp.sum(jnp.where(hit, logits, 0.0), axis=-1)
    shard_loss = jnp.sum(scale_row * log_total) * (s == 0).astype(f32) - jnp.sum(
        scale_row * target_logit
    )
    grad_final = p_rs(matmul(grad_logits, embedding).astype(bf).reshape(S, own, width), S, 6)
    grad_x2, grad_gain_final = norm_back(x2, gains[2], grad_final)

    row_pieces = head_gather(final_rows)
    log_pieces = head_gather(log_total.reshape(-1, 128))

    def own_columns(value):
        return lax.dynamic_slice_in_dim(value, h * quarter, quarter, 1)

    grad_table = contract_dims(grad_logits, own_columns(final_rows), 0, 0)
    for k in range(1, H):
        there = lax.rem(h - k + H, H)
        logits_k = contract_dims(row_pieces[k], embedding, 1, 1)
        grads_k = logits_grad(logits_k, log_pieces[k].reshape(-1), there)[0]
        grad_table = grad_table + contract_dims(grads_k, own_columns(row_pieces[k]), 0, 0)

    grad_branch = in_order(head_gather(grad_x2.astype(bf)))
    grad_hidden = contract_dims(grad_branch, contract, 1, 1)
    grad_contract = contract_dims(hidden, grad_branch, 0, 0)
    _, gelu_back = jax.vjp(gelu_gate, gate_up[:, :width_ff], gate_up[:, width_ff:])
    grad_gate_up = jnp.concatenate(gelu_back(grad_hidden), axis=1).astype(bf)
    grad_expand = contract_dims(normed_b, grad_gate_up, 0, 0)
    grad_normed_b = head_sum(own_rows(contract_dims(grad_gate_up, expand, 1, 1)))
    grad_x1, grad_gain_b = norm_back(x1, gains[1], grad_normed_b)
    grad_x1 = grad_x1 + grad_x2
    grad_attn = in_order(head_gather(grad_x1.astype(bf)))
    grad_gated = contract_dims(grad_attn, output, 1, 1)
    grad_output = contract_dims(gated, grad_attn, 0, 0)
    _, gate_back = jax.vjp(gate_norm, gate_pre, retained)
    grad_gate_pre, grad_ret = gate_back(grad_gated)
    grad_cross = (lead_decay * grad_ret).astype(bf)
    grad_ret = grad_ret.astype(bf)
    grad_state = contract_dims(query, grad_cross, 0, 0)
    grad_update = state_sum(grad_state, 7, True)
    grad_weights = contract_dims(grad_ret, values, 1, 1)
    grad_scores = (grad_weights * within).astype(bf)
    grad_query = matmul(grad_scores, keys) + contract_dims(grad_cross, state, 1, 1)
    grad_keys = contract_dims(grad_scores, query, 0, 0)
    grad_values = contract_dims(weights_blk, grad_ret, 0, 0) + matmul(weighted, grad_update)
    grad_keys = grad_keys + contract_dims(values, grad_update, 1, 1) * tail_decay
    grad_q_pre = rotate_back(grad_query, cosines_q, sines_q).astype(bf)
    grad_k_pre = rotate_back(grad_keys * KD ** (-0.5), cosines, sines).astype(bf)
    grad_qg = contract_dims(
        picker, jnp.concatenate([grad_q_pre, grad_gate_pre.astype(bf)], axis=1), 0, 0
    ).astype(bf)
    grad_proj = jnp.concatenate(
        [grad_qg[:, :KD], grad_k_pre, grad_values.astype(bf), grad_qg[:, KD:]], axis=1
    )
    grad_normed = contract_dims(grad_proj, mixer, 1, 1)
    grad_mixer = contract_dims(normed, grad_proj, 0, 0)

    scaled = grad_normed * gains[0]
    row_sums = jnp.stack([jnp.sum(scaled, axis=1), jnp.sum(scaled * hat0, axis=1)]).reshape(-1, 128)
    row_sums = sum(head_gather(row_sums)).reshape(2, span, 1) / width
    columns = head_sum(lambda head: lax.dynamic_slice_in_dim(grad_normed, head * quarter, quarter, 1))
    hat_cols = own_columns(hat0)
    gain_cols = lax.dynamic_slice_in_dim(gains[0], h * quarter, quarter, 0)
    grad_gain_a = jnp.sum(columns * hat_cols, axis=0)
    grad_in = row_scale(x0.astype(f32)) * (columns * gain_cols - row_sums[0] - hat_cols * row_sums[1])
    grad_in = grad_in + contract_dims(picker, own_columns(grad_attn), 0, 0)
    piece_rows = p_ag(grad_in.astype(bf), S, 8).reshape(total_tokens, quarter)
    local_id = token_ids - vocab_start
    one_hot = (jnp.arange(vocab_part)[:, None] == local_id[None, :]).astype(bf)
    grad_table = grad_table + matmul(one_hot, piece_rows)

    def scattered(value, dim):
        return lax.psum_scatter(value.astype(bf), "seq", scatter_dimension=dim, tiled=True).astype(f32)[None]

    grad_contract = scattered(grad_contract, 1)
    grad_expand = scattered(grad_expand, 0)
    grad_output = scattered(grad_output, 1)
    grad_mixer = scattered(grad_mixer, 0)
    grad_gains = jnp.stack(
        [lax.dynamic_update_slice_in_dim(jnp.zeros((width,), f32), grad_gain_a, h * quarter, 0), grad_gain_b, grad_gain_final]
    )

    mixer_f = w_mixer.astype(f32)
    output_f = w_output.astype(f32)
    expand_f = w_expand.astype(f32)
    contract_f = w_contract.astype(f32)
    table_own = own_columns(embedding).astype(f32)
    parts = [
        lamb_parts(mixer_f, mom_mixer, var_mixer, grad_mixer),
        lamb_parts(output_f, mom_output, var_output, grad_output),
        lamb_parts(expand_f, mom_expand, var_expand, grad_expand),
        lamb_parts(contract_f, mom_contract, var_contract, grad_contract),
        lamb_parts(table_own, mom_embed, var_embed, grad_table),
    ]
    held = [mixer_f, output_f, expand_f, contract_f, table_own]
    sums = jnp.stack(
        [jnp.sum(w * w) for w in held] + [jnp.sum(p[2] * p[2]) for p in parts] + [shard_loss]
    )
    packed = jnp.concatenate([jnp.pad(sums, (0, 1024 - sums.shape[0])).reshape(8, 128), grad_gains.reshape(-1, 128)])
    packed = all_sum(packed, S, H, 9)
    sums = packed[0]
    grad_gains = packed[8:].reshape(3, width)
    part_gains = lamb_parts(gains, mom_gains_all, var_gains_all, grad_gains)
    weight_squares = jnp.concatenate([sums[:5], jnp.sum(gains * gains, axis=1)])
    ratio_squares = jnp.concatenate([sums[5:10], jnp.sum(part_gains[2] * part_gains[2], axis=1)])
    trust = jnp.sqrt(weight_squares) * lax.rsqrt(ratio_squares + TRUST_EPSILON)
    new_w = [w - LEARN_RATE * trust[i] * parts[i][2] for i, w in enumerate(held)]
    new_gains = gains - LEARN_RATE * trust[5:][:, None] * part_gains[2]

    def own_gains(value):
        return lax.dynamic_slice_in_dim(value, s * (width // S), width // S, 1)

    return (
        sums[10],
        jnp.stack([weight_squares, ratio_squares], axis=1),
        parts[0][0],
        parts[0][1],
        new_w[0],
        parts[1][0],
        parts[1][1],
        new_w[1],
        parts[2][0],
        parts[2][1],
        new_w[2],
        parts[3][0],
        parts[3][1],
        new_w[3],
        own_gains(part_gains[0]),
        own_gains(part_gains[1]),
        own_gains(new_gains),
        parts[4][0],
        parts[4][1],
        new_w[4],
    )


def solution(mesh):
    placed = (
        P(),
        P(),
        P(None, "head"),
        P(None, "seq", "head"),
        P(None, "head", "seq"),
        P(None, "seq", "head"),
        P(None, "head", "seq"),
        P(None, "seq"),
        P("seq", None),
        P(None, "seq", "head"),
        P(None, "seq", "head"),
        P(None, "head", "seq"),
        P(None, "head", "seq"),
        P(None, "seq", "head"),
        P(None, "seq", "head"),
        P(None, "head", "seq"),
        P(None, "head", "seq"),
        P(None, "seq"),
        P(None, "seq"),
        P("seq", "head"),
        P("seq", "head"),
    )
    return jax.shard_map(
        local,
        mesh=mesh,
        in_specs=placed,
        out_specs=(P(), P()) + placed[3:4] * 3 + placed[4:5] * 3 + placed[3:4] * 3 + placed[4:5] * 3 + placed[7:8] * 3 + placed[19:20] * 3,
        check_vma=False,
    )
```

```python
import jax
import jax.numpy as jnp
from jax import lax
from jax.experimental import pallas as pl
from jax.experimental.pallas import tpu as pltpu
from jax.sharding import PartitionSpec as P

MESH = pl.DeviceIdType.MESH
ANY = pl.BlockSpec(memory_space=pl.ANY)
WHOLE = pl.BlockSpec(memory_space=pltpu.VMEM)
DMA = pltpu.SemaphoreType.DMA


def push(src, dst, sends, recvs, at, target):
    copy = pltpu.make_async_remote_copy(
        src_ref=src,
        dst_ref=dst,
        send_sem=sends.at[at],
        recv_sem=recvs.at[at],
        device_id=target,
        device_id_type=MESH,
    )
    copy.start()
    return copy


def fetch(src, dst, sems, at):
    copy = pltpu.make_async_copy(src, dst, sems.at[at])
    copy.start()
    return copy


def by_rows(count, step, body):
    def one(i, carry):
        body(pl.ds(pl.multiple_of(i * step, step), step))
        return carry

    lax.fori_loop(0, count // step, one, 0)


def row_step(rows):
    return 32 if rows % 32 == 0 else 16


class Here:
    def __init__(self, S, H):
        self.S, self.H, self.N = S, H, S // 2
        self.s, self.h = lax.axis_index("seq"), lax.axis_index("head")
        self.parity = lax.rem(self.s, 2)

    def head(self, k):
        return lax.rem(self.h + k, self.H)

    def seq(self, k):
        return lax.rem(self.s + 2 * k, self.S)

    def heads(self):
        return [{"head": self.head(k)} for k in range(1, self.H)]

    def chips(self):
        return [{"seq": self.seq(k)} for k in range(1, self.N)]

    def other(self):
        return {"seq": self.s + 1 - 2 * self.parity}


class Task:
    def __init__(self, axis, operands, outs, scratch, run):
        self.axis, self.operands, self.outs, self.scratch, self.run = axis, operands, outs, scratch, run


def fused(cid, S, H, tasks, name):
    operands, outs, specs, scratch = [], [], [], []
    for task in tasks:
        operands += task.operands
        for shape, dtype, spec in task.outs:
            outs.append(jax.ShapeDtypeStruct(shape, dtype))
            specs.append(spec)
        scratch += task.scratch

    def body(*refs):
        here = Here(S, H)
        ins, rest = refs[: len(operands)], refs[len(operands) :]
        results, held = rest[: len(outs)], rest[len(outs) :]
        live = []
        for task in tasks:
            live.append(
                task.run(here, ins[: len(task.operands)], results[: len(task.outs)], held[: len(task.scratch)])
            )
            ins, results, held = ins[len(task.operands) :], results[len(task.outs) :], held[len(task.scratch) :]
        axes = {task.axis for task in tasks}
        targets = []
        if axes & {"head", "both"}:
            targets += here.heads()
        if axes & {"seq", "both"}:
            targets += here.chips() + [here.other()]
        barrier = pltpu.get_barrier_semaphore()
        for target in targets:
            pl.semaphore_signal(barrier, inc=1, device_id=target, device_id_type=MESH)
        for run in live:
            next(run)
        pl.semaphore_wait(barrier, len(targets))
        while live:
            live = [run for run in live if next(run, "end") != "end"]

    got = pl.pallas_call(
        body,
        out_shape=outs,
        in_specs=[ANY] * len(operands),
        out_specs=specs,
        scratch_shapes=scratch,
        compiler_params=pltpu.CompilerParams(
            collective_id=cid, has_side_effects=True, vmem_limit_bytes=56 * 2**20
        ),
        cost_estimate=pl.CostEstimate(flops=0, bytes_accessed=2**25, transcendentals=0),
        name=name,
    )(*operands)
    split = []
    for task in tasks:
        split.append(got[: len(task.outs)])
        got = got[len(task.outs) :]
    return split


def gather_head(x, H):
    def run(here, ins, outs, held):
        (src,), (dst,), (sends, recvs, own) = ins, outs, held
        mine = fetch(src, dst.at[here.h], own, 0)
        yield
        copies = [push(src, dst.at[here.h], sends, recvs, k, to) for k, to in enumerate(here.heads())]
        yield
        for copy in copies:
            copy.wait()
        mine.wait()

    return Task("head", [x], [((H,) + x.shape, x.dtype, ANY)], [DMA((H - 1,)), DMA((H - 1,)), DMA((1,))], run)


def sum_head(x, H, columns=False):
    R, C = (x.shape[0], x.shape[1] // H) if columns else x.shape[1:]

    def run(here, ins, outs, held):
        (src,), (dst,), (got, sends, recvs, own) = ins, outs, held

        def block(i):
            return src.at[:, pl.ds(pl.multiple_of(i * C, C), C)] if columns else src.at[i]

        mine = fetch(block(here.h), got.at[0], own, 0)
        yield
        copies = [
            push(block(here.head(k)), got.at[k], sends, recvs, k - 1, {"head": here.head(k)}) for k in range(1, H)
        ]
        yield
        mine.wait()
        for copy in copies:
            copy.wait()

        def add(rows):
            total = got[0, rows, :].astype(jnp.float32)
            for k in range(1, H):
                total = total + got[k, rows, :].astype(jnp.float32)
            dst[rows, :] = total

        by_rows(R, row_step(R), add)

    return Task(
        "head",
        [x],
        [((R, C), jnp.float32, WHOLE)],
        [pltpu.VMEM((H, R, C), x.dtype), DMA((H - 1,)), DMA((H - 1,)), DMA((1,))],
        run,
    )


def gather_seq(x, S, columns=False, ahead=None):
    N = S // 2
    R, C = x.shape[-2:]

    def run(here, ins, outs, held):
        (src,), (dst,), (sends, recvs, fsends, frecvs, own) = ins, outs, held
        if ahead is not None:
            src = src.at[here.head(ahead)]

        def block(i):
            return dst.at[:, pl.ds(pl.multiple_of(i * C, C), C)] if columns else dst.at[i]

        mine = fetch(src, block(here.s), own, 0)
        yield
        copies = [push(src, block(here.s), sends, recvs, k, to) for k, to in enumerate(here.chips() + [here.other()])]
        passed = []
        for k in range(1, N):
            yield
            copies[k - 1].wait_recv()
            source = lax.rem(here.s - 2 * k + 2 * S, S)
            passed.append(push(block(source), block(source), fsends, frecvs, k - 1, here.other()))
        yield
        copies[N - 1].wait_recv()
        for copy in copies:
            copy.wait_send()
        for copy in passed:
            copy.wait()
        mine.wait()

    shape = (R, S * C) if columns else (S, R, C)
    return Task(
        "seq", [x], [(shape, x.dtype, ANY)], [DMA((N,)), DMA((N,)), DMA((N - 1,)), DMA((N - 1,)), DMA((1,))], run
    )


def sum_seq(x, S, columns=False):
    N = S // 2
    R, C = (x.shape[0], x.shape[1] // S) if columns else x.shape[1:]
    order = list(range(1, N)) + [0]

    def run(here, ins, outs, held):
        (src,), (dst,) = ins, outs
        theirs, ours, out, got, sends, recvs, csends, crecvs, own = held

        def block(i):
            return src.at[:, pl.ds(pl.multiple_of(i * C, C), C)] if columns else src.at[i]

        mine = {k: fetch(block(here.seq(k)), ours.at[k], own, k) for k in order}
        yield
        swaps = {
            k: push(block(here.seq(k) + 1 - 2 * here.parity), theirs.at[k], csends, crecvs, k, here.other())
            for k in order
        }
        copies = []
        for k in order:
            yield
            mine[k].wait()
            swaps[k].wait_recv()

            def add(rows, k=k):
                total = ours[k, rows, :].astype(jnp.float32) + theirs[k, rows, :].astype(jnp.float32)
                if k == 0:
                    dst[rows, :] = total
                else:
                    out[k - 1, rows, :] = total.astype(x.dtype)

            by_rows(R, row_step(R), add)
            if k > 0:
                copies.append(push(out.at[k - 1], got.at[k - 1], sends, recvs, k - 1, {"seq": here.seq(k)}))
        yield
        for copy in copies:
            copy.wait()
        for k in order:
            swaps[k].wait_send()

        def total(rows):
            value = dst[rows, :]
            for k in range(N - 1):
                value = value + got[k, rows, :].astype(jnp.float32)
            dst[rows, :] = value

        by_rows(R, row_step(R), total)

    blocks = lambda count: pltpu.VMEM((count, R, C), x.dtype)
    return Task(
        "seq",
        [x],
        [((R, C), jnp.float32, WHOLE)],
        [blocks(N), blocks(N), blocks(N - 1), blocks(N - 1)]
        + [DMA((N - 1,)), DMA((N - 1,)), DMA((N,)), DMA((N,)), DMA((N,))],
        run,
    )


def lookup(x, S, H, parts):
    N = S // 2
    R, C = x.shape[1:]
    piece = R // parts
    order = list(range(1, N)) + [0]

    def run(here, ins, outs, held):
        (src,), (dst,) = ins, outs
        theirs, ours, out, got, sends, recvs, csends, crecvs, zsends, zrecvs, own, left = held
        mine, swaps, copies, spread, kept = {}, {}, {}, [], []
        for q in range(parts):
            rows = pl.ds(q * piece, piece)
            for k in order:
                mine[q, k] = fetch(src.at[here.seq(k), rows], ours.at[k, rows], own, q * N + k)
        yield
        for q in range(parts):
            rows = pl.ds(q * piece, piece)
            for k in order:
                swaps[q, k] = push(
                    src.at[here.seq(k) + 1 - 2 * here.parity, rows],
                    theirs.at[k, rows],
                    csends,
                    crecvs,
                    q * N + k,
                    here.other(),
                )

        def first(q):
            for k in order:
                mine[q, k].wait()
                swaps[q, k].wait_recv()
                for at in range(q * piece, (q + 1) * piece, 16):
                    rows = pl.ds(at, 16)
                    total = ours[k, rows, :] + theirs[k, rows, :]
                    if k == 0:
                        ours[k, rows, :] = total
                    else:
                        out[k - 1, rows, :] = total
                if k > 0:
                    rows = pl.ds(q * piece, piece)
                    copies[q, k] = push(
                        out.at[k - 1, rows],
                        got.at[k - 1, rows],
                        sends,
                        recvs,
                        q * (N - 1) + k - 1,
                        {"seq": here.seq(k)},
                    )

        def second(q):
            for k in range(1, N):
                copies[q, k].wait_recv()
            for at in range(q * piece, (q + 1) * piece, 16):
                rows = pl.ds(at, 16)
                total = ours[0, rows, :]
                for k in range(1, N):
                    total = total + got[k - 1, rows, :]
                ours[0, rows, :] = total
            rows = pl.ds(q * piece, piece)
            kept.append(fetch(ours.at[0, rows], dst.at[here.h, rows], left, q))
            for k in range(1, H):
                spread.append(
                    push(
                        ours.at[0, rows],
                        dst.at[here.h, rows],
                        zsends,
                        zrecvs,
                        q * (H - 1) + k - 1,
                        {"head": here.head(k)},
                    )
                )

        for q in range(parts):
            first(q)
            yield
            if q > 0:
                second(q - 1)
        second(parts - 1)
        yield
        for copy in spread:
            copy.wait()
        for copy in kept:
            copy.wait()
        for q in range(parts):
            for k in order:
                swaps[q, k].wait_send()
                if k > 0:
                    copies[q, k].wait_send()

    blocks = lambda count: pltpu.VMEM((count, R, C), x.dtype)
    return Task(
        "both",
        [x],
        [((H, R, C), x.dtype, ANY)],
        [blocks(N), blocks(N), blocks(N - 1), blocks(N - 1)]
        + [DMA((parts * (N - 1),)), DMA((parts * (N - 1),)), DMA((parts * N,)), DMA((parts * N,))]
        + [DMA((parts * (H - 1),)), DMA((parts * (H - 1),)), DMA((parts * N,)), DMA((parts,))],
        run,
    )


def all_sum(x, S, H, cid):
    def body(x_ref, o_ref, first, middle, second, sends, recvs, zsends, zrecvs):
        s, h = lax.axis_index("seq"), lax.axis_index("head")
        peers = [{"seq": lax.rem(s + k, S)} for k in range(1, S)]
        heads = [{"head": lax.rem(h + k, H)} for k in range(1, H)]
        barrier = pltpu.get_barrier_semaphore()
        for target in peers + heads:
            pl.semaphore_signal(barrier, inc=1, device_id=target, device_id_type=MESH)
        pl.semaphore_wait(barrier, S + H - 2)
        copies = [push(x_ref, first.at[s], sends, recvs, k, peers[k]) for k in range(S - 1)]
        first[s] = x_ref[...]
        for copy in copies:
            copy.wait()
        total = first[0]
        for k in range(1, S):
            total = total + first[k]
        middle[...] = total
        copies = [push(middle, second.at[h], zsends, zrecvs, k, heads[k]) for k in range(H - 1)]
        second[h] = total
        for copy in copies:
            copy.wait()
        total = second[0]
        for k in range(1, H):
            total = total + second[k]
        o_ref[...] = total

    return pl.pallas_call(
        body,
        out_shape=jax.ShapeDtypeStruct(x.shape, x.dtype),
        in_specs=[WHOLE],
        out_specs=WHOLE,
        scratch_shapes=[
            pltpu.VMEM((S,) + x.shape, x.dtype),
            pltpu.VMEM(x.shape, x.dtype),
            pltpu.VMEM((H,) + x.shape, x.dtype),
            DMA((S - 1,)),
            DMA((S - 1,)),
            DMA((H - 1,)),
            DMA((H - 1,)),
        ],
        compiler_params=pltpu.CompilerParams(collective_id=cid, has_side_effects=True),
        name="all_sum",
    )(x)


KD = 256
VD = 512
STEP = 10

NORM_EPS = 1e-05
BETA_ONE = 0.9
BETA_TWO = 0.999
ADAM_EPS = 1e-08
DECAY_WT = 0.01
LEARN_RATE = 0.2
TRUST_EPSILON = 1e-06


def contract_dims(left_side, right_side, left_dim, right_dim):
    return lax.dot_general(
        left_side,
        right_side,
        (((left_dim,), (right_dim,)), ((), ())),
        preferred_element_type=jnp.float32,
    )


def matmul(left_side, right_side):
    return jnp.dot(left_side, right_side, preferred_element_type=jnp.float32)


def centre(values):
    centred = values - jnp.mean(values, axis=-1, keepdims=True)
    return centred * lax.rsqrt(jnp.mean(centred * centred, axis=-1, keepdims=True) + NORM_EPS)


def row_scale(values):
    centred = values - jnp.mean(values, axis=-1, keepdims=True)
    return lax.rsqrt(jnp.mean(centred * centred, axis=-1, keepdims=True) + NORM_EPS)


def norm_back(values, gain_row, grad):
    hat, scale = centre(values), row_scale(values)
    scaled = grad * gain_row
    mean_one = jnp.mean(scaled, axis=-1, keepdims=True)
    mean_two = jnp.mean(scaled * hat, axis=-1, keepdims=True)
    return scale * (scaled - mean_one - hat * mean_two), jnp.sum(grad * hat, axis=0)


def rotary_tables(positions):
    halfway = KD // 2
    frequency = jnp.exp(-jnp.log(10000.0) * jnp.arange(halfway).astype(jnp.float32) / halfway)
    phases = positions.astype(jnp.float32)[:, None] * frequency[None, :]
    return (jnp.cos(phases), jnp.sin(phases))


def rotate(values, cosines, sines):
    halfway = values.shape[-1] // 2
    leading = values[..., :halfway]
    trailing = values[..., halfway:]
    return jnp.concatenate(
        [leading * cosines - trailing * sines, leading * sines + trailing * cosines], axis=-1
    )


def rotate_back(grads, cosines, sines):
    return rotate(grads, cosines, -sines)


def gate_norm(gate_pre, retained):
    scaled = retained * lax.rsqrt(jnp.mean(retained * retained, axis=-1, keepdims=True) + NORM_EPS)
    return gate_pre * jax.nn.sigmoid(gate_pre) * scaled


def gelu_gate(gate_part, up_part):
    return jax.nn.gelu(gate_part) * up_part


def lamb_parts(weight, moment, second, grad):
    new_moment = BETA_ONE * moment + (1.0 - BETA_ONE) * grad
    new_second = BETA_TWO * second + (1.0 - BETA_TWO) * grad * grad
    moment_hat = new_moment / (1.0 - BETA_ONE**STEP)
    second_hat = new_second / (1.0 - BETA_TWO**STEP)
    ratio = moment_hat / (jnp.sqrt(second_hat) + ADAM_EPS) + DECAY_WT * weight
    return (new_moment, new_second, ratio)


def local(
    token_ids,
    completion,
    decay_rate,
    w_mixer,
    w_output,
    w_expand,
    w_contract,
    norm_gains,
    embedding,
    mom_mixer,
    var_mixer,
    mom_output,
    var_output,
    mom_expand,
    var_expand,
    mom_contract,
    var_contract,
    mom_gains,
    var_gains,
    mom_embed,
    var_embed,
):
    bf, f32 = jnp.bfloat16, jnp.float32
    s, h = lax.axis_index("seq"), lax.axis_index("head")
    S, H = lax.axis_size("seq"), lax.axis_size("head")
    total_tokens = token_ids.shape[0]
    span = total_tokens // S
    vocab_part, width = embedding.shape
    quarter = width // H
    cap = span // 2
    own = cap // H
    rows_own = span // H
    assert w_mixer.shape[0] == 1
    token_start = s * span
    vocab_start = s * vocab_part

    aligned = w_output.shape[2] % 128 == 0

    def run(cid, name, *tasks):
        return [results[0] for results in fused(cid, S, H, tasks, name)]

    def flat(blocks):
        return blocks.reshape((-1,) + blocks.shape[2:])

    def gather_columns(weight):
        return gather_seq(weight, S, columns=aligned)

    def joined(gathered):
        if aligned:
            return gathered
        return gathered.transpose(1, 0, 2).reshape(gathered.shape[1], -1)

    def sum_columns(grad):
        grad = grad.astype(bf)
        if not aligned:
            grad = grad.reshape(grad.shape[0], S, -1).transpose(1, 0, 2)
        return sum_seq(grad, S, columns=aligned)

    small = jnp.concatenate([norm_gains.astype(f32), mom_gains, var_gains], axis=0)
    small = jnp.concatenate([small, jnp.zeros((16 - small.shape[0], small.shape[1]), f32)], axis=0)

    ids_grid = token_ids.reshape(S, H, rows_own)
    ids_own = lax.dynamic_index_in_dim(ids_grid, h, 1, keepdims=False)
    chosen = ids_own.reshape(-1) - vocab_start
    inside = (chosen >= 0) & (chosen < vocab_part)
    found = jnp.take(embedding, jnp.clip(chosen, 0, vocab_part - 1), axis=0)
    found = jnp.where(inside[:, None], found, jnp.zeros((), bf))
    rows, mixer, small_all = run(
        1,
        "enter",
        lookup(found.reshape(S, rows_own, width), S, H, 4 if S <= 8 else 1),
        gather_seq(w_mixer[0], S),
        gather_seq(small, S),
    )
    x0, mixer = flat(rows), flat(mixer)
    small_all = small_all.transpose(1, 0, 2).reshape(16, width)
    gains, mom_gains_all, var_gains_all = small_all[:3], small_all[3:6], small_all[6:9]

    mask_own = lax.dynamic_slice_in_dim(completion, token_start, span)
    slot_of = jnp.where(mask_own == 1, jnp.cumsum(mask_own) - 1, -1)
    picker = (slot_of[None, :] == jnp.arange(cap)[:, None]).astype(bf)
    place = jnp.sum(
        jnp.where(slot_of[None, :] == jnp.arange(cap)[:, None], jnp.arange(span)[None, :], 0), axis=1
    )
    mask_grid = completion.reshape(S, span)
    next_ids = jnp.roll(token_ids, -1).reshape(S, span)
    live = (completion * (jnp.arange(total_tokens) < total_tokens - 1)).reshape(S, span)
    slot_grid = jnp.where(mask_grid == 1, jnp.cumsum(mask_grid, axis=1) - 1, -1)
    matches = slot_grid[:, None, :] == jnp.arange(cap)[None, :, None]
    targets = jnp.sum(jnp.where(matches, next_ids[:, None, :], 0), axis=-1)
    row_weights = jnp.sum(jnp.where(matches, live[:, None, :], 0), axis=-1).astype(f32)
    count_live = jnp.sum(live).astype(f32)

    def of_quarter(grid, head):
        return lax.dynamic_index_in_dim(grid.reshape(S, H, own), head, 1, keepdims=False).reshape(-1)

    rate = decay_rate[0, 0]
    steps_in = jnp.arange(span).astype(f32)
    offsets = place[:, None].astype(f32) - steps_in[None, :]
    within = jnp.where(offsets >= 0, jnp.exp(-rate * jnp.maximum(offsets, 0.0)), 0.0)
    tail_decay = jnp.exp(-rate * (span - 1.0 - steps_in))[:, None]
    lead_decay = jnp.exp(-rate * (place.astype(f32) + 1.0))[:, None]
    cosines, sines = rotary_tables(token_start + jnp.arange(span))
    cosines_q, sines_q = rotary_tables(token_start + place)

    def state_sum(everyone, backward):
        position = jnp.arange(S)
        gap = position - s - 1 if backward else s - 1 - position
        factor = jnp.where(gap >= 0, jnp.exp(-rate * span * jnp.maximum(gap, 0).astype(f32)), 0.0)
        return jnp.sum(everyone.astype(f32) * factor[:, None, None], axis=0).astype(bf)

    hat0 = centre(x0.astype(f32))
    normed = (hat0 * gains[0]).astype(bf)
    proj_kv = matmul(normed, mixer[:, KD : 2 * KD + VD])
    keys = (rotate(proj_kv[:, :KD], cosines, sines) * KD ** (-0.5)).astype(bf)
    values = proj_kv[:, KD:].astype(bf)
    weighted = (keys.astype(f32) * tail_decay).astype(bf)
    update = contract_dims(weighted, values, 0, 0)
    everyone, output = run(2, "states", gather_seq(update.astype(bf), S), gather_columns(w_output[0]))
    output = joined(output)
    state = state_sum(everyone, False)
    normed_q = matmul(picker, normed).astype(bf)
    query = rotate(matmul(normed_q, mixer[:, :KD]), cosines_q, sines_q).astype(bf)
    gate_pre = matmul(normed_q, mixer[:, 2 * KD + VD :])
    scores = contract_dims(query, keys, 1, 1)
    weights_blk = (scores * within).astype(bf)
    inner_part = matmul(weights_blk, values)
    retained = inner_part + lead_decay * matmul(query, state)
    gated = gate_norm(gate_pre, retained).astype(bf)

    def by_head(value):
        return sum_head(value.astype(bf).reshape(H, own, width), H)

    x0_own = matmul(lax.dynamic_slice_in_dim(picker, h * own, own, 0), x0)
    branch, expand, contract = run(
        3, "mid", by_head(matmul(gated, output)), gather_seq(w_expand[0], S), gather_columns(w_contract[0])
    )
    expand, contract = flat(expand), joined(contract)
    x1 = x0_own + branch
    normed_b_own = (centre(x1) * gains[1]).astype(bf)
    normed_b = flat(run(4, "normed", gather_head(normed_b_own, H))[0])
    gate_up = matmul(normed_b, expand)
    width_ff = gate_up.shape[1] // 2
    hidden = gelu_gate(gate_up[:, :width_ff], gate_up[:, width_ff:]).astype(bf)
    x2 = x1 + run(5, "feed", by_head(matmul(hidden, contract)))[0]
    final_own = (centre(x2) * gains[2]).astype(bf)

    final_rows = flat(run(6, "final", gather_seq(final_own, S))[0])
    logits = contract_dims(final_rows, embedding, 1, 1)
    peak = jnp.max(logits, axis=-1)
    exp_total = jnp.sum(jnp.exp(logits - peak[:, None]), axis=-1)
    stats = run(7, "stats", gather_seq(jnp.stack([peak, exp_total]).reshape(-1, 128), S))[0].reshape(S, 2, S * own)
    peak_all = jnp.max(stats[:, 0], axis=0)
    total_all = jnp.sum(stats[:, 1] * jnp.exp(stats[:, 0] - peak_all), axis=0)
    log_total = peak_all + jnp.log(total_all)

    def logits_grad(logits, log_total, head):
        scale = of_quarter(row_weights, head) / count_live
        local_target = of_quarter(targets, head) - vocab_start
        hit = jnp.arange(vocab_part)[None, :] == local_target[:, None]
        grads = jnp.exp(logits - log_total[:, None]) - hit.astype(f32)
        return (grads * scale[:, None]).astype(bf), hit, scale

    grad_logits, hit, scale_row = logits_grad(logits, log_total, h)
    target_logit = jnp.sum(jnp.where(hit, logits, 0.0), axis=-1)
    shard_loss = jnp.sum(scale_row * log_total) * (s == 0).astype(f32) - jnp.sum(
        scale_row * target_logit
    )
    grad_final, finals, logs = run(
        8,
        "logits_back",
        sum_seq(matmul(grad_logits, embedding).astype(bf).reshape(S, own, width), S),
        gather_head(final_own, H),
        gather_head(log_total.reshape(-1, 128), H),
    )
    grad_x2, grad_gain_final = norm_back(x2, gains[2], grad_final)

    pieces = {}
    grad_branch, pieces[1], pieces[2] = run(
        9,
        "branch_back",
        gather_head(grad_x2.astype(bf), H),
        gather_seq(finals, S, ahead=1),
        gather_seq(finals, S, ahead=2),
    )
    grad_branch = flat(grad_branch)
    grad_hidden = contract_dims(grad_branch, contract, 1, 1)
    grad_contract = contract_dims(hidden, grad_branch, 0, 0)
    _, gelu_back = jax.vjp(gelu_gate, gate_up[:, :width_ff], gate_up[:, width_ff:])
    grad_gate_up = jnp.concatenate(gelu_back(grad_hidden), axis=1).astype(bf)
    grad_expand = contract_dims(normed_b, grad_gate_up, 0, 0)
    grad_normed_b, pieces[3], grad_contract = run(
        10,
        "expand_back",
        by_head(contract_dims(grad_gate_up, expand, 1, 1)),
        gather_seq(finals, S, ahead=3),
        sum_columns(grad_contract),
    )
    grad_x1, grad_gain_b = norm_back(x1, gains[1], grad_normed_b)
    grad_x1 = grad_x1 + grad_x2
    grad_attn, grad_expand = run(
        11,
        "attn_back",
        gather_head(grad_x1.astype(bf), H),
        sum_seq(grad_expand.astype(bf).reshape(S, -1, grad_expand.shape[1]), S),
    )
    grad_attn = flat(grad_attn)
    grad_gated = contract_dims(grad_attn, output, 1, 1)
    grad_output = contract_dims(gated, grad_attn, 0, 0)
    _, gate_back = jax.vjp(gate_norm, gate_pre, retained)
    grad_gate_pre, grad_ret = gate_back(grad_gated)
    grad_cross = (lead_decay * grad_ret).astype(bf)
    grad_ret = grad_ret.astype(bf)
    grad_state = contract_dims(query, grad_cross, 0, 0)
    everyone, grad_output = run(12, "states_back", gather_seq(grad_state.astype(bf), S), sum_columns(grad_output))
    grad_update = state_sum(everyone, True)
    grad_weights = contract_dims(grad_ret, values, 1, 1)
    grad_scores = (grad_weights * within).astype(bf)
    grad_query = matmul(grad_scores, keys) + contract_dims(grad_cross, state, 1, 1)
    grad_keys = contract_dims(grad_scores, query, 0, 0)
    grad_values = contract_dims(weights_blk, grad_ret, 0, 0) + matmul(weighted, grad_update)
    grad_keys = grad_keys + contract_dims(values, grad_update, 1, 1) * tail_decay
    grad_q_pre = rotate_back(grad_query, cosines_q, sines_q).astype(bf)
    grad_k_pre = rotate_back(grad_keys * KD ** (-0.5), cosines, sines).astype(bf)
    grad_qg = contract_dims(
        picker, jnp.concatenate([grad_q_pre, grad_gate_pre.astype(bf)], axis=1), 0, 0
    ).astype(bf)
    grad_proj = jnp.concatenate(
        [grad_qg[:, :KD], grad_k_pre, grad_values.astype(bf), grad_qg[:, KD:]], axis=1
    )
    grad_normed = contract_dims(grad_proj, mixer, 1, 1)
    grad_mixer = contract_dims(normed, grad_proj, 0, 0)

    def own_columns(value):
        return lax.dynamic_slice_in_dim(value, h * quarter, quarter, 1)

    scaled = grad_normed * gains[0]
    row_sums = jnp.stack([jnp.sum(scaled, axis=1), jnp.sum(scaled * hat0, axis=1)]).reshape(-1, 128)
    columns, row_sums, grad_mixer = run(
        13,
        "mixer_back",
        sum_head(grad_normed.astype(bf), H, columns=True),
        gather_head(row_sums, H),
        sum_seq(grad_mixer.astype(bf).reshape(S, -1, grad_mixer.shape[1]), S),
    )
    row_sums = jnp.sum(row_sums, axis=0).reshape(2, span, 1) / width
    hat_cols = own_columns(hat0)
    gain_cols = lax.dynamic_slice_in_dim(gains[0], h * quarter, quarter, 0)
    grad_gain_a = jnp.sum(columns * hat_cols, axis=0)
    grad_in = row_scale(x0.astype(f32)) * (columns * gain_cols - row_sums[0] - hat_cols * row_sums[1])
    grad_in = grad_in + contract_dims(picker, own_columns(grad_attn), 0, 0)
    piece_rows = flat(run(14, "rows", gather_seq(grad_in.astype(bf), S))[0])
    grad_table = contract_dims(grad_logits, own_columns(final_rows), 0, 0)
    for k in range(1, H):
        there = lax.rem(h + k, H)
        rows_k = flat(pieces[k])
        logits_k = contract_dims(rows_k, embedding, 1, 1)
        log_k = lax.dynamic_index_in_dim(logs, there, 0, keepdims=False).reshape(-1)
        grads_k = logits_grad(logits_k, log_k, there)[0]
        grad_table = grad_table + contract_dims(grads_k, own_columns(rows_k), 0, 0)

    local_id = token_ids - vocab_start
    one_hot = (jnp.arange(vocab_part)[:, None] == local_id[None, :]).astype(bf)
    grad_table = grad_table + matmul(one_hot, piece_rows)

    grad_mixer, grad_output, grad_expand, grad_contract = (
        grad_mixer[None],
        grad_output[None],
        grad_expand[None],
        grad_contract[None],
    )
    grad_gains = jnp.stack(
        [lax.dynamic_update_slice_in_dim(jnp.zeros((width,), f32), grad_gain_a, h * quarter, 0), grad_gain_b, grad_gain_final]
    )

    mixer_f = w_mixer.astype(f32)
    output_f = w_output.astype(f32)
    expand_f = w_expand.astype(f32)
    contract_f = w_contract.astype(f32)
    table_own = own_columns(embedding).astype(f32)
    parts = [
        lamb_parts(mixer_f, mom_mixer, var_mixer, grad_mixer),
        lamb_parts(output_f, mom_output, var_output, grad_output),
        lamb_parts(expand_f, mom_expand, var_expand, grad_expand),
        lamb_parts(contract_f, mom_contract, var_contract, grad_contract),
        lamb_parts(table_own, mom_embed, var_embed, grad_table),
    ]
    held = [mixer_f, output_f, expand_f, contract_f, table_own]
    sums = jnp.stack(
        [jnp.sum(w * w) for w in held] + [jnp.sum(p[2] * p[2]) for p in parts] + [shard_loss]
    )
    packed = jnp.concatenate([jnp.pad(sums, (0, 1024 - sums.shape[0])).reshape(8, 128), grad_gains.reshape(-1, 128)])
    packed = all_sum(packed, S, H, 15)
    sums = packed[0]
    grad_gains = packed[8:].reshape(3, width)
    part_gains = lamb_parts(gains, mom_gains_all, var_gains_all, grad_gains)
    weight_squares = jnp.concatenate([sums[:5], jnp.sum(gains * gains, axis=1)])
    ratio_squares = jnp.concatenate([sums[5:10], jnp.sum(part_gains[2] * part_gains[2], axis=1)])
    trust = jnp.sqrt(weight_squares) * lax.rsqrt(ratio_squares + TRUST_EPSILON)
    new_w = [w - LEARN_RATE * trust[i] * parts[i][2] for i, w in enumerate(held)]
    new_gains = gains - LEARN_RATE * trust[5:][:, None] * part_gains[2]

    def own_gains(value):
        return lax.dynamic_slice_in_dim(value, s * (width // S), width // S, 1)

    return (
        sums[10],
        jnp.stack([weight_squares, ratio_squares], axis=1),
        parts[0][0],
        parts[0][1],
        new_w[0],
        parts[1][0],
        parts[1][1],
        new_w[1],
        parts[2][0],
        parts[2][1],
        new_w[2],
        parts[3][0],
        parts[3][1],
        new_w[3],
        own_gains(part_gains[0]),
        own_gains(part_gains[1]),
        own_gains(new_gains),
        parts[4][0],
        parts[4][1],
        new_w[4],
    )


def solution(mesh):
    placed = (
        P(),
        P(),
        P(None, "head"),
        P(None, "seq", "head"),
        P(None, "head", "seq"),
        P(None, "seq", "head"),
        P(None, "head", "seq"),
        P(None, "seq"),
        P("seq", None),
        P(None, "seq", "head"),
        P(None, "seq", "head"),
        P(None, "head", "seq"),
        P(None, "head", "seq"),
        P(None, "seq", "head"),
        P(None, "seq", "head"),
        P(None, "head", "seq"),
        P(None, "head", "seq"),
        P(None, "seq"),
        P(None, "seq"),
        P("seq", "head"),
        P("seq", "head"),
    )
    return jax.shard_map(
        local,
        mesh=mesh,
        in_specs=placed,
        out_specs=(P(), P()) + placed[3:4] * 3 + placed[4:5] * 3 + placed[3:4] * 3 + placed[4:5] * 3 + placed[7:8] * 3 + placed[19:20] * 3,
        check_vma=False,
    )
```

```python
import jax
import jax.numpy as jnp
from jax import lax
from jax.experimental import pallas as pl
from jax.experimental.pallas import tpu as pltpu
from jax.sharding import PartitionSpec as P

MESH = pl.DeviceIdType.MESH
ANY = pl.BlockSpec(memory_space=pl.ANY)
WHOLE = pl.BlockSpec(memory_space=pltpu.VMEM)
DMA = pltpu.SemaphoreType.DMA


def push(src, dst, sends, recvs, at, target):
    copy = pltpu.make_async_remote_copy(
        src_ref=src,
        dst_ref=dst,
        send_sem=sends.at[at],
        recv_sem=recvs.at[at],
        device_id=target,
        device_id_type=MESH,
    )
    copy.start()
    return copy


def fetch(src, dst, sems, at):
    copy = pltpu.make_async_copy(src, dst, sems.at[at])
    copy.start()
    return copy


def by_rows(count, step, body):
    def one(i, carry):
        body(pl.ds(pl.multiple_of(i * step, step), step))
        return carry

    lax.fori_loop(0, count // step, one, 0)


def row_step(rows):
    return 32 if rows % 32 == 0 else 16


class Here:
    def __init__(self, S, H):
        self.S, self.H, self.N = S, H, S // 2
        self.s, self.h = lax.axis_index("seq"), lax.axis_index("head")
        self.parity = lax.rem(self.s, 2)

    def head(self, k):
        return lax.rem(self.h + k, self.H)

    def seq(self, k):
        return lax.rem(self.s + 2 * k, self.S)

    def heads(self):
        return [{"head": self.head(k)} for k in range(1, self.H)]

    def chips(self):
        return [{"seq": self.seq(k)} for k in range(1, self.N)]

    def other(self):
        return {"seq": self.s + 1 - 2 * self.parity}


class Task:
    def __init__(self, axis, operands, outs, scratch, run):
        self.axis, self.operands, self.outs, self.scratch, self.run = axis, operands, outs, scratch, run


def fused(cid, S, H, tasks, name):
    operands, outs, specs, scratch = [], [], [], []
    for task in tasks:
        operands += task.operands
        for shape, dtype, spec in task.outs:
            outs.append(jax.ShapeDtypeStruct(shape, dtype))
            specs.append(spec)
        scratch += task.scratch

    def body(*refs):
        here = Here(S, H)
        ins, rest = refs[: len(operands)], refs[len(operands) :]
        results, held = rest[: len(outs)], rest[len(outs) :]
        live = []
        for task in tasks:
            live.append(
                task.run(here, ins[: len(task.operands)], results[: len(task.outs)], held[: len(task.scratch)])
            )
            ins, results, held = ins[len(task.operands) :], results[len(task.outs) :], held[len(task.scratch) :]
        axes = {task.axis for task in tasks}
        targets = []
        if axes & {"head", "both"}:
            targets += here.heads()
        if axes & {"seq", "both"}:
            targets += here.chips() + [here.other()]
        barrier = pltpu.get_barrier_semaphore()
        for target in targets:
            pl.semaphore_signal(barrier, inc=1, device_id=target, device_id_type=MESH)
        for run in live:
            next(run)
        pl.semaphore_wait(barrier, len(targets))
        while live:
            live = [run for run in live if next(run, "end") != "end"]

    got = pl.pallas_call(
        body,
        out_shape=outs,
        in_specs=[ANY] * len(operands),
        out_specs=specs,
        scratch_shapes=scratch,
        compiler_params=pltpu.CompilerParams(
            collective_id=cid, has_side_effects=True, vmem_limit_bytes=56 * 2**20
        ),
        cost_estimate=pl.CostEstimate(flops=0, bytes_accessed=2**25, transcendentals=0),
        name=name,
    )(*operands)
    split = []
    for task in tasks:
        split.append(got[: len(task.outs)])
        got = got[len(task.outs) :]
    return split


def gather_head(x, H):
    def run(here, ins, outs, held):
        (src,), (dst,), (sends, recvs, own) = ins, outs, held
        mine = fetch(src, dst.at[here.h], own, 0)
        yield
        copies = [push(src, dst.at[here.h], sends, recvs, k, to) for k, to in enumerate(here.heads())]
        yield
        for copy in copies:
            copy.wait()
        mine.wait()

    return Task("head", [x], [((H,) + x.shape, x.dtype, ANY)], [DMA((H - 1,)), DMA((H - 1,)), DMA((1,))], run)


def sum_head(x, H, columns=False):
    R, C = (x.shape[0], x.shape[1] // H) if columns else x.shape[1:]

    def run(here, ins, outs, held):
        (src,), (dst,), (got, sends, recvs, own) = ins, outs, held

        def block(i):
            return src.at[:, pl.ds(pl.multiple_of(i * C, C), C)] if columns else src.at[i]

        mine = fetch(block(here.h), got.at[0], own, 0)
        yield
        copies = [
            push(block(here.head(k)), got.at[k], sends, recvs, k - 1, {"head": here.head(k)}) for k in range(1, H)
        ]
        yield
        mine.wait()
        for copy in copies:
            copy.wait()

        def add(rows):
            total = got[0, rows, :].astype(jnp.float32)
            for k in range(1, H):
                total = total + got[k, rows, :].astype(jnp.float32)
            dst[rows, :] = total

        by_rows(R, row_step(R), add)

    return Task(
        "head",
        [x],
        [((R, C), jnp.float32, WHOLE)],
        [pltpu.VMEM((H, R, C), x.dtype), DMA((H - 1,)), DMA((H - 1,)), DMA((1,))],
        run,
    )


def gather_seq(x, S, columns=False, ahead=None):
    N = S // 2
    R, C = x.shape[-2:]

    def run(here, ins, outs, held):
        (src,), (dst,), (sends, recvs, fsends, frecvs, own) = ins, outs, held
        if ahead is not None:
            src = src.at[here.head(ahead)]

        def block(i):
            return dst.at[:, pl.ds(pl.multiple_of(i * C, C), C)] if columns else dst.at[i]

        mine = fetch(src, block(here.s), own, 0)
        yield
        copies = [push(src, block(here.s), sends, recvs, k, to) for k, to in enumerate(here.chips() + [here.other()])]
        passed = []
        for k in range(1, N):
            yield
            copies[k - 1].wait_recv()
            source = lax.rem(here.s - 2 * k + 2 * S, S)
            passed.append(push(block(source), block(source), fsends, frecvs, k - 1, here.other()))
        yield
        copies[N - 1].wait_recv()
        for copy in copies:
            copy.wait_send()
        for copy in passed:
            copy.wait()
        mine.wait()

    shape = (R, S * C) if columns else (S, R, C)
    return Task(
        "seq", [x], [(shape, x.dtype, ANY)], [DMA((N,)), DMA((N,)), DMA((N - 1,)), DMA((N - 1,)), DMA((1,))], run
    )


def sum_seq(x, S, columns=False):
    N = S // 2
    R, C = (x.shape[0], x.shape[1] // S) if columns else x.shape[1:]
    order = list(range(1, N)) + [0]

    def run(here, ins, outs, held):
        (src,), (dst,) = ins, outs
        theirs, ours, out, got, sends, recvs, csends, crecvs, own = held

        def block(i):
            return src.at[:, pl.ds(pl.multiple_of(i * C, C), C)] if columns else src.at[i]

        mine = {k: fetch(block(here.seq(k)), ours.at[k], own, k) for k in order}
        yield
        swaps = {
            k: push(block(here.seq(k) + 1 - 2 * here.parity), theirs.at[k], csends, crecvs, k, here.other())
            for k in order
        }
        copies = []
        for k in order:
            yield
            mine[k].wait()
            swaps[k].wait_recv()

            def add(rows, k=k):
                total = ours[k, rows, :].astype(jnp.float32) + theirs[k, rows, :].astype(jnp.float32)
                if k == 0:
                    dst[rows, :] = total
                else:
                    out[k - 1, rows, :] = total.astype(x.dtype)

            by_rows(R, row_step(R), add)
            if k > 0:
                copies.append(push(out.at[k - 1], got.at[k - 1], sends, recvs, k - 1, {"seq": here.seq(k)}))
        yield
        for copy in copies:
            copy.wait()
        for k in order:
            swaps[k].wait_send()

        def total(rows):
            value = dst[rows, :]
            for k in range(N - 1):
                value = value + got[k, rows, :].astype(jnp.float32)
            dst[rows, :] = value

        by_rows(R, row_step(R), total)

    blocks = lambda count: pltpu.VMEM((count, R, C), x.dtype)
    return Task(
        "seq",
        [x],
        [((R, C), jnp.float32, WHOLE)],
        [blocks(N), blocks(N), blocks(N - 1), blocks(N - 1)]
        + [DMA((N - 1,)), DMA((N - 1,)), DMA((N,)), DMA((N,)), DMA((N,))],
        run,
    )


def lookup(x, S, H, parts):
    N = S // 2
    R, C = x.shape[1:]
    piece = R // parts
    order = list(range(1, N)) + [0]

    def run(here, ins, outs, held):
        (src,), (dst,) = ins, outs
        theirs, ours, out, got, sends, recvs, csends, crecvs, zsends, zrecvs, own, left = held
        mine, swaps, copies, spread, kept = {}, {}, {}, [], []
        for q in range(parts):
            rows = pl.ds(q * piece, piece)
            for k in order:
                mine[q, k] = fetch(src.at[here.seq(k), rows], ours.at[k, rows], own, q * N + k)
        yield
        for q in range(parts):
            rows = pl.ds(q * piece, piece)
            for k in order:
                swaps[q, k] = push(
                    src.at[here.seq(k) + 1 - 2 * here.parity, rows],
                    theirs.at[k, rows],
                    csends,
                    crecvs,
                    q * N + k,
                    here.other(),
                )

        def first(q):
            for k in order:
                mine[q, k].wait()
                swaps[q, k].wait_recv()
                for at in range(q * piece, (q + 1) * piece, 16):
                    rows = pl.ds(at, 16)
                    total = ours[k, rows, :] + theirs[k, rows, :]
                    if k == 0:
                        ours[k, rows, :] = total
                    else:
                        out[k - 1, rows, :] = total
                if k > 0:
                    rows = pl.ds(q * piece, piece)
                    copies[q, k] = push(
                        out.at[k - 1, rows],
                        got.at[k - 1, rows],
                        sends,
                        recvs,
                        q * (N - 1) + k - 1,
                        {"seq": here.seq(k)},
                    )

        def second(q):
            for k in range(1, N):
                copies[q, k].wait_recv()
            for at in range(q * piece, (q + 1) * piece, 16):
                rows = pl.ds(at, 16)
                total = ours[0, rows, :]
                for k in range(1, N):
                    total = total + got[k - 1, rows, :]
                ours[0, rows, :] = total
            rows = pl.ds(q * piece, piece)
            kept.append(fetch(ours.at[0, rows], dst.at[here.h, rows], left, q))
            for k in range(1, H):
                spread.append(
                    push(
                        ours.at[0, rows],
                        dst.at[here.h, rows],
                        zsends,
                        zrecvs,
                        q * (H - 1) + k - 1,
                        {"head": here.head(k)},
                    )
                )

        for q in range(parts):
            first(q)
            yield
            if q > 0:
                second(q - 1)
        second(parts - 1)
        yield
        for copy in spread:
            copy.wait()
        for copy in kept:
            copy.wait()
        for q in range(parts):
            for k in order:
                swaps[q, k].wait_send()
                if k > 0:
                    copies[q, k].wait_send()

    blocks = lambda count: pltpu.VMEM((count, R, C), x.dtype)
    return Task(
        "both",
        [x],
        [((H, R, C), x.dtype, ANY)],
        [blocks(N), blocks(N), blocks(N - 1), blocks(N - 1)]
        + [DMA((parts * (N - 1),)), DMA((parts * (N - 1),)), DMA((parts * N,)), DMA((parts * N,))]
        + [DMA((parts * (H - 1),)), DMA((parts * (H - 1),)), DMA((parts * N,)), DMA((parts,))],
        run,
    )


def all_sum(x, S, H, cid):
    def body(x_ref, o_ref, first, middle, second, sends, recvs, zsends, zrecvs):
        s, h = lax.axis_index("seq"), lax.axis_index("head")
        peers = [{"seq": lax.rem(s + k, S)} for k in range(1, S)]
        heads = [{"head": lax.rem(h + k, H)} for k in range(1, H)]
        barrier = pltpu.get_barrier_semaphore()
        for target in peers + heads:
            pl.semaphore_signal(barrier, inc=1, device_id=target, device_id_type=MESH)
        pl.semaphore_wait(barrier, S + H - 2)
        copies = [push(x_ref, first.at[s], sends, recvs, k, peers[k]) for k in range(S - 1)]
        first[s] = x_ref[...]
        for copy in copies:
            copy.wait()
        total = first[0]
        for k in range(1, S):
            total = total + first[k]
        middle[...] = total
        copies = [push(middle, second.at[h], zsends, zrecvs, k, heads[k]) for k in range(H - 1)]
        second[h] = total
        for copy in copies:
            copy.wait()
        total = second[0]
        for k in range(1, H):
            total = total + second[k]
        o_ref[...] = total

    return pl.pallas_call(
        body,
        out_shape=jax.ShapeDtypeStruct(x.shape, x.dtype),
        in_specs=[WHOLE],
        out_specs=WHOLE,
        scratch_shapes=[
            pltpu.VMEM((S,) + x.shape, x.dtype),
            pltpu.VMEM(x.shape, x.dtype),
            pltpu.VMEM((H,) + x.shape, x.dtype),
            DMA((S - 1,)),
            DMA((S - 1,)),
            DMA((H - 1,)),
            DMA((H - 1,)),
        ],
        compiler_params=pltpu.CompilerParams(collective_id=cid, has_side_effects=True),
        name="all_sum",
    )(x)


def late(task, turns):
    before = task.run

    def run(here, ins, outs, held):
        live = before(here, ins, outs, held)
        next(live)
        for _ in range(turns + 1):
            yield
        yield from live

    task.run = run
    return task


def tile_of(count, most):
    fits = [d for d in range(16, most + 1, 16) if count % d == 0]
    return max(fits) if fits else count


def table_grad(embedding, finals, logs, targets, scales, head, H, most=400, slots=768, unroll=1):
    V, D = embedding.shape
    R = finals[0].shape[0]
    Q = D // H
    tile = tile_of(V, most)
    count = R // slots

    def body(head_ref, e_ref, *refs):
        rows, columns = refs[:H], refs[H : 2 * H]
        log_ref, target_ref, scale_ref, o_ref = refs[2 * H :]
        table = e_ref[...]
        first = pl.program_id(0) * tile
        ids = first + lax.broadcasted_iota(jnp.int32, (tile, slots), 0)
        o_ref[...] = jnp.zeros((tile, Q), jnp.float32)
        for k in range(H):

            def chunk(i, carry, k=k):
                at = pl.ds(pl.multiple_of(i * slots, slots), slots)
                logits = lax.dot_general(
                    table, rows[k][at, :], (((1,), (1,)), ((), ())), preferred_element_type=jnp.float32
                )
                place = k * count + i
                grads = jnp.exp(logits - log_ref[place]) - (ids == target_ref[place]).astype(jnp.float32)
                grads = (grads * scale_ref[place]).astype(jnp.bfloat16)
                o_ref[...] += jnp.dot(grads, columns[k][at, :], preferred_element_type=jnp.float32)
                return carry

            lax.fori_loop(0, count, chunk, 0, unroll=unroll)

    fixed = pl.Buffered(1)
    whole = lambda shape: pl.BlockSpec(shape, lambda t, head_ref: (0,) * len(shape), pipeline_mode=fixed)
    shaped = lambda value: value.reshape(H * count, 1, slots)
    return pl.pallas_call(
        body,
        out_shape=jax.ShapeDtypeStruct((V, Q), jnp.float32),
        grid_spec=pltpu.PrefetchScalarGridSpec(
            num_scalar_prefetch=1,
            grid=(V // tile,),
            in_specs=[pl.BlockSpec((tile, D), lambda t, head_ref: (t, 0))]
            + [whole((R, D))] * H
            + [pl.BlockSpec((R, Q), lambda t, head_ref: (0, head_ref[0]), pipeline_mode=fixed)] * H
            + [whole((H * count, 1, slots))] * 3,
            out_specs=pl.BlockSpec((tile, Q), lambda t, head_ref: (t, 0)),
        ),
        compiler_params=pltpu.CompilerParams(vmem_limit_bytes=56 * 2**20),
        cost_estimate=pl.CostEstimate(
            flops=2 * V * H * R * (D + Q), bytes_accessed=V * D * 2 + V * Q * 4 + H * R * D * 2, transcendentals=V * H * R
        ),
        name="table_grad",
    )(head.reshape(1), embedding, *finals, *finals, shaped(logs), shaped(targets), shaped(scales))


KD = 256
VD = 512
STEP = 10

NORM_EPS = 1e-05
BETA_ONE = 0.9
BETA_TWO = 0.999
ADAM_EPS = 1e-08
DECAY_WT = 0.01
LEARN_RATE = 0.2
TRUST_EPSILON = 1e-06


def contract_dims(left_side, right_side, left_dim, right_dim):
    return lax.dot_general(
        left_side,
        right_side,
        (((left_dim,), (right_dim,)), ((), ())),
        preferred_element_type=jnp.float32,
    )


def matmul(left_side, right_side):
    return jnp.dot(left_side, right_side, preferred_element_type=jnp.float32)


def centre(values):
    centred = values - jnp.mean(values, axis=-1, keepdims=True)
    return centred * lax.rsqrt(jnp.mean(centred * centred, axis=-1, keepdims=True) + NORM_EPS)


def row_scale(values):
    centred = values - jnp.mean(values, axis=-1, keepdims=True)
    return lax.rsqrt(jnp.mean(centred * centred, axis=-1, keepdims=True) + NORM_EPS)


def norm_back(values, gain_row, grad):
    hat, scale = centre(values), row_scale(values)
    scaled = grad * gain_row
    mean_one = jnp.mean(scaled, axis=-1, keepdims=True)
    mean_two = jnp.mean(scaled * hat, axis=-1, keepdims=True)
    return scale * (scaled - mean_one - hat * mean_two), jnp.sum(grad * hat, axis=0)


def rotary_tables(positions):
    halfway = KD // 2
    frequency = jnp.exp(-jnp.log(10000.0) * jnp.arange(halfway).astype(jnp.float32) / halfway)
    phases = positions.astype(jnp.float32)[:, None] * frequency[None, :]
    return (jnp.cos(phases), jnp.sin(phases))


def rotate(values, cosines, sines):
    halfway = values.shape[-1] // 2
    leading = values[..., :halfway]
    trailing = values[..., halfway:]
    return jnp.concatenate(
        [leading * cosines - trailing * sines, leading * sines + trailing * cosines], axis=-1
    )


def rotate_back(grads, cosines, sines):
    return rotate(grads, cosines, -sines)


def gate_norm(gate_pre, retained):
    scaled = retained * lax.rsqrt(jnp.mean(retained * retained, axis=-1, keepdims=True) + NORM_EPS)
    return gate_pre * jax.nn.sigmoid(gate_pre) * scaled


def gelu_gate(gate_part, up_part):
    return jax.nn.gelu(gate_part) * up_part


def lamb_parts(weight, moment, second, grad):
    new_moment = BETA_ONE * moment + (1.0 - BETA_ONE) * grad
    new_second = BETA_TWO * second + (1.0 - BETA_TWO) * grad * grad
    moment_hat = new_moment / (1.0 - BETA_ONE**STEP)
    second_hat = new_second / (1.0 - BETA_TWO**STEP)
    ratio = moment_hat / (jnp.sqrt(second_hat) + ADAM_EPS) + DECAY_WT * weight
    return (new_moment, new_second, ratio)


def shift(value, axis, by):
    count = lax.axis_size(axis)
    return lax.ppermute(value, axis, [(i, (i + by) % count) for i in range(count)])


def local(
    token_ids,
    completion,
    decay_rate,
    w_mixer,
    w_output,
    w_expand,
    w_contract,
    norm_gains,
    embedding,
    mom_mixer,
    var_mixer,
    mom_output,
    var_output,
    mom_expand,
    var_expand,
    mom_contract,
    var_contract,
    mom_gains,
    var_gains,
    mom_embed,
    var_embed,
):
    bf, f32 = jnp.bfloat16, jnp.float32
    s, h = lax.axis_index("seq"), lax.axis_index("head")
    S, H = lax.axis_size("seq"), lax.axis_size("head")
    total_tokens = token_ids.shape[0]
    span = total_tokens // S
    vocab_part, width = embedding.shape
    quarter = width // H
    cap = span // 2
    own = cap // H
    rows_own = span // H
    assert w_mixer.shape[0] == 1
    token_start = s * span
    vocab_start = s * vocab_part

    def run(cid, name, *tasks):
        return [results[0] for results in fused(cid, S, H, tasks, name)]

    def flat(blocks):
        return blocks.reshape((-1,) + blocks.shape[2:])

    mixer = lax.all_gather(w_mixer[0], "seq", axis=0, tiled=True)
    output = lax.all_gather(w_output[0], "seq", axis=1, tiled=True)
    expand = lax.all_gather(w_expand[0], "seq", axis=0, tiled=True)
    contract = lax.all_gather(w_contract[0], "seq", axis=1, tiled=True)
    small = jnp.concatenate([norm_gains.astype(f32), mom_gains, var_gains], axis=0)
    small = jnp.concatenate([small, jnp.zeros((16 - small.shape[0], small.shape[1]), f32)], axis=0)

    ids_grid = token_ids.reshape(S, H, rows_own)
    ids_own = lax.dynamic_index_in_dim(ids_grid, h, 1, keepdims=False)
    chosen = ids_own.reshape(-1) - vocab_start
    inside = (chosen >= 0) & (chosen < vocab_part)
    found = jnp.take(embedding, jnp.clip(chosen, 0, vocab_part - 1), axis=0)
    found = jnp.where(inside[:, None], found, jnp.zeros((), bf))
    rows, small_all = run(
        1,
        "enter",
        lookup(found.reshape(S, rows_own, width), S, H, 4 if S <= 8 else 1),
        gather_seq(small, S),
    )
    x0 = flat(rows)
    small_all = small_all.transpose(1, 0, 2).reshape(16, width)
    gains, mom_gains_all, var_gains_all = small_all[:3], small_all[3:6], small_all[6:9]

    mask_own = lax.dynamic_slice_in_dim(completion, token_start, span)
    slot_of = jnp.where(mask_own == 1, jnp.cumsum(mask_own) - 1, -1)
    picker = (slot_of[None, :] == jnp.arange(cap)[:, None]).astype(bf)
    place = jnp.sum(
        jnp.where(slot_of[None, :] == jnp.arange(cap)[:, None], jnp.arange(span)[None, :], 0), axis=1
    )
    mask_grid = completion.reshape(S, span)
    next_ids = jnp.roll(token_ids, -1).reshape(S, span)
    live = (completion * (jnp.arange(total_tokens) < total_tokens - 1)).reshape(S, span)
    slot_grid = jnp.where(mask_grid == 1, jnp.cumsum(mask_grid, axis=1) - 1, -1)
    matches = slot_grid[:, None, :] == jnp.arange(cap)[None, :, None]
    targets = jnp.sum(jnp.where(matches, next_ids[:, None, :], 0), axis=-1)
    row_weights = jnp.sum(jnp.where(matches, live[:, None, :], 0), axis=-1).astype(f32)
    count_live = jnp.sum(live).astype(f32)

    def of_quarter(grid, head):
        return lax.dynamic_index_in_dim(grid.reshape(S, H, own), head, 1, keepdims=False).reshape(-1)

    rate = decay_rate[0, 0]
    steps_in = jnp.arange(span).astype(f32)
    offsets = place[:, None].astype(f32) - steps_in[None, :]
    within = jnp.where(offsets >= 0, jnp.exp(-rate * jnp.maximum(offsets, 0.0)), 0.0)
    tail_decay = jnp.exp(-rate * (span - 1.0 - steps_in))[:, None]
    lead_decay = jnp.exp(-rate * (place.astype(f32) + 1.0))[:, None]
    cosines, sines = rotary_tables(token_start + jnp.arange(span))
    cosines_q, sines_q = rotary_tables(token_start + place)

    def state_sum(everyone, backward):
        position = jnp.arange(S)
        gap = position - s - 1 if backward else s - 1 - position
        factor = jnp.where(gap >= 0, jnp.exp(-rate * span * jnp.maximum(gap, 0).astype(f32)), 0.0)
        return jnp.sum(everyone.astype(f32) * factor[:, None, None], axis=0).astype(bf)

    hat0 = centre(x0.astype(f32))
    normed = (hat0 * gains[0]).astype(bf)
    proj_kv = matmul(normed, mixer[:, KD : 2 * KD + VD])
    keys = (rotate(proj_kv[:, :KD], cosines, sines) * KD ** (-0.5)).astype(bf)
    values = proj_kv[:, KD:].astype(bf)
    weighted = (keys.astype(f32) * tail_decay).astype(bf)
    update = contract_dims(weighted, values, 0, 0)
    state = state_sum(run(2, "states", gather_seq(update.astype(bf), S))[0], False)
    normed_q = matmul(picker, normed).astype(bf)
    query = rotate(matmul(normed_q, mixer[:, :KD]), cosines_q, sines_q).astype(bf)
    gate_pre = matmul(normed_q, mixer[:, 2 * KD + VD :])
    scores = contract_dims(query, keys, 1, 1)
    weights_blk = (scores * within).astype(bf)
    inner_part = matmul(weights_blk, values)
    retained = inner_part + lead_decay * matmul(query, state)
    gated = gate_norm(gate_pre, retained).astype(bf)

    def by_head(value):
        return sum_head(value.astype(bf).reshape(H, own, width), H)

    x0_own = matmul(lax.dynamic_slice_in_dim(picker, h * own, own, 0), x0)
    x1 = x0_own + run(3, "mid", by_head(matmul(gated, output)))[0]
    normed_b_own = (centre(x1) * gains[1]).astype(bf)
    normed_b = flat(run(4, "normed", gather_head(normed_b_own, H))[0])
    gate_up = matmul(normed_b, expand)
    width_ff = gate_up.shape[1] // 2
    hidden = gelu_gate(gate_up[:, :width_ff], gate_up[:, width_ff:]).astype(bf)
    x2 = x1 + run(5, "feed", by_head(matmul(hidden, contract)))[0]
    final_own = (centre(x2) * gains[2]).astype(bf)

    final_rows = flat(run(6, "final", gather_seq(final_own, S))[0])
    logits = contract_dims(final_rows, embedding, 1, 1)
    peak = jnp.max(logits, axis=-1)
    exp_total = jnp.sum(jnp.exp(logits - peak[:, None]), axis=-1)
    stats = run(7, "stats", gather_seq(jnp.stack([peak, exp_total]).reshape(-1, 128), S))[0].reshape(S, 2, S * own)
    peak_all = jnp.max(stats[:, 0], axis=0)
    total_all = jnp.sum(stats[:, 1] * jnp.exp(stats[:, 0] - peak_all), axis=0)
    log_total = peak_all + jnp.log(total_all)

    def logits_grad(logits, log_total, head):
        scale = of_quarter(row_weights, head) / count_live
        local_target = of_quarter(targets, head) - vocab_start
        hit = jnp.arange(vocab_part)[None, :] == local_target[:, None]
        grads = jnp.exp(logits - log_total[:, None]) - hit.astype(f32)
        return (grads * scale[:, None]).astype(bf), hit, scale

    grad_logits, hit, scale_row = logits_grad(logits, log_total, h)
    target_logit = jnp.sum(jnp.where(hit, logits, 0.0), axis=-1)
    shard_loss = jnp.sum(scale_row * log_total) * (s == 0).astype(f32) - jnp.sum(
        scale_row * target_logit
    )
    grad_final, finals, logs = run(
        8,
        "logits_back",
        sum_seq(matmul(grad_logits, embedding).astype(bf).reshape(S, own, width), S),
        late(gather_head(final_own, H), 2),
        gather_head(log_total.reshape(-1, 128), H),
    )
    grad_x2, grad_gain_final = norm_back(x2, gains[2], grad_final)

    pieces = {}
    grad_branch, pieces[1] = run(
        9, "branch_back", gather_head(grad_x2.astype(bf), H), gather_seq(finals, S, ahead=1)
    )
    grad_branch = flat(grad_branch)
    grad_hidden = contract_dims(grad_branch, contract, 1, 1)
    grad_contract = contract_dims(hidden, grad_branch, 0, 0)
    _, gelu_back = jax.vjp(gelu_gate, gate_up[:, :width_ff], gate_up[:, width_ff:])
    grad_gate_up = jnp.concatenate(gelu_back(grad_hidden), axis=1).astype(bf)
    grad_expand = contract_dims(normed_b, grad_gate_up, 0, 0)
    grad_normed_b, pieces[2] = run(
        10, "expand_back", by_head(contract_dims(grad_gate_up, expand, 1, 1)), gather_seq(finals, S, ahead=2)
    )
    grad_x1, grad_gain_b = norm_back(x1, gains[1], grad_normed_b)
    grad_x1 = grad_x1 + grad_x2
    grad_attn, pieces[3] = run(
        11, "attn_back", gather_head(grad_x1.astype(bf), H), gather_seq(finals, S, ahead=3)
    )
    grad_attn = flat(grad_attn)
    grad_gated = contract_dims(grad_attn, output, 1, 1)
    grad_output = contract_dims(gated, grad_attn, 0, 0)
    _, gate_back = jax.vjp(gate_norm, gate_pre, retained)
    grad_gate_pre, grad_ret = gate_back(grad_gated)
    grad_cross = (lead_decay * grad_ret).astype(bf)
    grad_ret = grad_ret.astype(bf)
    grad_state = contract_dims(query, grad_cross, 0, 0)
    grad_update = state_sum(run(12, "states_back", gather_seq(grad_state.astype(bf), S))[0], True)
    grad_weights = contract_dims(grad_ret, values, 1, 1)
    grad_scores = (grad_weights * within).astype(bf)
    grad_query = matmul(grad_scores, keys) + contract_dims(grad_cross, state, 1, 1)
    grad_keys = contract_dims(grad_scores, query, 0, 0)
    grad_values = contract_dims(weights_blk, grad_ret, 0, 0) + matmul(weighted, grad_update)
    grad_keys = grad_keys + contract_dims(values, grad_update, 1, 1) * tail_decay
    grad_q_pre = rotate_back(grad_query, cosines_q, sines_q).astype(bf)
    grad_k_pre = rotate_back(grad_keys * KD ** (-0.5), cosines, sines).astype(bf)
    grad_qg = contract_dims(
        picker, jnp.concatenate([grad_q_pre, grad_gate_pre.astype(bf)], axis=1), 0, 0
    ).astype(bf)
    grad_proj = jnp.concatenate(
        [grad_qg[:, :KD], grad_k_pre, grad_values.astype(bf), grad_qg[:, KD:]], axis=1
    )
    grad_normed = contract_dims(grad_proj, mixer, 1, 1)
    grad_mixer = contract_dims(normed, grad_proj, 0, 0)

    def own_columns(value):
        return lax.dynamic_slice_in_dim(value, h * quarter, quarter, 1)

    scaled = grad_normed * gains[0]
    row_sums = jnp.stack([jnp.sum(scaled, axis=1), jnp.sum(scaled * hat0, axis=1)]).reshape(-1, 128)
    there = lax.rem(h + jnp.arange(H), H)

    def in_turn(grid):
        return jnp.take(grid.reshape(S, H, own).transpose(1, 0, 2).reshape(H, S * own), there, axis=0)

    logs = jnp.take(logs.reshape(H, S * own), there, axis=0)
    scales = in_turn(row_weights / count_live)
    aims = in_turn(targets) - vocab_start
    sent = grad_normed.astype(bf)
    sent, row_sums, logs = lax.optimization_barrier((sent, row_sums, logs))
    column_parts, sum_parts = [own_columns(sent)], [row_sums]
    for k in range(1, H):
        part = lax.dynamic_slice_in_dim(sent, lax.rem(h + k, H) * quarter, quarter, 1)
        column_parts.append(shift(part, "head", k))
        sum_parts.append(shift(row_sums, "head", k))
    grad_table = table_grad(
        embedding, [final_rows, flat(pieces[1]), flat(pieces[2]), flat(pieces[3])], logs, aims, scales, h, H
    )
    column_parts, sum_parts, grad_table = lax.optimization_barrier((column_parts, sum_parts, grad_table))
    columns = sum(part.astype(f32) for part in column_parts)
    row_sums = sum(sum_parts).reshape(2, span, 1) / width
    hat_cols = own_columns(hat0)
    gain_cols = lax.dynamic_slice_in_dim(gains[0], h * quarter, quarter, 0)
    grad_gain_a = jnp.sum(columns * hat_cols, axis=0)
    grad_in = row_scale(x0.astype(f32)) * (columns * gain_cols - row_sums[0] - hat_cols * row_sums[1])
    grad_in = grad_in + contract_dims(picker, own_columns(grad_attn), 0, 0)
    piece_rows = flat(run(14, "rows", gather_seq(grad_in.astype(bf), S))[0])
    local_id = token_ids - vocab_start
    one_hot = (jnp.arange(vocab_part)[:, None] == local_id[None, :]).astype(bf)
    grad_table = grad_table + matmul(one_hot, piece_rows)

    def scattered(value, dim):
        return lax.psum_scatter(value.astype(bf), "seq", scatter_dimension=dim, tiled=True).astype(f32)[None]

    grad_contract = scattered(grad_contract, 1)
    grad_expand = scattered(grad_expand, 0)
    grad_output = scattered(grad_output, 1)
    grad_mixer = scattered(grad_mixer, 0)
    grad_gains = jnp.stack(
        [lax.dynamic_update_slice_in_dim(jnp.zeros((width,), f32), grad_gain_a, h * quarter, 0), grad_gain_b, grad_gain_final]
    )

    mixer_f = w_mixer.astype(f32)
    output_f = w_output.astype(f32)
    expand_f = w_expand.astype(f32)
    contract_f = w_contract.astype(f32)
    table_own = own_columns(embedding).astype(f32)
    parts = [
        lamb_parts(mixer_f, mom_mixer, var_mixer, grad_mixer),
        lamb_parts(output_f, mom_output, var_output, grad_output),
        lamb_parts(expand_f, mom_expand, var_expand, grad_expand),
        lamb_parts(contract_f, mom_contract, var_contract, grad_contract),
        lamb_parts(table_own, mom_embed, var_embed, grad_table),
    ]
    held = [mixer_f, output_f, expand_f, contract_f, table_own]
    sums = jnp.stack(
        [jnp.sum(w * w) for w in held] + [jnp.sum(p[2] * p[2]) for p in parts] + [shard_loss]
    )
    packed = jnp.concatenate([jnp.pad(sums, (0, 1024 - sums.shape[0])).reshape(8, 128), grad_gains.reshape(-1, 128)])
    packed = all_sum(packed, S, H, 15)
    sums = packed[0]
    grad_gains = packed[8:].reshape(3, width)
    part_gains = lamb_parts(gains, mom_gains_all, var_gains_all, grad_gains)
    weight_squares = jnp.concatenate([sums[:5], jnp.sum(gains * gains, axis=1)])
    ratio_squares = jnp.concatenate([sums[5:10], jnp.sum(part_gains[2] * part_gains[2], axis=1)])
    trust = jnp.sqrt(weight_squares) * lax.rsqrt(ratio_squares + TRUST_EPSILON)
    new_w = [w - LEARN_RATE * trust[i] * parts[i][2] for i, w in enumerate(held)]
    new_gains = gains - LEARN_RATE * trust[5:][:, None] * part_gains[2]

    def own_gains(value):
        return lax.dynamic_slice_in_dim(value, s * (width // S), width // S, 1)

    return (
        sums[10],
        jnp.stack([weight_squares, ratio_squares], axis=1),
        parts[0][0],
        parts[0][1],
        new_w[0],
        parts[1][0],
        parts[1][1],
        new_w[1],
        parts[2][0],
        parts[2][1],
        new_w[2],
        parts[3][0],
        parts[3][1],
        new_w[3],
        own_gains(part_gains[0]),
        own_gains(part_gains[1]),
        own_gains(new_gains),
        parts[4][0],
        parts[4][1],
        new_w[4],
    )


def solution(mesh):
    placed = (
        P(),
        P(),
        P(None, "head"),
        P(None, "seq", "head"),
        P(None, "head", "seq"),
        P(None, "seq", "head"),
        P(None, "head", "seq"),
        P(None, "seq"),
        P("seq", None),
        P(None, "seq", "head"),
        P(None, "seq", "head"),
        P(None, "head", "seq"),
        P(None, "head", "seq"),
        P(None, "seq", "head"),
        P(None, "seq", "head"),
        P(None, "head", "seq"),
        P(None, "head", "seq"),
        P(None, "seq"),
        P(None, "seq"),
        P("seq", "head"),
        P("seq", "head"),
    )
    return jax.shard_map(
        local,
        mesh=mesh,
        in_specs=placed,
        out_specs=(P(), P()) + placed[3:4] * 3 + placed[4:5] * 3 + placed[3:4] * 3 + placed[4:5] * 3 + placed[7:8] * 3 + placed[19:20] * 3,
        check_vma=False,
    )
```

```python
import jax
import jax.numpy as jnp
from jax import lax
from jax.experimental import pallas as pl
from jax.experimental.pallas import tpu as pltpu
from jax.sharding import PartitionSpec as P

MESH = pl.DeviceIdType.MESH
ANY = pl.BlockSpec(memory_space=pl.ANY)
WHOLE = pl.BlockSpec(memory_space=pltpu.VMEM)
DMA = pltpu.SemaphoreType.DMA


def push(src, dst, sends, recvs, at, target):
    copy = pltpu.make_async_remote_copy(
        src_ref=src,
        dst_ref=dst,
        send_sem=sends.at[at],
        recv_sem=recvs.at[at],
        device_id=target,
        device_id_type=MESH,
    )
    copy.start()
    return copy


def fetch(src, dst, sems, at):
    copy = pltpu.make_async_copy(src, dst, sems.at[at])
    copy.start()
    return copy


def by_rows(count, step, body):
    def one(i, carry):
        body(pl.ds(pl.multiple_of(i * step, step), step))
        return carry

    lax.fori_loop(0, count // step, one, 0)


def row_step(rows):
    return 32 if rows % 32 == 0 else 16


class Here:
    def __init__(self, S, H):
        self.S, self.H, self.N = S, H, S // 2
        self.s, self.h = lax.axis_index("seq"), lax.axis_index("head")
        self.parity = lax.rem(self.s, 2)

    def head(self, k):
        return lax.rem(self.h + k, self.H)

    def seq(self, k):
        return lax.rem(self.s + 2 * k, self.S)

    def heads(self):
        return [{"head": self.head(k)} for k in range(1, self.H)]

    def chips(self):
        return [{"seq": self.seq(k)} for k in range(1, self.N)]

    def other(self):
        return {"seq": self.s + 1 - 2 * self.parity}


class Task:
    def __init__(self, axis, operands, outs, scratch, run):
        self.axis, self.operands, self.outs, self.scratch, self.run = axis, operands, outs, scratch, run


def fused(cid, S, H, tasks, name):
    operands, outs, specs, scratch = [], [], [], []
    for task in tasks:
        operands += task.operands
        for shape, dtype, spec in task.outs:
            outs.append(jax.ShapeDtypeStruct(shape, dtype))
            specs.append(spec)
        scratch += task.scratch

    def body(*refs):
        here = Here(S, H)
        ins, rest = refs[: len(operands)], refs[len(operands) :]
        results, held = rest[: len(outs)], rest[len(outs) :]
        live = []
        for task in tasks:
            live.append(
                task.run(here, ins[: len(task.operands)], results[: len(task.outs)], held[: len(task.scratch)])
            )
            ins, results, held = ins[len(task.operands) :], results[len(task.outs) :], held[len(task.scratch) :]
        axes = {task.axis for task in tasks}
        targets = []
        if axes & {"head", "both"}:
            targets += here.heads()
        if axes & {"seq", "both"}:
            targets += here.chips() + [here.other()]
        barrier = pltpu.get_barrier_semaphore()
        for target in targets:
            pl.semaphore_signal(barrier, inc=1, device_id=target, device_id_type=MESH)
        for run in live:
            next(run)
        pl.semaphore_wait(barrier, len(targets))
        while live:
            live = [run for run in live if next(run, "end") != "end"]

    got = pl.pallas_call(
        body,
        out_shape=outs,
        in_specs=[ANY] * len(operands),
        out_specs=specs,
        scratch_shapes=scratch,
        compiler_params=pltpu.CompilerParams(
            collective_id=cid, has_side_effects=True, vmem_limit_bytes=56 * 2**20
        ),
        cost_estimate=pl.CostEstimate(flops=0, bytes_accessed=2**25, transcendentals=0),
        name=name,
    )(*operands)
    split = []
    for task in tasks:
        split.append(got[: len(task.outs)])
        got = got[len(task.outs) :]
    return split


def gather_head(x, H):
    def run(here, ins, outs, held):
        (src,), (dst,), (sends, recvs, own) = ins, outs, held
        mine = fetch(src, dst.at[here.h], own, 0)
        yield
        copies = [push(src, dst.at[here.h], sends, recvs, k, to) for k, to in enumerate(here.heads())]
        yield
        for copy in copies:
            copy.wait()
        mine.wait()

    return Task("head", [x], [((H,) + x.shape, x.dtype, ANY)], [DMA((H - 1,)), DMA((H - 1,)), DMA((1,))], run)


def sum_head(x, H, columns=False):
    R, C = (x.shape[0], x.shape[1] // H) if columns else x.shape[1:]

    def run(here, ins, outs, held):
        (src,), (dst,), (got, sends, recvs, own) = ins, outs, held

        def block(i):
            return src.at[:, pl.ds(pl.multiple_of(i * C, C), C)] if columns else src.at[i]

        mine = fetch(block(here.h), got.at[0], own, 0)
        yield
        copies = [
            push(block(here.head(k)), got.at[k], sends, recvs, k - 1, {"head": here.head(k)}) for k in range(1, H)
        ]
        yield
        mine.wait()
        for copy in copies:
            copy.wait()

        def add(rows):
            total = got[0, rows, :].astype(jnp.float32)
            for k in range(1, H):
                total = total + got[k, rows, :].astype(jnp.float32)
            dst[rows, :] = total

        by_rows(R, row_step(R), add)

    return Task(
        "head",
        [x],
        [((R, C), jnp.float32, WHOLE)],
        [pltpu.VMEM((H, R, C), x.dtype), DMA((H - 1,)), DMA((H - 1,)), DMA((1,))],
        run,
    )


def gather_seq(x, S, columns=False, ahead=None):
    N = S // 2
    R, C = x.shape[-2:]

    def run(here, ins, outs, held):
        (src,), (dst,), (sends, recvs, fsends, frecvs, own) = ins, outs, held
        if ahead is not None:
            src = src.at[here.head(ahead)]

        def block(i):
            return dst.at[:, pl.ds(pl.multiple_of(i * C, C), C)] if columns else dst.at[i]

        mine = fetch(src, block(here.s), own, 0)
        yield
        copies = [push(src, block(here.s), sends, recvs, k, to) for k, to in enumerate(here.chips() + [here.other()])]
        passed = []
        for k in range(1, N):
            yield
            copies[k - 1].wait_recv()
            source = lax.rem(here.s - 2 * k + 2 * S, S)
            passed.append(push(block(source), block(source), fsends, frecvs, k - 1, here.other()))
        yield
        copies[N - 1].wait_recv()
        for copy in copies:
            copy.wait_send()
        for copy in passed:
            copy.wait()
        mine.wait()

    shape = (R, S * C) if columns else (S, R, C)
    return Task(
        "seq", [x], [(shape, x.dtype, ANY)], [DMA((N,)), DMA((N,)), DMA((N - 1,)), DMA((N - 1,)), DMA((1,))], run
    )


def sum_seq(x, S, columns=False):
    N = S // 2
    R, C = (x.shape[0], x.shape[1] // S) if columns else x.shape[1:]
    order = list(range(1, N)) + [0]

    def run(here, ins, outs, held):
        (src,), (dst,) = ins, outs
        theirs, ours, out, got, sends, recvs, csends, crecvs, own = held

        def block(i):
            return src.at[:, pl.ds(pl.multiple_of(i * C, C), C)] if columns else src.at[i]

        mine = {k: fetch(block(here.seq(k)), ours.at[k], own, k) for k in order}
        yield
        swaps = {
            k: push(block(here.seq(k) + 1 - 2 * here.parity), theirs.at[k], csends, crecvs, k, here.other())
            for k in order
        }
        copies = []
        for k in order:
            yield
            mine[k].wait()
            swaps[k].wait_recv()

            def add(rows, k=k):
                total = ours[k, rows, :].astype(jnp.float32) + theirs[k, rows, :].astype(jnp.float32)
                if k == 0:
                    dst[rows, :] = total
                else:
                    out[k - 1, rows, :] = total.astype(x.dtype)

            by_rows(R, row_step(R), add)
            if k > 0:
                copies.append(push(out.at[k - 1], got.at[k - 1], sends, recvs, k - 1, {"seq": here.seq(k)}))
        yield
        for copy in copies:
            copy.wait()
        for k in order:
            swaps[k].wait_send()

        def total(rows):
            value = dst[rows, :]
            for k in range(N - 1):
                value = value + got[k, rows, :].astype(jnp.float32)
            dst[rows, :] = value

        by_rows(R, row_step(R), total)

    blocks = lambda count: pltpu.VMEM((count, R, C), x.dtype)
    return Task(
        "seq",
        [x],
        [((R, C), jnp.float32, WHOLE)],
        [blocks(N), blocks(N), blocks(N - 1), blocks(N - 1)]
        + [DMA((N - 1,)), DMA((N - 1,)), DMA((N,)), DMA((N,)), DMA((N,))],
        run,
    )


def lookup(x, S, H, parts):
    N = S // 2
    R, C = x.shape[1:]
    piece = R // parts
    order = list(range(1, N)) + [0]

    def run(here, ins, outs, held):
        (src,), (dst,) = ins, outs
        theirs, ours, out, got, sends, recvs, csends, crecvs, zsends, zrecvs, own, left = held
        mine, swaps, copies, spread, kept = {}, {}, {}, [], []
        for q in range(parts):
            rows = pl.ds(q * piece, piece)
            for k in order:
                mine[q, k] = fetch(src.at[here.seq(k), rows], ours.at[k, rows], own, q * N + k)
        yield
        for q in range(parts):
            rows = pl.ds(q * piece, piece)
            for k in order:
                swaps[q, k] = push(
                    src.at[here.seq(k) + 1 - 2 * here.parity, rows],
                    theirs.at[k, rows],
                    csends,
                    crecvs,
                    q * N + k,
                    here.other(),
                )

        def first(q):
            for k in order:
                mine[q, k].wait()
                swaps[q, k].wait_recv()
                for at in range(q * piece, (q + 1) * piece, 16):
                    rows = pl.ds(at, 16)
                    total = ours[k, rows, :] + theirs[k, rows, :]
                    if k == 0:
                        ours[k, rows, :] = total
                    else:
                        out[k - 1, rows, :] = total
                if k > 0:
                    rows = pl.ds(q * piece, piece)
                    copies[q, k] = push(
                        out.at[k - 1, rows],
                        got.at[k - 1, rows],
                        sends,
                        recvs,
                        q * (N - 1) + k - 1,
                        {"seq": here.seq(k)},
                    )

        def second(q):
            for k in range(1, N):
                copies[q, k].wait_recv()
            for at in range(q * piece, (q + 1) * piece, 16):
                rows = pl.ds(at, 16)
                total = ours[0, rows, :]
                for k in range(1, N):
                    total = total + got[k - 1, rows, :]
                ours[0, rows, :] = total
            rows = pl.ds(q * piece, piece)
            kept.append(fetch(ours.at[0, rows], dst.at[here.h, rows], left, q))
            for k in range(1, H):
                spread.append(
                    push(
                        ours.at[0, rows],
                        dst.at[here.h, rows],
                        zsends,
                        zrecvs,
                        q * (H - 1) + k - 1,
                        {"head": here.head(k)},
                    )
                )

        for q in range(parts):
            first(q)
            yield
            if q > 0:
                second(q - 1)
        second(parts - 1)
        yield
        for copy in spread:
            copy.wait()
        for copy in kept:
            copy.wait()
        for q in range(parts):
            for k in order:
                swaps[q, k].wait_send()
                if k > 0:
                    copies[q, k].wait_send()

    blocks = lambda count: pltpu.VMEM((count, R, C), x.dtype)
    return Task(
        "both",
        [x],
        [((H, R, C), x.dtype, ANY)],
        [blocks(N), blocks(N), blocks(N - 1), blocks(N - 1)]
        + [DMA((parts * (N - 1),)), DMA((parts * (N - 1),)), DMA((parts * N,)), DMA((parts * N,))]
        + [DMA((parts * (H - 1),)), DMA((parts * (H - 1),)), DMA((parts * N,)), DMA((parts,))],
        run,
    )


def all_sum(x, S, H, cid):
    def body(x_ref, o_ref, first, middle, second, sends, recvs, zsends, zrecvs):
        s, h = lax.axis_index("seq"), lax.axis_index("head")
        peers = [{"seq": lax.rem(s + k, S)} for k in range(1, S)]
        heads = [{"head": lax.rem(h + k, H)} for k in range(1, H)]
        barrier = pltpu.get_barrier_semaphore()
        for target in peers + heads:
            pl.semaphore_signal(barrier, inc=1, device_id=target, device_id_type=MESH)
        pl.semaphore_wait(barrier, S + H - 2)
        copies = [push(x_ref, first.at[s], sends, recvs, k, peers[k]) for k in range(S - 1)]
        first[s] = x_ref[...]
        for copy in copies:
            copy.wait()
        total = first[0]
        for k in range(1, S):
            total = total + first[k]
        middle[...] = total
        copies = [push(middle, second.at[h], zsends, zrecvs, k, heads[k]) for k in range(H - 1)]
        second[h] = total
        for copy in copies:
            copy.wait()
        total = second[0]
        for k in range(1, H):
            total = total + second[k]
        o_ref[...] = total

    return pl.pallas_call(
        body,
        out_shape=jax.ShapeDtypeStruct(x.shape, x.dtype),
        in_specs=[WHOLE],
        out_specs=WHOLE,
        scratch_shapes=[
            pltpu.VMEM((S,) + x.shape, x.dtype),
            pltpu.VMEM(x.shape, x.dtype),
            pltpu.VMEM((H,) + x.shape, x.dtype),
            DMA((S - 1,)),
            DMA((S - 1,)),
            DMA((H - 1,)),
            DMA((H - 1,)),
        ],
        compiler_params=pltpu.CompilerParams(collective_id=cid, has_side_effects=True),
        name="all_sum",
    )(x)


def late(task, turns):
    before = task.run

    def run(here, ins, outs, held):
        live = before(here, ins, outs, held)
        next(live)
        for _ in range(turns + 1):
            yield
        yield from live

    task.run = run
    return task


def tile_of(count, most):
    fits = [d for d in range(16, most + 1, 16) if count % d == 0]
    return max(fits) if fits else count


def table_grad(embedding, finals, logs, targets, scales, head, H, most=400, slots=768, unroll=1):
    V, D = embedding.shape
    R = finals[0].shape[0]
    Q = D // H
    tile = tile_of(V, most)
    count = R // slots

    def body(head_ref, e_ref, *refs):
        rows, columns = refs[:H], refs[H : 2 * H]
        log_ref, target_ref, scale_ref, o_ref = refs[2 * H :]
        table = e_ref[...]
        first = pl.program_id(0) * tile
        ids = first + lax.broadcasted_iota(jnp.int32, (tile, slots), 0)
        o_ref[...] = jnp.zeros((tile, Q), jnp.float32)
        for k in range(H):

            def chunk(i, carry, k=k):
                at = pl.ds(pl.multiple_of(i * slots, slots), slots)
                logits = lax.dot_general(
                    table, rows[k][at, :], (((1,), (1,)), ((), ())), preferred_element_type=jnp.float32
                )
                place = k * count + i
                grads = jnp.exp(logits - log_ref[place]) - (ids == target_ref[place]).astype(jnp.float32)
                grads = (grads * scale_ref[place]).astype(jnp.bfloat16)
                o_ref[...] += jnp.dot(grads, columns[k][at, :], preferred_element_type=jnp.float32)
                return carry

            lax.fori_loop(0, count, chunk, 0, unroll=unroll)

    fixed = pl.Buffered(1)
    whole = lambda shape: pl.BlockSpec(shape, lambda t, head_ref: (0,) * len(shape), pipeline_mode=fixed)
    shaped = lambda value: value.reshape(H * count, 1, slots)
    return pl.pallas_call(
        body,
        out_shape=jax.ShapeDtypeStruct((V, Q), jnp.float32),
        grid_spec=pltpu.PrefetchScalarGridSpec(
            num_scalar_prefetch=1,
            grid=(V // tile,),
            in_specs=[pl.BlockSpec((tile, D), lambda t, head_ref: (t, 0))]
            + [whole((R, D))] * H
            + [pl.BlockSpec((R, Q), lambda t, head_ref: (0, head_ref[0]), pipeline_mode=fixed)] * H
            + [whole((H * count, 1, slots))] * 3,
            out_specs=pl.BlockSpec((tile, Q), lambda t, head_ref: (t, 0)),
        ),
        compiler_params=pltpu.CompilerParams(vmem_limit_bytes=56 * 2**20),
        cost_estimate=pl.CostEstimate(
            flops=2 * V * H * R * (D + Q), bytes_accessed=V * D * 2 + V * Q * 4 + H * R * D * 2, transcendentals=V * H * R
        ),
        name="table_grad",
    )(head.reshape(1), embedding, *finals, *finals, shaped(logs), shaped(targets), shaped(scales))


KD = 256
VD = 512
STEP = 10

NORM_EPS = 1e-05
BETA_ONE = 0.9
BETA_TWO = 0.999
ADAM_EPS = 1e-08
DECAY_WT = 0.01
LEARN_RATE = 0.2
TRUST_EPSILON = 1e-06


def contract_dims(left_side, right_side, left_dim, right_dim):
    return lax.dot_general(
        left_side,
        right_side,
        (((left_dim,), (right_dim,)), ((), ())),
        preferred_element_type=jnp.float32,
    )


def matmul(left_side, right_side):
    return jnp.dot(left_side, right_side, preferred_element_type=jnp.float32)


def centre(values):
    centred = values - jnp.mean(values, axis=-1, keepdims=True)
    return centred * lax.rsqrt(jnp.mean(centred * centred, axis=-1, keepdims=True) + NORM_EPS)


def row_scale(values):
    centred = values - jnp.mean(values, axis=-1, keepdims=True)
    return lax.rsqrt(jnp.mean(centred * centred, axis=-1, keepdims=True) + NORM_EPS)


def norm_back(values, gain_row, grad):
    hat, scale = centre(values), row_scale(values)
    scaled = grad * gain_row
    mean_one = jnp.mean(scaled, axis=-1, keepdims=True)
    mean_two = jnp.mean(scaled * hat, axis=-1, keepdims=True)
    return scale * (scaled - mean_one - hat * mean_two), jnp.sum(grad * hat, axis=0)


def rotary_tables(positions):
    halfway = KD // 2
    frequency = jnp.exp(-jnp.log(10000.0) * jnp.arange(halfway).astype(jnp.float32) / halfway)
    phases = positions.astype(jnp.float32)[:, None] * frequency[None, :]
    return (jnp.cos(phases), jnp.sin(phases))


def rotate(values, cosines, sines):
    halfway = values.shape[-1] // 2
    leading = values[..., :halfway]
    trailing = values[..., halfway:]
    return jnp.concatenate(
        [leading * cosines - trailing * sines, leading * sines + trailing * cosines], axis=-1
    )


def rotate_back(grads, cosines, sines):
    return rotate(grads, cosines, -sines)


def gate_norm(gate_pre, retained):
    scaled = retained * lax.rsqrt(jnp.mean(retained * retained, axis=-1, keepdims=True) + NORM_EPS)
    return gate_pre * jax.nn.sigmoid(gate_pre) * scaled


def gelu_gate(gate_part, up_part):
    return jax.nn.gelu(gate_part) * up_part


def lamb_parts(weight, moment, second, grad):
    new_moment = BETA_ONE * moment + (1.0 - BETA_ONE) * grad
    new_second = BETA_TWO * second + (1.0 - BETA_TWO) * grad * grad
    moment_hat = new_moment / (1.0 - BETA_ONE**STEP)
    second_hat = new_second / (1.0 - BETA_TWO**STEP)
    ratio = moment_hat / (jnp.sqrt(second_hat) + ADAM_EPS) + DECAY_WT * weight
    return (new_moment, new_second, ratio)


def shift(value, axis, by):
    count = lax.axis_size(axis)
    return lax.ppermute(value, axis, [(i, (i + by) % count) for i in range(count)])


def head_gather(value):
    return jnp.concatenate([value] + [shift(value, "head", k) for k in range(1, lax.axis_size("head"))])


def head_sum(value):
    count = lax.axis_size("head")
    rows = value.shape[0] // count
    total = value[:rows].astype(jnp.float32)
    for k in range(1, count):
        at = (count - k) * rows
        total = total + shift(value[at : at + rows].astype(jnp.bfloat16), "head", k).astype(jnp.float32)
    return total


def local(
    token_ids,
    completion,
    decay_rate,
    w_mixer,
    w_output,
    w_expand,
    w_contract,
    norm_gains,
    embedding,
    mom_mixer,
    var_mixer,
    mom_output,
    var_output,
    mom_expand,
    var_expand,
    mom_contract,
    var_contract,
    mom_gains,
    var_gains,
    mom_embed,
    var_embed,
):
    bf, f32 = jnp.bfloat16, jnp.float32
    s, h = lax.axis_index("seq"), lax.axis_index("head")
    S, H = lax.axis_size("seq"), lax.axis_size("head")
    total_tokens = token_ids.shape[0]
    span = total_tokens // S
    vocab_part, width = embedding.shape
    quarter = width // H
    cap = span // 2
    own = cap // H
    rows_own = span // H
    assert w_mixer.shape[0] == 1
    token_start = s * span
    vocab_start = s * vocab_part

    def run(cid, name, *tasks):
        return [results[0] for results in fused(cid, S, H, tasks, name)]

    def flat(blocks):
        return blocks.reshape((-1,) + blocks.shape[2:])

    mixer = lax.all_gather(w_mixer[0], "seq", axis=0, tiled=True)
    output = lax.all_gather(w_output[0], "seq", axis=1, tiled=True)
    expand = lax.all_gather(w_expand[0], "seq", axis=0, tiled=True)
    contract = lax.all_gather(w_contract[0], "seq", axis=1, tiled=True)
    small = jnp.concatenate([norm_gains.astype(f32), mom_gains, var_gains], axis=0)
    small = jnp.concatenate([small, jnp.zeros((16 - small.shape[0], small.shape[1]), f32)], axis=0)

    ids_grid = token_ids.reshape(S, H, rows_own)
    ids_own = lax.dynamic_index_in_dim(ids_grid, h, 1, keepdims=False)
    chosen = ids_own.reshape(-1) - vocab_start
    inside = (chosen >= 0) & (chosen < vocab_part)
    found = jnp.take(embedding, jnp.clip(chosen, 0, vocab_part - 1), axis=0)
    found = jnp.where(inside[:, None], found, jnp.zeros((), bf))
    rows, small_all = run(
        1,
        "enter",
        lookup(found.reshape(S, rows_own, width), S, H, 4 if S <= 8 else 1),
        gather_seq(small, S),
    )
    x0 = flat(rows)
    small_all = small_all.transpose(1, 0, 2).reshape(16, width)
    gains, mom_gains_all, var_gains_all = small_all[:3], small_all[3:6], small_all[6:9]

    mask_own = lax.dynamic_slice_in_dim(completion, token_start, span)
    slot_of = jnp.where(mask_own == 1, jnp.cumsum(mask_own) - 1, -1)
    in_turn = jnp.arange(cap)
    in_turn = lax.rem(h - in_turn // own + H, H) * own + lax.rem(in_turn, own)
    at_slot = slot_of[None, :] == in_turn[:, None]
    picker = at_slot.astype(bf)
    place = jnp.sum(jnp.where(at_slot, jnp.arange(span)[None, :], 0), axis=1)
    mask_grid = completion.reshape(S, span)
    next_ids = jnp.roll(token_ids, -1).reshape(S, span)
    live = (completion * (jnp.arange(total_tokens) < total_tokens - 1)).reshape(S, span)
    slot_grid = jnp.where(mask_grid == 1, jnp.cumsum(mask_grid, axis=1) - 1, -1)
    matches = slot_grid[:, None, :] == jnp.arange(cap)[None, :, None]
    targets = jnp.sum(jnp.where(matches, next_ids[:, None, :], 0), axis=-1)
    row_weights = jnp.sum(jnp.where(matches, live[:, None, :], 0), axis=-1).astype(f32)
    count_live = jnp.sum(live).astype(f32)

    def of_quarter(grid, head):
        return lax.dynamic_index_in_dim(grid.reshape(S, H, own), head, 1, keepdims=False).reshape(-1)

    rate = decay_rate[0, 0]
    steps_in = jnp.arange(span).astype(f32)
    offsets = place[:, None].astype(f32) - steps_in[None, :]
    within = jnp.where(offsets >= 0, jnp.exp(-rate * jnp.maximum(offsets, 0.0)), 0.0)
    tail_decay = jnp.exp(-rate * (span - 1.0 - steps_in))[:, None]
    lead_decay = jnp.exp(-rate * (place.astype(f32) + 1.0))[:, None]
    cosines, sines = rotary_tables(token_start + jnp.arange(span))
    cosines_q, sines_q = rotary_tables(token_start + place)

    def state_sum(everyone, backward):
        position = jnp.arange(S)
        gap = position - s - 1 if backward else s - 1 - position
        factor = jnp.where(gap >= 0, jnp.exp(-rate * span * jnp.maximum(gap, 0).astype(f32)), 0.0)
        return jnp.sum(everyone.astype(f32) * factor[:, None, None], axis=0).astype(bf)

    hat0 = centre(x0.astype(f32))
    normed = (hat0 * gains[0]).astype(bf)
    proj_kv = matmul(normed, mixer[:, KD : 2 * KD + VD])
    keys = (rotate(proj_kv[:, :KD], cosines, sines) * KD ** (-0.5)).astype(bf)
    values = proj_kv[:, KD:].astype(bf)
    weighted = (keys.astype(f32) * tail_decay).astype(bf)
    update = contract_dims(weighted, values, 0, 0)
    state = state_sum(run(2, "states", gather_seq(update.astype(bf), S))[0], False)
    normed_q = matmul(picker, normed).astype(bf)
    query = rotate(matmul(normed_q, mixer[:, :KD]), cosines_q, sines_q).astype(bf)
    gate_pre = matmul(normed_q, mixer[:, 2 * KD + VD :])
    scores = contract_dims(query, keys, 1, 1)
    weights_blk = (scores * within).astype(bf)
    inner_part = matmul(weights_blk, values)
    retained = inner_part + lead_decay * matmul(query, state)
    gated = gate_norm(gate_pre, retained).astype(bf)

    x1 = matmul(picker[:own], x0) + head_sum(matmul(gated, output))
    normed_b_own = (centre(x1) * gains[1]).astype(bf)
    normed_b = head_gather(normed_b_own)
    gate_up = matmul(normed_b, expand)
    width_ff = gate_up.shape[1] // 2
    hidden = gelu_gate(gate_up[:, :width_ff], gate_up[:, width_ff:]).astype(bf)
    x2 = x1 + head_sum(matmul(hidden, contract))
    final_own = (centre(x2) * gains[2]).astype(bf)

    final_rows = flat(run(6, "final", gather_seq(final_own, S))[0])
    final_rows, final_own = lax.optimization_barrier((final_rows, final_own))
    pieces = jnp.concatenate([shift(final_own, "head", k) for k in range(1, H)])
    logits = contract_dims(final_rows, embedding, 1, 1)
    peak = jnp.max(logits, axis=-1)
    exp_total = jnp.sum(jnp.exp(logits - peak[:, None]), axis=-1)
    stats = run(7, "stats", gather_seq(jnp.stack([peak, exp_total]).reshape(-1, 128), S))[0].reshape(S, 2, S * own)
    peak_all = jnp.max(stats[:, 0], axis=0)
    total_all = jnp.sum(stats[:, 1] * jnp.exp(stats[:, 0] - peak_all), axis=0)
    log_total = peak_all + jnp.log(total_all)

    def logits_grad(logits, log_total, head):
        scale = of_quarter(row_weights, head) / count_live
        local_target = of_quarter(targets, head) - vocab_start
        hit = jnp.arange(vocab_part)[None, :] == local_target[:, None]
        grads = jnp.exp(logits - log_total[:, None]) - hit.astype(f32)
        return (grads * scale[:, None]).astype(bf), hit, scale

    grad_logits, hit, scale_row = logits_grad(logits, log_total, h)
    target_logit = jnp.sum(jnp.where(hit, logits, 0.0), axis=-1)
    shard_loss = jnp.sum(scale_row * log_total) * (s == 0).astype(f32) - jnp.sum(
        scale_row * target_logit
    )
    grad_rows = matmul(grad_logits, embedding).astype(bf)
    grad_rows, pieces = lax.optimization_barrier((grad_rows, pieces))
    grad_final = run(8, "logits_back", sum_seq(grad_rows.reshape(S, own, width), S))[0]
    grad_x2, grad_gain_final = norm_back(x2, gains[2], grad_final)

    pieces, grad_final = lax.optimization_barrier((pieces, grad_final))
    pieces = jnp.stack([pieces] + [shift(pieces, "seq", 2 * k) for k in range(1, S // 2)])
    chips = 2 * jnp.arange(S // 2)
    from_seq = jnp.concatenate([lax.rem(s - chips + S, S), lax.rem(s + 1 - 2 * lax.rem(s, 2) - chips + S, S)])

    grad_branch = head_gather(grad_x2.astype(bf))
    logs = jnp.stack([log_total] + [shift(log_total.reshape(-1, 128), "head", k).reshape(-1) for k in range(1, H)])
    logs = logs.reshape(H, S, own)
    grad_hidden = contract_dims(grad_branch, contract, 1, 1)
    grad_contract = contract_dims(hidden, grad_branch, 0, 0)
    _, gelu_back = jax.vjp(gelu_gate, gate_up[:, :width_ff], gate_up[:, width_ff:])
    grad_gate_up = jnp.concatenate(gelu_back(grad_hidden), axis=1).astype(bf)
    grad_expand = contract_dims(normed_b, grad_gate_up, 0, 0)
    grad_normed_b = head_sum(contract_dims(grad_gate_up, expand, 1, 1))
    grad_normed_b, pieces = lax.optimization_barrier((grad_normed_b, pieces))
    other_pieces = lax.ppermute(pieces, "seq", [(i, i ^ 1) for i in range(S)])
    grad_x1, grad_gain_b = norm_back(x1, gains[1], grad_normed_b)
    grad_x1 = grad_x1 + grad_x2
    grad_attn = head_gather(grad_x1.astype(bf))
    grad_attn, other_pieces = lax.optimization_barrier((grad_attn, other_pieces))
    pieces = jnp.concatenate([pieces, other_pieces])
    pieces = pieces.reshape(S, H - 1, own, width).transpose(1, 0, 2, 3).reshape(H - 1, S * own, width)
    grad_gated = contract_dims(grad_attn, output, 1, 1)
    grad_output = contract_dims(gated, grad_attn, 0, 0)
    _, gate_back = jax.vjp(gate_norm, gate_pre, retained)
    grad_gate_pre, grad_ret = gate_back(grad_gated)
    grad_cross = (lead_decay * grad_ret).astype(bf)
    grad_ret = grad_ret.astype(bf)
    grad_state = contract_dims(query, grad_cross, 0, 0)
    grad_update = state_sum(run(12, "states_back", gather_seq(grad_state.astype(bf), S))[0], True)
    grad_weights = contract_dims(grad_ret, values, 1, 1)
    grad_scores = (grad_weights * within).astype(bf)
    grad_query = matmul(grad_scores, keys) + contract_dims(grad_cross, state, 1, 1)
    grad_keys = contract_dims(grad_scores, query, 0, 0)
    grad_values = contract_dims(weights_blk, grad_ret, 0, 0) + matmul(weighted, grad_update)
    grad_keys = grad_keys + contract_dims(values, grad_update, 1, 1) * tail_decay
    grad_q_pre = rotate_back(grad_query, cosines_q, sines_q).astype(bf)
    grad_k_pre = rotate_back(grad_keys * KD ** (-0.5), cosines, sines).astype(bf)
    grad_qg = contract_dims(
        picker, jnp.concatenate([grad_q_pre, grad_gate_pre.astype(bf)], axis=1), 0, 0
    ).astype(bf)
    grad_proj = jnp.concatenate(
        [grad_qg[:, :KD], grad_k_pre, grad_values.astype(bf), grad_qg[:, KD:]], axis=1
    )
    grad_normed = contract_dims(grad_proj, mixer, 1, 1)
    grad_mixer = contract_dims(normed, grad_proj, 0, 0)

    def own_columns(value):
        return lax.dynamic_slice_in_dim(value, h * quarter, quarter, 1)

    scaled = grad_normed * gains[0]
    row_sums = jnp.stack([jnp.sum(scaled, axis=1), jnp.sum(scaled * hat0, axis=1)]).reshape(-1, 128)
    back = lax.rem(h - jnp.arange(H) + H, H)
    numbers = jnp.stack([targets.astype(f32), row_weights]).reshape(2, S, H, own).transpose(2, 0, 1, 3)
    numbers = jnp.concatenate([jnp.take(numbers, back, axis=0), logs[:, None]], axis=1)
    numbers = jnp.concatenate([numbers[:1], jnp.take(numbers[1:], from_seq, axis=2)]).reshape(H, 3, S * own)
    aims = numbers[:, 0].astype(jnp.int32) - vocab_start
    scales = numbers[:, 1] / count_live
    logs = numbers[:, 2]
    sent = grad_normed.astype(bf)
    sent, row_sums, logs = lax.optimization_barrier((sent, row_sums, logs))
    column_parts, sum_parts = [own_columns(sent)], [row_sums]
    for k in range(1, H):
        part = lax.dynamic_slice_in_dim(sent, lax.rem(h + k, H) * quarter, quarter, 1)
        column_parts.append(shift(part, "head", k))
        sum_parts.append(shift(row_sums, "head", k))
    grad_table = table_grad(
        embedding, [final_rows] + [pieces[k] for k in range(H - 1)], logs, aims, scales, h, H
    )
    column_parts, sum_parts, grad_table = lax.optimization_barrier((column_parts, sum_parts, grad_table))
    columns = sum(part.astype(f32) for part in column_parts)
    row_sums = sum(sum_parts).reshape(2, span, 1) / width
    hat_cols = own_columns(hat0)
    gain_cols = lax.dynamic_slice_in_dim(gains[0], h * quarter, quarter, 0)
    grad_gain_a = jnp.sum(columns * hat_cols, axis=0)
    grad_in = row_scale(x0.astype(f32)) * (columns * gain_cols - row_sums[0] - hat_cols * row_sums[1])
    grad_in = grad_in + contract_dims(picker, own_columns(grad_attn), 0, 0)
    piece_rows = flat(run(14, "rows", gather_seq(grad_in.astype(bf), S))[0])
    local_id = token_ids - vocab_start
    one_hot = (jnp.arange(vocab_part)[:, None] == local_id[None, :]).astype(bf)
    grad_table = grad_table + matmul(one_hot, piece_rows)

    def scattered(value, dim):
        return lax.psum_scatter(value.astype(bf), "seq", scatter_dimension=dim, tiled=True).astype(f32)[None]

    grad_contract = scattered(grad_contract, 1)
    grad_expand = scattered(grad_expand, 0)
    grad_output = scattered(grad_output, 1)
    grad_mixer = scattered(grad_mixer, 0)
    grad_gains = jnp.stack(
        [lax.dynamic_update_slice_in_dim(jnp.zeros((width,), f32), grad_gain_a, h * quarter, 0), grad_gain_b, grad_gain_final]
    )

    mixer_f = w_mixer.astype(f32)
    output_f = w_output.astype(f32)
    expand_f = w_expand.astype(f32)
    contract_f = w_contract.astype(f32)
    table_own = own_columns(embedding).astype(f32)
    parts = [
        lamb_parts(mixer_f, mom_mixer, var_mixer, grad_mixer),
        lamb_parts(output_f, mom_output, var_output, grad_output),
        lamb_parts(expand_f, mom_expand, var_expand, grad_expand),
        lamb_parts(contract_f, mom_contract, var_contract, grad_contract),
        lamb_parts(table_own, mom_embed, var_embed, grad_table),
    ]
    held = [mixer_f, output_f, expand_f, contract_f, table_own]
    sums = [jnp.sum(w * w) for w in held] + [jnp.sum(p[2] * p[2]) for p in parts] + [shard_loss]
    lane = lax.broadcasted_iota(jnp.int32, (8, 128), 1)
    packed = jnp.zeros((8, 128), f32)
    for i, value in enumerate(sums):
        packed = packed + jnp.where(lane == i, value, 0.0)
    packed = jnp.concatenate([packed, grad_gains.reshape(-1, 128)])
    packed = all_sum(packed, S, H, 15)
    sums = packed[0]
    grad_gains = packed[8:].reshape(3, width)
    part_gains = lamb_parts(gains, mom_gains_all, var_gains_all, grad_gains)
    weight_squares = jnp.concatenate([sums[:5], jnp.sum(gains * gains, axis=1)])
    ratio_squares = jnp.concatenate([sums[5:10], jnp.sum(part_gains[2] * part_gains[2], axis=1)])
    trust = jnp.sqrt(weight_squares) * lax.rsqrt(ratio_squares + TRUST_EPSILON)
    new_w = [w - LEARN_RATE * trust[i] * parts[i][2] for i, w in enumerate(held)]
    new_gains = gains - LEARN_RATE * trust[5:][:, None] * part_gains[2]

    def own_gains(value):
        return lax.dynamic_slice_in_dim(value, s * (width // S), width // S, 1)

    return (
        sums[10],
        jnp.stack([weight_squares, ratio_squares], axis=1),
        parts[0][0],
        parts[0][1],
        new_w[0],
        parts[1][0],
        parts[1][1],
        new_w[1],
        parts[2][0],
        parts[2][1],
        new_w[2],
        parts[3][0],
        parts[3][1],
        new_w[3],
        own_gains(part_gains[0]),
        own_gains(part_gains[1]),
        own_gains(new_gains),
        parts[4][0],
        parts[4][1],
        new_w[4],
    )


def solution(mesh):
    placed = (
        P(),
        P(),
        P(None, "head"),
        P(None, "seq", "head"),
        P(None, "head", "seq"),
        P(None, "seq", "head"),
        P(None, "head", "seq"),
        P(None, "seq"),
        P("seq", None),
        P(None, "seq", "head"),
        P(None, "seq", "head"),
        P(None, "head", "seq"),
        P(None, "head", "seq"),
        P(None, "seq", "head"),
        P(None, "seq", "head"),
        P(None, "head", "seq"),
        P(None, "head", "seq"),
        P(None, "seq"),
        P(None, "seq"),
        P("seq", "head"),
        P("seq", "head"),
    )
    return jax.shard_map(
        local,
        mesh=mesh,
        in_specs=placed,
        out_specs=(P(), P()) + placed[3:4] * 3 + placed[4:5] * 3 + placed[3:4] * 3 + placed[4:5] * 3 + placed[7:8] * 3 + placed[19:20] * 3,
        check_vma=False,
    )
```

```python
import jax
import jax.numpy as jnp
from jax import lax
from jax.experimental import pallas as pl
from jax.experimental.pallas import tpu as pltpu
from jax.sharding import PartitionSpec as P

MESH = pl.DeviceIdType.MESH
ANY = pl.BlockSpec(memory_space=pl.ANY)
WHOLE = pl.BlockSpec(memory_space=pltpu.VMEM)
DMA = pltpu.SemaphoreType.DMA


def push(src, dst, sends, recvs, at, target):
    copy = pltpu.make_async_remote_copy(
        src_ref=src,
        dst_ref=dst,
        send_sem=sends.at[at],
        recv_sem=recvs.at[at],
        device_id=target,
        device_id_type=MESH,
    )
    copy.start()
    return copy


def fetch(src, dst, sems, at):
    copy = pltpu.make_async_copy(src, dst, sems.at[at])
    copy.start()
    return copy


def by_rows(count, step, body):
    def one(i, carry):
        body(pl.ds(pl.multiple_of(i * step, step), step))
        return carry

    lax.fori_loop(0, count // step, one, 0)


def row_step(rows):
    return 32 if rows % 32 == 0 else 16


class Here:
    def __init__(self, S, H):
        self.S, self.H, self.N = S, H, S // 2
        self.s, self.h = lax.axis_index("seq"), lax.axis_index("head")
        self.parity = lax.rem(self.s, 2)

    def head(self, k):
        return lax.rem(self.h + k, self.H)

    def seq(self, k):
        return lax.rem(self.s + 2 * k, self.S)

    def heads(self):
        return [{"head": self.head(k)} for k in range(1, self.H)]

    def chips(self):
        return [{"seq": self.seq(k)} for k in range(1, self.N)]

    def other(self):
        return {"seq": self.s + 1 - 2 * self.parity}


class Task:
    def __init__(self, axis, operands, outs, scratch, run):
        self.axis, self.operands, self.outs, self.scratch, self.run = axis, operands, outs, scratch, run


def fused(cid, S, H, tasks, name):
    operands, outs, specs, scratch = [], [], [], []
    for task in tasks:
        operands += task.operands
        for shape, dtype, spec in task.outs:
            outs.append(jax.ShapeDtypeStruct(shape, dtype))
            specs.append(spec)
        scratch += task.scratch

    def body(*refs):
        here = Here(S, H)
        ins, rest = refs[: len(operands)], refs[len(operands) :]
        results, held = rest[: len(outs)], rest[len(outs) :]
        live = []
        for task in tasks:
            live.append(
                task.run(here, ins[: len(task.operands)], results[: len(task.outs)], held[: len(task.scratch)])
            )
            ins, results, held = ins[len(task.operands) :], results[len(task.outs) :], held[len(task.scratch) :]
        axes = {task.axis for task in tasks}
        targets = []
        if axes & {"head", "both"}:
            targets += here.heads()
        if axes & {"seq", "both"}:
            targets += here.chips() + [here.other()]
        barrier = pltpu.get_barrier_semaphore()
        for target in targets:
            pl.semaphore_signal(barrier, inc=1, device_id=target, device_id_type=MESH)
        for run in live:
            next(run)
        pl.semaphore_wait(barrier, len(targets))
        while live:
            live = [run for run in live if next(run, "end") != "end"]

    got = pl.pallas_call(
        body,
        out_shape=outs,
        in_specs=[ANY] * len(operands),
        out_specs=specs,
        scratch_shapes=scratch,
        compiler_params=pltpu.CompilerParams(
            collective_id=cid, has_side_effects=True, vmem_limit_bytes=56 * 2**20
        ),
        cost_estimate=pl.CostEstimate(flops=0, bytes_accessed=2**25, transcendentals=0),
        name=name,
    )(*operands)
    split = []
    for task in tasks:
        split.append(got[: len(task.outs)])
        got = got[len(task.outs) :]
    return split


def gather_head(x, H):
    def run(here, ins, outs, held):
        (src,), (dst,), (sends, recvs, own) = ins, outs, held
        mine = fetch(src, dst.at[here.h], own, 0)
        yield
        copies = [push(src, dst.at[here.h], sends, recvs, k, to) for k, to in enumerate(here.heads())]
        yield
        for copy in copies:
            copy.wait()
        mine.wait()

    return Task("head", [x], [((H,) + x.shape, x.dtype, ANY)], [DMA((H - 1,)), DMA((H - 1,)), DMA((1,))], run)


def sum_head(x, H, columns=False):
    R, C = (x.shape[0], x.shape[1] // H) if columns else x.shape[1:]

    def run(here, ins, outs, held):
        (src,), (dst,), (got, sends, recvs, own) = ins, outs, held

        def block(i):
            return src.at[:, pl.ds(pl.multiple_of(i * C, C), C)] if columns else src.at[i]

        mine = fetch(block(here.h), got.at[0], own, 0)
        yield
        copies = [
            push(block(here.head(k)), got.at[k], sends, recvs, k - 1, {"head": here.head(k)}) for k in range(1, H)
        ]
        yield
        mine.wait()
        for copy in copies:
            copy.wait()

        def add(rows):
            total = got[0, rows, :].astype(jnp.float32)
            for k in range(1, H):
                total = total + got[k, rows, :].astype(jnp.float32)
            dst[rows, :] = total

        by_rows(R, row_step(R), add)

    return Task(
        "head",
        [x],
        [((R, C), jnp.float32, WHOLE)],
        [pltpu.VMEM((H, R, C), x.dtype), DMA((H - 1,)), DMA((H - 1,)), DMA((1,))],
        run,
    )


def gather_seq(x, S, columns=False, ahead=None):
    N = S // 2
    R, C = x.shape[-2:]

    def run(here, ins, outs, held):
        (src,), (dst,), (sends, recvs, fsends, frecvs, own) = ins, outs, held
        if ahead is not None:
            src = src.at[here.head(ahead)]

        def block(i):
            return dst.at[:, pl.ds(pl.multiple_of(i * C, C), C)] if columns else dst.at[i]

        mine = fetch(src, block(here.s), own, 0)
        yield
        copies = [push(src, block(here.s), sends, recvs, k, to) for k, to in enumerate(here.chips() + [here.other()])]
        passed = []
        for k in range(1, N):
            yield
            copies[k - 1].wait_recv()
            source = lax.rem(here.s - 2 * k + 2 * S, S)
            passed.append(push(block(source), block(source), fsends, frecvs, k - 1, here.other()))
        yield
        copies[N - 1].wait_recv()
        for copy in copies:
            copy.wait_send()
        for copy in passed:
            copy.wait()
        mine.wait()

    shape = (R, S * C) if columns else (S, R, C)
    return Task(
        "seq", [x], [(shape, x.dtype, ANY)], [DMA((N,)), DMA((N,)), DMA((N - 1,)), DMA((N - 1,)), DMA((1,))], run
    )


def sum_seq(x, S, columns=False):
    N = S // 2
    R, C = (x.shape[0], x.shape[1] // S) if columns else x.shape[1:]
    order = list(range(1, N)) + [0]

    def run(here, ins, outs, held):
        (src,), (dst,) = ins, outs
        theirs, ours, out, got, sends, recvs, csends, crecvs, own = held

        def block(i):
            return src.at[:, pl.ds(pl.multiple_of(i * C, C), C)] if columns else src.at[i]

        mine = {k: fetch(block(here.seq(k)), ours.at[k], own, k) for k in order}
        yield
        swaps = {
            k: push(block(here.seq(k) + 1 - 2 * here.parity), theirs.at[k], csends, crecvs, k, here.other())
            for k in order
        }
        copies = []
        for k in order:
            yield
            mine[k].wait()
            swaps[k].wait_recv()

            def add(rows, k=k):
                total = ours[k, rows, :].astype(jnp.float32) + theirs[k, rows, :].astype(jnp.float32)
                if k == 0:
                    dst[rows, :] = total
                else:
                    out[k - 1, rows, :] = total.astype(x.dtype)

            by_rows(R, row_step(R), add)
            if k > 0:
                copies.append(push(out.at[k - 1], got.at[k - 1], sends, recvs, k - 1, {"seq": here.seq(k)}))
        yield
        for copy in copies:
            copy.wait()
        for k in order:
            swaps[k].wait_send()

        def total(rows):
            value = dst[rows, :]
            for k in range(N - 1):
                value = value + got[k, rows, :].astype(jnp.float32)
            dst[rows, :] = value

        by_rows(R, row_step(R), total)

    blocks = lambda count: pltpu.VMEM((count, R, C), x.dtype)
    return Task(
        "seq",
        [x],
        [((R, C), jnp.float32, WHOLE)],
        [blocks(N), blocks(N), blocks(N - 1), blocks(N - 1)]
        + [DMA((N - 1,)), DMA((N - 1,)), DMA((N,)), DMA((N,)), DMA((N,))],
        run,
    )


def lookup(x, S, H, parts):
    N = S // 2
    R, C = x.shape[1:]
    piece = R // parts
    order = list(range(1, N)) + [0]

    def run(here, ins, outs, held):
        (src,), (dst,) = ins, outs
        theirs, ours, out, got, sends, recvs, csends, crecvs, zsends, zrecvs, own, left = held
        mine, swaps, copies, spread, kept = {}, {}, {}, [], []
        for q in range(parts):
            rows = pl.ds(q * piece, piece)
            for k in order:
                mine[q, k] = fetch(src.at[here.seq(k), rows], ours.at[k, rows], own, q * N + k)
        yield
        for q in range(parts):
            rows = pl.ds(q * piece, piece)
            for k in order:
                swaps[q, k] = push(
                    src.at[here.seq(k) + 1 - 2 * here.parity, rows],
                    theirs.at[k, rows],
                    csends,
                    crecvs,
                    q * N + k,
                    here.other(),
                )

        def first(q):
            for k in order:
                mine[q, k].wait()
                swaps[q, k].wait_recv()
                for at in range(q * piece, (q + 1) * piece, 16):
                    rows = pl.ds(at, 16)
                    total = ours[k, rows, :] + theirs[k, rows, :]
                    if k == 0:
                        ours[k, rows, :] = total
                    else:
                        out[k - 1, rows, :] = total
                if k > 0:
                    rows = pl.ds(q * piece, piece)
                    copies[q, k] = push(
                        out.at[k - 1, rows],
                        got.at[k - 1, rows],
                        sends,
                        recvs,
                        q * (N - 1) + k - 1,
                        {"seq": here.seq(k)},
                    )

        def second(q):
            for k in range(1, N):
                copies[q, k].wait_recv()
            for at in range(q * piece, (q + 1) * piece, 16):
                rows = pl.ds(at, 16)
                total = ours[0, rows, :]
                for k in range(1, N):
                    total = total + got[k - 1, rows, :]
                ours[0, rows, :] = total
            rows = pl.ds(q * piece, piece)
            kept.append(fetch(ours.at[0, rows], dst.at[here.h, rows], left, q))
            for k in range(1, H):
                spread.append(
                    push(
                        ours.at[0, rows],
                        dst.at[here.h, rows],
                        zsends,
                        zrecvs,
                        q * (H - 1) + k - 1,
                        {"head": here.head(k)},
                    )
                )

        for q in range(parts):
            first(q)
            yield
            if q > 0:
                second(q - 1)
        second(parts - 1)
        yield
        for copy in spread:
            copy.wait()
        for copy in kept:
            copy.wait()
        for q in range(parts):
            for k in order:
                swaps[q, k].wait_send()
                if k > 0:
                    copies[q, k].wait_send()

    blocks = lambda count: pltpu.VMEM((count, R, C), x.dtype)
    return Task(
        "both",
        [x],
        [((H, R, C), x.dtype, ANY)],
        [blocks(N), blocks(N), blocks(N - 1), blocks(N - 1)]
        + [DMA((parts * (N - 1),)), DMA((parts * (N - 1),)), DMA((parts * N,)), DMA((parts * N,))]
        + [DMA((parts * (H - 1),)), DMA((parts * (H - 1),)), DMA((parts * N,)), DMA((parts,))],
        run,
    )


def finish(vectors, grad_gains, state, S, H, cid):
    count = len(vectors)
    groups = (count - 1) // 2
    gain_rows = grad_gains.shape[0] // 3
    first_gain = 16
    rows = first_gain + 3 * gain_rows

    def body(*refs):
        ins, grads_ref, state_ref = refs[:count], refs[count], refs[count + 1]
        loss_ref, square_ref, trust_ref, m_ref, v_ref, w_ref = refs[count + 2 : count + 8]
        packed, first, middle, second, sends, recvs, zsends, zrecvs = refs[count + 8 :]
        s, h = lax.axis_index("seq"), lax.axis_index("head")
        peers = [{"seq": lax.rem(s + k, S)} for k in range(1, S)]
        heads = [{"head": lax.rem(h + k, H)} for k in range(1, H)]
        packed[pl.ds(0, first_gain), :] = jnp.zeros((first_gain, 128), jnp.float32)
        for i in range(count):
            packed[pl.ds(i, 1), :] = ins[i][...]
        packed[pl.ds(first_gain, 3 * gain_rows), :] = grads_ref[...]
        barrier = pltpu.get_barrier_semaphore()
        for target in peers + heads:
            pl.semaphore_signal(barrier, inc=1, device_id=target, device_id_type=MESH)
        first[s] = packed[...]
        pl.semaphore_wait(barrier, S + H - 2)
        copies = [push(packed, first.at[s], sends, recvs, k, peers[k]) for k in range(S - 1)]
        for copy in copies:
            copy.wait()
        total = first[0]
        for k in range(1, S):
            total = total + first[k]
        middle[...] = total
        second[h] = total
        copies = [push(middle, second.at[h], zsends, zrecvs, k, heads[k]) for k in range(H - 1)]
        for copy in copies:
            copy.wait()
        total = second[0]
        for k in range(1, H):
            total = total + second[k]
        middle[...] = total

        def group_sum(value):
            return jnp.sum(jnp.sum(value, axis=1, keepdims=True), axis=0, keepdims=True)

        lane = lax.broadcasted_iota(jnp.int32, (1, 128), 1)
        weights = [group_sum(middle[pl.ds(i, 1), :]) for i in range(groups)]
        ratios = [group_sum(middle[pl.ds(groups + i, 1), :]) for i in range(groups)]
        loss_ref[...] = jnp.broadcast_to(group_sum(middle[pl.ds(2 * groups, 1), :]), (1, 128))
        parts = []
        for g in range(3):
            at = pl.ds(g * gain_rows, gain_rows)
            weight = state_ref[0, at, :]
            grad = middle[pl.ds(first_gain + g * gain_rows, gain_rows), :]
            part = lamb_parts(weight, state_ref[1, at, :], state_ref[2, at, :], grad)
            weights.append(group_sum(weight * weight))
            ratios.append(group_sum(part[2] * part[2]))
            parts.append((at, weight, part))
        for i in range(groups + 3):
            trust = jnp.sqrt(weights[i]) * lax.rsqrt(ratios[i] + TRUST_EPSILON)
            square_ref[pl.ds(i, 1), :] = jnp.where(lane == 0, weights[i], ratios[i])
            trust_ref[pl.ds(i, 1), :] = jnp.broadcast_to(trust, (1, 128))
            if i >= groups:
                at, weight, part = parts[i - groups]
                m_ref[at, :], v_ref[at, :] = part[0], part[1]
                w_ref[at, :] = weight - LEARN_RATE * trust * part[2]

    shapes = [(1, 128), (groups + 3, 128), (groups + 3, 128)] + [grad_gains.shape] * 3
    return pl.pallas_call(
        body,
        out_shape=[jax.ShapeDtypeStruct(shape, jnp.float32) for shape in shapes],
        in_specs=[WHOLE] * (count + 2),
        out_specs=[WHOLE] * len(shapes),
        scratch_shapes=[
            pltpu.VMEM((rows, 128), jnp.float32),
            pltpu.VMEM((S, rows, 128), jnp.float32),
            pltpu.VMEM((rows, 128), jnp.float32),
            pltpu.VMEM((H, rows, 128), jnp.float32),
            DMA((S - 1,)),
            DMA((S - 1,)),
            DMA((H - 1,)),
            DMA((H - 1,)),
        ],
        compiler_params=pltpu.CompilerParams(collective_id=cid, has_side_effects=True),
        name="finish",
    )(*vectors, grad_gains, state)


def late(task, turns):
    before = task.run

    def run(here, ins, outs, held):
        live = before(here, ins, outs, held)
        next(live)
        for _ in range(turns + 1):
            yield
        yield from live

    task.run = run
    return task


def tile_of(count, most):
    fits = [d for d in range(16, most + 1, 16) if count % d == 0]
    return max(fits) if fits else count


def table_grad(embedding, finals, logs, targets, scales, head, H, base=None, most=400, slots=768):
    V, D = embedding.shape
    pieces = len(finals)
    R = finals[0].shape[0]
    Q = D // H
    tile = tile_of(V, most)
    count = R // slots

    def body(head_ref, e_ref, *refs):
        rows, columns = refs[:pieces], refs[pieces : 2 * pieces]
        log_ref, target_ref, scale_ref = refs[2 * pieces : 2 * pieces + 3]
        o_ref = refs[-1]
        table = e_ref[...]
        first = pl.program_id(0) * tile
        ids = first + lax.broadcasted_iota(jnp.int32, (tile, slots), 0)
        o_ref[...] = jnp.zeros((tile, Q), jnp.float32) if base is None else refs[-2][...]
        for k in range(pieces):

            def chunk(i, carry, k=k):
                at = pl.ds(pl.multiple_of(i * slots, slots), slots)
                logits = lax.dot_general(
                    table, rows[k][at, :], (((1,), (1,)), ((), ())), preferred_element_type=jnp.float32
                )
                place = k * count + i
                grads = jnp.exp(logits - log_ref[place]) - (ids == target_ref[place]).astype(jnp.float32)
                grads = (grads * scale_ref[place]).astype(jnp.bfloat16)
                o_ref[...] += jnp.dot(grads, columns[k][at, :], preferred_element_type=jnp.float32)
                return carry

            lax.fori_loop(0, count, chunk, 0)

    fixed = pl.Buffered(1)
    whole = lambda shape: pl.BlockSpec(shape, lambda t, head_ref: (0,) * len(shape), pipeline_mode=fixed)
    shaped = lambda value: value.reshape(pieces * count, 1, slots)
    extra = [] if base is None else [base]
    return pl.pallas_call(
        body,
        out_shape=jax.ShapeDtypeStruct((V, Q), jnp.float32),
        grid_spec=pltpu.PrefetchScalarGridSpec(
            num_scalar_prefetch=1,
            grid=(V // tile,),
            in_specs=[pl.BlockSpec((tile, D), lambda t, head_ref: (t, 0))]
            + [whole((R, D))] * pieces
            + [pl.BlockSpec((R, Q), lambda t, head_ref: (0, head_ref[0]), pipeline_mode=fixed)] * pieces
            + [whole((pieces * count, 1, slots))] * 3
            + [pl.BlockSpec((tile, Q), lambda t, head_ref: (t, 0))] * len(extra),
            out_specs=pl.BlockSpec((tile, Q), lambda t, head_ref: (t, 0)),
        ),
        compiler_params=pltpu.CompilerParams(vmem_limit_bytes=56 * 2**20),
        cost_estimate=pl.CostEstimate(
            flops=2 * V * pieces * R * (D + Q), bytes_accessed=V * D * 2 + V * Q * 4 + pieces * R * D * 2, transcendentals=V * pieces * R
        ),
        name="table_grad",
    )(head.reshape(1), embedding, *finals, *finals, shaped(logs), shaped(targets), shaped(scales), *extra)


KD = 256
VD = 512
STEP = 10

NORM_EPS = 1e-05
BETA_ONE = 0.9
BETA_TWO = 0.999
ADAM_EPS = 1e-08
DECAY_WT = 0.01
LEARN_RATE = 0.2
TRUST_EPSILON = 1e-06


def contract_dims(left_side, right_side, left_dim, right_dim):
    return lax.dot_general(
        left_side,
        right_side,
        (((left_dim,), (right_dim,)), ((), ())),
        preferred_element_type=jnp.float32,
    )


def matmul(left_side, right_side):
    return jnp.dot(left_side, right_side, preferred_element_type=jnp.float32)


def centre(values):
    centred = values - jnp.mean(values, axis=-1, keepdims=True)
    return centred * lax.rsqrt(jnp.mean(centred * centred, axis=-1, keepdims=True) + NORM_EPS)


def row_scale(values):
    centred = values - jnp.mean(values, axis=-1, keepdims=True)
    return lax.rsqrt(jnp.mean(centred * centred, axis=-1, keepdims=True) + NORM_EPS)


def norm_back(values, gain_row, grad):
    hat, scale = centre(values), row_scale(values)
    scaled = grad * gain_row
    mean_one = jnp.mean(scaled, axis=-1, keepdims=True)
    mean_two = jnp.mean(scaled * hat, axis=-1, keepdims=True)
    return scale * (scaled - mean_one - hat * mean_two), jnp.sum(grad * hat, axis=0)


def rotary_tables(positions):
    halfway = KD // 2
    frequency = jnp.exp(-jnp.log(10000.0) * jnp.arange(halfway).astype(jnp.float32) / halfway)
    phases = positions.astype(jnp.float32)[:, None] * frequency[None, :]
    return (jnp.cos(phases), jnp.sin(phases))


def rotate(values, cosines, sines):
    halfway = values.shape[-1] // 2
    leading = values[..., :halfway]
    trailing = values[..., halfway:]
    return jnp.concatenate(
        [leading * cosines - trailing * sines, leading * sines + trailing * cosines], axis=-1
    )


def rotate_back(grads, cosines, sines):
    return rotate(grads, cosines, -sines)


def gate_norm(gate_pre, retained):
    scaled = retained * lax.rsqrt(jnp.mean(retained * retained, axis=-1, keepdims=True) + NORM_EPS)
    return gate_pre * jax.nn.sigmoid(gate_pre) * scaled


def gelu_gate(gate_part, up_part):
    return jax.nn.gelu(gate_part) * up_part


def lamb_parts(weight, moment, second, grad):
    new_moment = BETA_ONE * moment + (1.0 - BETA_ONE) * grad
    new_second = BETA_TWO * second + (1.0 - BETA_TWO) * grad * grad
    moment_hat = new_moment / (1.0 - BETA_ONE**STEP)
    second_hat = new_second / (1.0 - BETA_TWO**STEP)
    ratio = moment_hat / (jnp.sqrt(second_hat) + ADAM_EPS) + DECAY_WT * weight
    return (new_moment, new_second, ratio)


def shift(value, axis, by):
    count = lax.axis_size(axis)
    return lax.ppermute(value, axis, [(i, (i + by) % count) for i in range(count)])


def head_gather(value):
    return jnp.concatenate([value] + [shift(value, "head", k) for k in range(1, lax.axis_size("head"))])


def head_sum(value):
    count = lax.axis_size("head")
    rows = value.shape[0] // count
    total = value[:rows].astype(jnp.float32)
    for k in range(1, count):
        at = (count - k) * rows
        total = total + shift(value[at : at + rows].astype(jnp.bfloat16), "head", k).astype(jnp.float32)
    return total


def local(
    token_ids,
    completion,
    decay_rate,
    w_mixer,
    w_output,
    w_expand,
    w_contract,
    norm_gains,
    embedding,
    mom_mixer,
    var_mixer,
    mom_output,
    var_output,
    mom_expand,
    var_expand,
    mom_contract,
    var_contract,
    mom_gains,
    var_gains,
    mom_embed,
    var_embed,
):
    bf, f32 = jnp.bfloat16, jnp.float32
    s, h = lax.axis_index("seq"), lax.axis_index("head")
    S, H = lax.axis_size("seq"), lax.axis_size("head")
    total_tokens = token_ids.shape[0]
    span = total_tokens // S
    vocab_part, width = embedding.shape
    quarter = width // H
    cap = span // 2
    own = cap // H
    rows_own = span // H
    assert w_mixer.shape[0] == 1
    token_start = s * span
    vocab_start = s * vocab_part

    def run(cid, name, *tasks):
        return [results[0] for results in fused(cid, S, H, tasks, name)]

    def flat(blocks):
        return blocks.reshape((-1,) + blocks.shape[2:])

    mixer = lax.all_gather(w_mixer[0], "seq", axis=0, tiled=True)
    output = lax.all_gather(w_output[0], "seq", axis=1, tiled=True)
    expand = lax.all_gather(w_expand[0], "seq", axis=0, tiled=True)
    contract = lax.all_gather(w_contract[0], "seq", axis=1, tiled=True)
    small = jnp.concatenate([norm_gains.astype(f32), mom_gains, var_gains], axis=0)
    small = jnp.concatenate([small, jnp.zeros((16 - small.shape[0], small.shape[1]), f32)], axis=0)

    ids_grid = token_ids.reshape(S, H, rows_own)
    ids_own = lax.dynamic_index_in_dim(ids_grid, h, 1, keepdims=False)
    chosen = ids_own.reshape(-1) - vocab_start
    inside = (chosen >= 0) & (chosen < vocab_part)
    found = jnp.take(embedding, jnp.clip(chosen, 0, vocab_part - 1), axis=0)
    found = jnp.where(inside[:, None], found, jnp.zeros((), bf))
    rows, small_all = run(
        1,
        "enter",
        lookup(found.reshape(S, rows_own, width), S, H, 4 if S <= 8 else 1),
        gather_seq(small, S),
    )
    x0 = flat(rows)
    small_all = small_all.transpose(1, 0, 2).reshape(16, width)
    gains, mom_gains_all, var_gains_all = small_all[:3], small_all[3:6], small_all[6:9]

    mask_own = lax.dynamic_slice_in_dim(completion, token_start, span)
    slot_of = jnp.where(mask_own == 1, jnp.cumsum(mask_own) - 1, -1)
    in_turn = jnp.arange(cap)
    in_turn = lax.rem(h - in_turn // own + H, H) * own + lax.rem(in_turn, own)
    at_slot = slot_of[None, :] == in_turn[:, None]
    picker = at_slot.astype(bf)
    place = jnp.sum(jnp.where(at_slot, jnp.arange(span)[None, :], 0), axis=1)
    mask_grid = completion.reshape(S, span)
    next_ids = jnp.roll(token_ids, -1).reshape(S, span)
    live = (completion * (jnp.arange(total_tokens) < total_tokens - 1)).reshape(S, span)
    slot_grid = jnp.where(mask_grid == 1, jnp.cumsum(mask_grid, axis=1) - 1, -1)
    matches = slot_grid[:, None, :] == jnp.arange(cap)[None, :, None]
    targets = jnp.sum(jnp.where(matches, next_ids[:, None, :], 0), axis=-1)
    row_weights = jnp.sum(jnp.where(matches, live[:, None, :], 0), axis=-1).astype(f32)
    count_live = jnp.sum(live).astype(f32)

    def of_quarter(grid, head):
        return lax.dynamic_index_in_dim(grid.reshape(S, H, own), head, 1, keepdims=False).reshape(-1)

    rate = decay_rate[0, 0]
    steps_in = jnp.arange(span).astype(f32)
    offsets = place[:, None].astype(f32) - steps_in[None, :]
    within = jnp.where(offsets >= 0, jnp.exp(-rate * jnp.maximum(offsets, 0.0)), 0.0)
    tail_decay = jnp.exp(-rate * (span - 1.0 - steps_in))[:, None]
    lead_decay = jnp.exp(-rate * (place.astype(f32) + 1.0))[:, None]
    cosines, sines = rotary_tables(token_start + jnp.arange(span))
    cosines_q, sines_q = rotary_tables(token_start + place)

    def state_sum(everyone, backward):
        position = jnp.arange(S)
        gap = position - s - 1 if backward else s - 1 - position
        factor = jnp.where(gap >= 0, jnp.exp(-rate * span * jnp.maximum(gap, 0).astype(f32)), 0.0)
        return jnp.sum(everyone.astype(f32) * factor[:, None, None], axis=0).astype(bf)

    hat0 = centre(x0.astype(f32))
    normed = (hat0 * gains[0]).astype(bf)
    proj_kv = matmul(normed, mixer[:, KD : 2 * KD + VD])
    keys = (rotate(proj_kv[:, :KD], cosines, sines) * KD ** (-0.5)).astype(bf)
    values = proj_kv[:, KD:].astype(bf)
    weighted = (keys.astype(f32) * tail_decay).astype(bf)
    update = contract_dims(weighted, values, 0, 0)
    state = state_sum(run(2, "states", gather_seq(update.astype(bf), S))[0], False)
    normed_q = matmul(picker, normed).astype(bf)
    query = rotate(matmul(normed_q, mixer[:, :KD]), cosines_q, sines_q).astype(bf)
    gate_pre = matmul(normed_q, mixer[:, 2 * KD + VD :])
    scores = contract_dims(query, keys, 1, 1)
    weights_blk = (scores * within).astype(bf)
    inner_part = matmul(weights_blk, values)
    retained = inner_part + lead_decay * matmul(query, state)
    gated = gate_norm(gate_pre, retained).astype(bf)

    x1 = matmul(picker[:own], x0) + head_sum(matmul(gated, output))
    normed_b_own = (centre(x1) * gains[1]).astype(bf)
    normed_b = head_gather(normed_b_own)
    gate_up = matmul(normed_b, expand)
    width_ff = gate_up.shape[1] // 2
    hidden = gelu_gate(gate_up[:, :width_ff], gate_up[:, width_ff:]).astype(bf)
    x2 = x1 + head_sum(matmul(hidden, contract))
    final_own = (centre(x2) * gains[2]).astype(bf)

    final_rows = flat(run(6, "final", gather_seq(final_own, S))[0])
    final_rows, final_own = lax.optimization_barrier((final_rows, final_own))
    pieces = jnp.concatenate([shift(final_own, "head", k) for k in range(1, H)])
    logits = contract_dims(final_rows, embedding, 1, 1)
    peak = jnp.max(logits, axis=-1)
    exp_total = jnp.sum(jnp.exp(logits - peak[:, None]), axis=-1)
    stats = run(7, "stats", gather_seq(jnp.stack([peak, exp_total]).reshape(-1, 128), S))[0].reshape(S, 2, S * own)
    peak_all = jnp.max(stats[:, 0], axis=0)
    total_all = jnp.sum(stats[:, 1] * jnp.exp(stats[:, 0] - peak_all), axis=0)
    log_total = peak_all + jnp.log(total_all)

    def logits_grad(logits, log_total, head):
        scale = of_quarter(row_weights, head) / count_live
        local_target = of_quarter(targets, head) - vocab_start
        hit = jnp.arange(vocab_part)[None, :] == local_target[:, None]
        grads = jnp.exp(logits - log_total[:, None]) - hit.astype(f32)
        return (grads * scale[:, None]).astype(bf), hit, scale

    grad_logits, hit, scale_row = logits_grad(logits, log_total, h)
    target_logit = jnp.sum(jnp.where(hit, logits, 0.0), axis=-1)
    loss_lanes = scale_row * (log_total * (s == 0).astype(f32) - target_logit)
    loss_lanes = jnp.sum(loss_lanes.reshape(-1, 128), axis=0)[None]
    grad_rows = matmul(grad_logits, embedding).astype(bf)
    grad_rows, pieces = lax.optimization_barrier((grad_rows, pieces))
    grad_final = run(8, "logits_back", sum_seq(grad_rows.reshape(S, own, width), S))[0]
    grad_x2, grad_gain_final = norm_back(x2, gains[2], grad_final)

    pieces, grad_final = lax.optimization_barrier((pieces, grad_final))
    pieces = jnp.stack([pieces] + [shift(pieces, "seq", 2 * k) for k in range(1, S // 2)])
    chips = 2 * jnp.arange(S // 2)
    from_seq = jnp.concatenate([lax.rem(s - chips + S, S), lax.rem(s + 1 - 2 * lax.rem(s, 2) - chips + S, S)])

    back = lax.rem(h - jnp.arange(H) + H, H)
    numbers = jnp.stack([targets.astype(f32), row_weights]).reshape(2, S, H, own).transpose(2, 0, 1, 3)
    numbers = jnp.take(numbers, back, axis=0)

    def of_pieces(numbers, logs):
        rows = numbers[:, 0].reshape(logs.shape).astype(jnp.int32)
        return logs, rows - vocab_start, numbers[:, 1].reshape(logs.shape) / count_live

    sent = grad_x2.astype(bf)
    sent, log_total, final_rows = lax.optimization_barrier((sent, log_total, final_rows))
    parts = [sent] + [shift(sent, "head", k) for k in range(1, H)]
    grad_table = table_grad(embedding, [final_rows], *of_pieces(numbers[:1], log_total[None]), h, H)
    parts, grad_table = lax.optimization_barrier((parts, grad_table))
    grad_branch = jnp.concatenate(parts)
    logs = jnp.stack([shift(log_total.reshape(-1, 128), "head", k) for k in range(1, H)]).reshape(H - 1, S, own)
    grad_hidden = contract_dims(grad_branch, contract, 1, 1)
    grad_contract = contract_dims(hidden, grad_branch, 0, 0)
    _, gelu_back = jax.vjp(gelu_gate, gate_up[:, :width_ff], gate_up[:, width_ff:])
    grad_gate_up = jnp.concatenate(gelu_back(grad_hidden), axis=1).astype(bf)
    grad_expand = contract_dims(normed_b, grad_gate_up, 0, 0)
    grad_normed_b = head_sum(contract_dims(grad_gate_up, expand, 1, 1))
    grad_normed_b, pieces = lax.optimization_barrier((grad_normed_b, pieces))
    other_pieces = lax.ppermute(pieces, "seq", [(i, i ^ 1) for i in range(S)])
    grad_x1, grad_gain_b = norm_back(x1, gains[1], grad_normed_b)
    grad_x1 = grad_x1 + grad_x2
    grad_attn = head_gather(grad_x1.astype(bf))
    grad_attn, other_pieces = lax.optimization_barrier((grad_attn, other_pieces))
    pieces = jnp.concatenate([pieces, other_pieces])
    pieces = pieces.reshape(S, H - 1, own, width).transpose(1, 0, 2, 3).reshape(H - 1, S * own, width)
    grad_gated = contract_dims(grad_attn, output, 1, 1)
    grad_output = contract_dims(gated, grad_attn, 0, 0)
    _, gate_back = jax.vjp(gate_norm, gate_pre, retained)
    grad_gate_pre, grad_ret = gate_back(grad_gated)
    grad_cross = (lead_decay * grad_ret).astype(bf)
    grad_ret = grad_ret.astype(bf)
    grad_state = contract_dims(query, grad_cross, 0, 0)
    grad_update = state_sum(run(12, "states_back", gather_seq(grad_state.astype(bf), S))[0], True)
    grad_weights = contract_dims(grad_ret, values, 1, 1)
    grad_scores = (grad_weights * within).astype(bf)
    grad_query = matmul(grad_scores, keys) + contract_dims(grad_cross, state, 1, 1)
    grad_keys = contract_dims(grad_scores, query, 0, 0)
    grad_values = contract_dims(weights_blk, grad_ret, 0, 0) + matmul(weighted, grad_update)
    grad_keys = grad_keys + contract_dims(values, grad_update, 1, 1) * tail_decay
    grad_q_pre = rotate_back(grad_query, cosines_q, sines_q).astype(bf)
    grad_k_pre = rotate_back(grad_keys * KD ** (-0.5), cosines, sines).astype(bf)
    grad_qg = contract_dims(
        picker, jnp.concatenate([grad_q_pre, grad_gate_pre.astype(bf)], axis=1), 0, 0
    ).astype(bf)
    grad_proj = jnp.concatenate(
        [grad_qg[:, :KD], grad_k_pre, grad_values.astype(bf), grad_qg[:, KD:]], axis=1
    )
    grad_normed = contract_dims(grad_proj, mixer, 1, 1)
    grad_mixer = contract_dims(normed, grad_proj, 0, 0)

    def own_columns(value):
        return lax.dynamic_slice_in_dim(value, h * quarter, quarter, 1)

    scaled = grad_normed * gains[0]
    row_sums = jnp.stack([jnp.sum(scaled, axis=1), jnp.sum(scaled * hat0, axis=1)]).reshape(-1, 128)
    numbers = jnp.take(jnp.concatenate([numbers[1:], logs[:, None]], axis=1), from_seq, axis=2)
    logs, aims, scales = of_pieces(numbers, numbers[:, 2].reshape(H - 1, S * own))
    sent = grad_normed.astype(bf)
    sent, row_sums, logs = lax.optimization_barrier((sent, row_sums, logs))
    column_parts, sum_parts = [own_columns(sent)], [row_sums]
    for k in range(1, H):
        part = lax.dynamic_slice_in_dim(sent, lax.rem(h + k, H) * quarter, quarter, 1)
        column_parts.append(shift(part, "head", k))
        sum_parts.append(shift(row_sums, "head", k))
    grad_table = table_grad(
        embedding, [pieces[k] for k in range(H - 1)], logs, aims, scales, h, H, grad_table
    )
    column_parts, sum_parts, grad_table = lax.optimization_barrier((column_parts, sum_parts, grad_table))
    columns = sum(part.astype(f32) for part in column_parts)
    row_sums = sum(sum_parts).reshape(2, span, 1) / width
    hat_cols = own_columns(hat0)
    gain_cols = lax.dynamic_slice_in_dim(gains[0], h * quarter, quarter, 0)
    grad_gain_a = jnp.sum(columns * hat_cols, axis=0)
    grad_in = row_scale(x0.astype(f32)) * (columns * gain_cols - row_sums[0] - hat_cols * row_sums[1])
    grad_in = grad_in + contract_dims(picker, own_columns(grad_attn), 0, 0)
    piece_rows = flat(run(14, "rows", gather_seq(grad_in.astype(bf), S))[0])
    local_id = token_ids - vocab_start
    one_hot = (jnp.arange(vocab_part)[:, None] == local_id[None, :]).astype(bf)
    grad_table = grad_table + matmul(one_hot, piece_rows)

    def scattered(value, dim):
        return lax.psum_scatter(value.astype(bf), "seq", scatter_dimension=dim, tiled=True).astype(f32)[None]

    grad_contract, _ = lax.optimization_barrier((scattered(grad_contract, 1), grad_update))
    grad_expand = scattered(grad_expand, 0)
    grad_output = scattered(grad_output, 1)
    grad_mixer = scattered(grad_mixer, 0)
    grad_gains = jnp.stack(
        [lax.dynamic_update_slice_in_dim(jnp.zeros((width,), f32), grad_gain_a, h * quarter, 0), grad_gain_b, grad_gain_final]
    )

    mixer_f = w_mixer.astype(f32)
    output_f = w_output.astype(f32)
    expand_f = w_expand.astype(f32)
    contract_f = w_contract.astype(f32)
    table_own = own_columns(embedding).astype(f32)
    parts = [
        lamb_parts(mixer_f, mom_mixer, var_mixer, grad_mixer),
        lamb_parts(output_f, mom_output, var_output, grad_output),
        lamb_parts(expand_f, mom_expand, var_expand, grad_expand),
        lamb_parts(contract_f, mom_contract, var_contract, grad_contract),
        lamb_parts(table_own, mom_embed, var_embed, grad_table),
    ]
    held = [mixer_f, output_f, expand_f, contract_f, table_own]
    def lanes(value):
        total = jnp.sum((value * value).reshape(-1, value.shape[-1]), axis=0)
        return jnp.pad(total, (0, -total.shape[0] % 128)).reshape(-1, 128).sum(axis=0)[None]

    sums = [lanes(w) for w in held] + [lanes(p[2]) for p in parts]
    loss, squares, trust, moment_gains, second_gains, new_gains = finish(
        sums + [loss_lanes], grad_gains.reshape(-1, 128), jnp.stack([gains, mom_gains_all, var_gains_all]).reshape(3, -1, 128), S, H, 15
    )
    new_w = [w - LEARN_RATE * trust[i, 0] * parts[i][2] for i, w in enumerate(held)]

    def own_gains(value):
        return lax.dynamic_slice_in_dim(value.reshape(3, width), s * (width // S), width // S, 1)

    return (
        loss[0, 0],
        squares[:, :2],
        parts[0][0],
        parts[0][1],
        new_w[0],
        parts[1][0],
        parts[1][1],
        new_w[1],
        parts[2][0],
        parts[2][1],
        new_w[2],
        parts[3][0],
        parts[3][1],
        new_w[3],
        own_gains(moment_gains),
        own_gains(second_gains),
        own_gains(new_gains),
        parts[4][0],
        parts[4][1],
        new_w[4],
    )


def solution(mesh):
    placed = (
        P(),
        P(),
        P(None, "head"),
        P(None, "seq", "head"),
        P(None, "head", "seq"),
        P(None, "seq", "head"),
        P(None, "head", "seq"),
        P(None, "seq"),
        P("seq", None),
        P(None, "seq", "head"),
        P(None, "seq", "head"),
        P(None, "head", "seq"),
        P(None, "head", "seq"),
        P(None, "seq", "head"),
        P(None, "seq", "head"),
        P(None, "head", "seq"),
        P(None, "head", "seq"),
        P(None, "seq"),
        P(None, "seq"),
        P("seq", "head"),
        P("seq", "head"),
    )
    return jax.shard_map(
        local,
        mesh=mesh,
        in_specs=placed,
        out_specs=(P(), P()) + placed[3:4] * 3 + placed[4:5] * 3 + placed[3:4] * 3 + placed[4:5] * 3 + placed[7:8] * 3 + placed[19:20] * 3,
        check_vma=False,
    )
```

```python
import jax
import jax.numpy as jnp
from jax import lax
from jax.experimental import pallas as pl
from jax.experimental.pallas import tpu as pltpu
from jax.sharding import PartitionSpec as P

MESH = pl.DeviceIdType.MESH
ANY = pl.BlockSpec(memory_space=pl.ANY)
WHOLE = pl.BlockSpec(memory_space=pltpu.VMEM)
DMA = pltpu.SemaphoreType.DMA


def push(src, dst, sends, recvs, at, target):
    copy = pltpu.make_async_remote_copy(
        src_ref=src,
        dst_ref=dst,
        send_sem=sends.at[at],
        recv_sem=recvs.at[at],
        device_id=target,
        device_id_type=MESH,
    )
    copy.start()
    return copy


def fetch(src, dst, sems, at):
    copy = pltpu.make_async_copy(src, dst, sems.at[at])
    copy.start()
    return copy


def by_rows(count, step, body):
    def one(i, carry):
        body(pl.ds(pl.multiple_of(i * step, step), step))
        return carry

    lax.fori_loop(0, count // step, one, 0)


def row_step(rows):
    return 32 if rows % 32 == 0 else 16


class Here:
    def __init__(self, S, H):
        self.S, self.H, self.N = S, H, S // 2
        self.s, self.h = lax.axis_index("seq"), lax.axis_index("head")
        self.parity = lax.rem(self.s, 2)

    def head(self, k):
        return lax.rem(self.h + k, self.H)

    def seq(self, k):
        return lax.rem(self.s + 2 * k, self.S)

    def heads(self):
        return [{"head": self.head(k)} for k in range(1, self.H)]

    def chips(self):
        return [{"seq": self.seq(k)} for k in range(1, self.N)]

    def other(self):
        return {"seq": self.s + 1 - 2 * self.parity}


class Task:
    def __init__(self, axis, operands, outs, scratch, run):
        self.axis, self.operands, self.outs, self.scratch, self.run = axis, operands, outs, scratch, run


def fused(cid, S, H, tasks, name):
    operands, outs, specs, scratch = [], [], [], []
    for task in tasks:
        operands += task.operands
        for shape, dtype, spec in task.outs:
            outs.append(jax.ShapeDtypeStruct(shape, dtype))
            specs.append(spec)
        scratch += task.scratch

    def body(*refs):
        here = Here(S, H)
        ins, rest = refs[: len(operands)], refs[len(operands) :]
        results, held = rest[: len(outs)], rest[len(outs) :]
        live = []
        for task in tasks:
            live.append(
                task.run(here, ins[: len(task.operands)], results[: len(task.outs)], held[: len(task.scratch)])
            )
            ins, results, held = ins[len(task.operands) :], results[len(task.outs) :], held[len(task.scratch) :]
        axes = {task.axis for task in tasks}
        targets = []
        if axes & {"head", "both"}:
            targets += here.heads()
        if axes & {"seq", "both"}:
            targets += here.chips() + [here.other()]
        barrier = pltpu.get_barrier_semaphore()
        for target in targets:
            pl.semaphore_signal(barrier, inc=1, device_id=target, device_id_type=MESH)
        for run in live:
            next(run)
        pl.semaphore_wait(barrier, len(targets))
        while live:
            live = [run for run in live if next(run, "end") != "end"]

    got = pl.pallas_call(
        body,
        out_shape=outs,
        in_specs=[ANY] * len(operands),
        out_specs=specs,
        scratch_shapes=scratch,
        compiler_params=pltpu.CompilerParams(
            collective_id=cid, has_side_effects=True, vmem_limit_bytes=56 * 2**20
        ),
        cost_estimate=pl.CostEstimate(flops=0, bytes_accessed=2**25, transcendentals=0),
        name=name,
    )(*operands)
    split = []
    for task in tasks:
        split.append(got[: len(task.outs)])
        got = got[len(task.outs) :]
    return split


def gather_head(x, H):
    def run(here, ins, outs, held):
        (src,), (dst,), (sends, recvs, own) = ins, outs, held
        mine = fetch(src, dst.at[here.h], own, 0)
        yield
        copies = [push(src, dst.at[here.h], sends, recvs, k, to) for k, to in enumerate(here.heads())]
        yield
        for copy in copies:
            copy.wait()
        mine.wait()

    return Task("head", [x], [((H,) + x.shape, x.dtype, ANY)], [DMA((H - 1,)), DMA((H - 1,)), DMA((1,))], run)


def sum_head(x, H, columns=False):
    R, C = (x.shape[0], x.shape[1] // H) if columns else x.shape[1:]

    def run(here, ins, outs, held):
        (src,), (dst,), (got, sends, recvs, own) = ins, outs, held

        def block(i):
            return src.at[:, pl.ds(pl.multiple_of(i * C, C), C)] if columns else src.at[i]

        mine = fetch(block(here.h), got.at[0], own, 0)
        yield
        copies = [
            push(block(here.head(k)), got.at[k], sends, recvs, k - 1, {"head": here.head(k)}) for k in range(1, H)
        ]
        yield
        mine.wait()
        for copy in copies:
            copy.wait()

        def add(rows):
            total = got[0, rows, :].astype(jnp.float32)
            for k in range(1, H):
                total = total + got[k, rows, :].astype(jnp.float32)
            dst[rows, :] = total

        by_rows(R, row_step(R), add)

    return Task(
        "head",
        [x],
        [((R, C), jnp.float32, WHOLE)],
        [pltpu.VMEM((H, R, C), x.dtype), DMA((H - 1,)), DMA((H - 1,)), DMA((1,))],
        run,
    )


def gather_seq(x, S, columns=False, ahead=None):
    N = S // 2
    R, C = x.shape[-2:]

    def run(here, ins, outs, held):
        (src,), (dst,), (sends, recvs, fsends, frecvs, own) = ins, outs, held
        if ahead is not None:
            src = src.at[here.head(ahead)]

        def block(i):
            return dst.at[:, pl.ds(pl.multiple_of(i * C, C), C)] if columns else dst.at[i]

        mine = fetch(src, block(here.s), own, 0)
        yield
        copies = [push(src, block(here.s), sends, recvs, k, to) for k, to in enumerate(here.chips() + [here.other()])]
        passed = []
        for k in range(1, N):
            yield
            copies[k - 1].wait_recv()
            source = lax.rem(here.s - 2 * k + 2 * S, S)
            passed.append(push(block(source), block(source), fsends, frecvs, k - 1, here.other()))
        yield
        copies[N - 1].wait_recv()
        for copy in copies:
            copy.wait_send()
        for copy in passed:
            copy.wait()
        mine.wait()

    shape = (R, S * C) if columns else (S, R, C)
    return Task(
        "seq", [x], [(shape, x.dtype, ANY)], [DMA((N,)), DMA((N,)), DMA((N - 1,)), DMA((N - 1,)), DMA((1,))], run
    )


def sum_seq(x, S, columns=False):
    N = S // 2
    R, C = (x.shape[0], x.shape[1] // S) if columns else x.shape[1:]
    order = list(range(1, N)) + [0]

    def run(here, ins, outs, held):
        (src,), (dst,) = ins, outs
        theirs, ours, out, got, sends, recvs, csends, crecvs, own = held

        def block(i):
            return src.at[:, pl.ds(pl.multiple_of(i * C, C), C)] if columns else src.at[i]

        mine = {k: fetch(block(here.seq(k)), ours.at[k], own, k) for k in order}
        yield
        swaps = {
            k: push(block(here.seq(k) + 1 - 2 * here.parity), theirs.at[k], csends, crecvs, k, here.other())
            for k in order
        }
        copies = []
        for k in order:
            yield
            mine[k].wait()
            swaps[k].wait_recv()

            def add(rows, k=k):
                total = ours[k, rows, :].astype(jnp.float32) + theirs[k, rows, :].astype(jnp.float32)
                if k == 0:
                    dst[rows, :] = total
                else:
                    out[k - 1, rows, :] = total.astype(x.dtype)

            by_rows(R, row_step(R), add)
            if k > 0:
                copies.append(push(out.at[k - 1], got.at[k - 1], sends, recvs, k - 1, {"seq": here.seq(k)}))
        yield
        for copy in copies:
            copy.wait()
        for k in order:
            swaps[k].wait_send()

        def total(rows):
            value = dst[rows, :]
            for k in range(N - 1):
                value = value + got[k, rows, :].astype(jnp.float32)
            dst[rows, :] = value

        by_rows(R, row_step(R), total)

    blocks = lambda count: pltpu.VMEM((count, R, C), x.dtype)
    return Task(
        "seq",
        [x],
        [((R, C), jnp.float32, WHOLE)],
        [blocks(N), blocks(N), blocks(N - 1), blocks(N - 1)]
        + [DMA((N - 1,)), DMA((N - 1,)), DMA((N,)), DMA((N,)), DMA((N,))],
        run,
    )


def scatter_seq(x, base, ids, S):
    N = S // 2
    R, C = x.shape
    V = base.shape[0]
    tile = tile_of(V, 400)
    ids = ids.reshape(S, 1, R)

    def run(here, ins, outs, held):
        (src, base_ref, id_ref), (dst,) = ins, outs
        got, places, sends, recvs, fsends, frecvs, own = held
        mine = fetch(src, got.at[here.s], own, 0)
        start = fetch(base_ref, dst, own, 1)
        ids_in = fetch(id_ref, places, own, 2)

        def add(source):
            place = places[source]
            rows = got[source]

            def one(i, carry):
                at = pl.ds(pl.multiple_of(i * tile, tile), tile)
                hit = lax.broadcasted_iota(jnp.int32, (tile, R), 0) + i * tile == place
                hit = jnp.where(hit, 1.0, 0.0).astype(jnp.bfloat16)
                dst[at, :] += jnp.dot(hit, rows, preferred_element_type=jnp.float32)
                return carry

            lax.fori_loop(0, V // tile, one, 0, unroll=1 if V // tile % 5 else 5)

        yield
        copies = [push(src, got.at[here.s], sends, recvs, k, to) for k, to in enumerate(here.chips() + [here.other()])]
        yield
        for copy in (mine, start, ids_in):
            copy.wait()
        add(here.s)
        passed = []
        for k in range(1, N):
            copies[k - 1].wait_recv()
            source = lax.rem(here.s - 2 * k + 2 * S, S)
            passed.append(push(got.at[source], got.at[source], fsends, frecvs, k - 1, here.other()))
            add(source)
        across = here.s + 1 - 2 * here.parity
        copies[N - 1].wait_recv()
        add(across)
        for k in range(1, N):
            passed[k - 1].wait_recv()
            add(lax.rem(across - 2 * k + 2 * S, S))
        yield
        for copy in copies + passed:
            copy.wait_send()

    return Task(
        "seq",
        [x, base, ids],
        [((V, C), jnp.float32, WHOLE)],
        [pltpu.VMEM((S, R, C), x.dtype), pltpu.VMEM((S, 1, R), jnp.int32)]
        + [DMA((N,)), DMA((N,)), DMA((N - 1,)), DMA((N - 1,)), DMA((3,))],
        run,
    )


def finish(vectors, grad_gains, state, S, H, cid):
    count = len(vectors)
    groups = (count - 1) // 2
    gain_rows = grad_gains.shape[0] // 3
    first_gain = 16
    rows = first_gain + 3 * gain_rows
    mine = gain_rows == S

    def body(*refs):
        ins, grads_ref, state_ref = refs[:count], refs[count], refs[count + 1]
        loss_ref, square_ref, trust_ref, m_ref, v_ref, w_ref = refs[count + 2 : count + 8]
        packed, first, middle, second, fresh, sends, recvs, zsends, zrecvs = refs[count + 8 :]
        s, h = lax.axis_index("seq"), lax.axis_index("head")
        peers = [{"seq": lax.rem(s + k, S)} for k in range(1, S)]
        heads = [{"head": lax.rem(h + k, H)} for k in range(1, H)]
        packed[pl.ds(0, first_gain), :] = jnp.zeros((first_gain, 128), jnp.float32)
        for i in range(count):
            packed[pl.ds(i, 1), :] = ins[i][...]
        packed[pl.ds(first_gain, 3 * gain_rows), :] = grads_ref[...]
        barrier = pltpu.get_barrier_semaphore()
        for target in peers + heads:
            pl.semaphore_signal(barrier, inc=1, device_id=target, device_id_type=MESH)
        first[s] = packed[...]
        pl.semaphore_wait(barrier, S + H - 2)
        copies = [push(packed, first.at[s], sends, recvs, k, peers[k]) for k in range(S - 1)]
        for copy in copies:
            copy.wait()
        total = first[0]
        for k in range(1, S):
            total = total + first[k]
        middle[...] = total
        second[h] = total
        copies = [push(middle, second.at[h], zsends, zrecvs, k, heads[k]) for k in range(H - 1)]
        for copy in copies:
            copy.wait()
        total = second[0]
        for k in range(1, H):
            total = total + second[k]
        middle[...] = total

        def group_sum(value):
            return jnp.sum(jnp.sum(value, axis=1, keepdims=True), axis=0, keepdims=True)

        lane = lax.broadcasted_iota(jnp.int32, (1, 128), 1)
        weights = [group_sum(middle[pl.ds(i, 1), :]) for i in range(groups)]
        ratios = [group_sum(middle[pl.ds(groups + i, 1), :]) for i in range(groups)]
        loss_ref[...] = jnp.broadcast_to(group_sum(middle[pl.ds(2 * groups, 1), :]), (1, 128))
        parts = []
        for g in range(3):
            at = pl.ds(g * gain_rows, gain_rows)
            weight = state_ref[0, at, :]
            grad = middle[pl.ds(first_gain + g * gain_rows, gain_rows), :]
            part = lamb_parts(weight, state_ref[1, at, :], state_ref[2, at, :], grad)
            weights.append(group_sum(weight * weight))
            ratios.append(group_sum(part[2] * part[2]))
            parts.append((at, weight, part))
        for i in range(groups + 3):
            trust = jnp.sqrt(weights[i]) * lax.rsqrt(ratios[i] + TRUST_EPSILON)
            square_ref[pl.ds(i, 1), :] = jnp.where(lane == 0, weights[i], ratios[i])
            trust_ref[pl.ds(i, 1), :] = jnp.broadcast_to(trust, (1, 128))
            if i >= groups:
                at, weight, part = parts[i - groups]
                results = (part[0], part[1], weight - LEARN_RATE * trust * part[2])
                for result, ref in zip(results, (m_ref, v_ref, w_ref), strict=True):
                    if mine:
                        fresh[...] = result
                        ref[pl.ds(i - groups, 1), :] = fresh[pl.ds(s, 1), :]
                    else:
                        ref[at, :] = result

    shapes = [(1, 128), (groups + 3, 128), (groups + 3, 128)] + [(3 if mine else 3 * gain_rows, 128)] * 3
    return pl.pallas_call(
        body,
        out_shape=[jax.ShapeDtypeStruct(shape, jnp.float32) for shape in shapes],
        in_specs=[WHOLE] * (count + 2),
        out_specs=[WHOLE] * len(shapes),
        scratch_shapes=[
            pltpu.VMEM((rows, 128), jnp.float32),
            pltpu.VMEM((S, rows, 128), jnp.float32),
            pltpu.VMEM((rows, 128), jnp.float32),
            pltpu.VMEM((H, rows, 128), jnp.float32),
            pltpu.VMEM((gain_rows, 128), jnp.float32),
            DMA((S - 1,)),
            DMA((S - 1,)),
            DMA((H - 1,)),
            DMA((H - 1,)),
        ],
        compiler_params=pltpu.CompilerParams(collective_id=cid, has_side_effects=True),
        name="finish",
    )(*vectors, grad_gains, state)


def tile_of(count, most):
    fits = [d for d in range(16, most + 1, 16) if count % d == 0]
    return max(fits) if fits else count


def table_grad(embedding, finals, logs, targets, scales, head, H, base=None, most=400, slots=768):
    V, D = embedding.shape
    pieces = len(finals)
    R = finals[0].shape[0]
    Q = D // H
    tile = tile_of(V, most)
    count = R // slots

    def body(head_ref, e_ref, *refs):
        rows, columns = refs[:pieces], refs[pieces : 2 * pieces]
        log_ref, target_ref, scale_ref = refs[2 * pieces : 2 * pieces + 3]
        o_ref = refs[-1]
        table = e_ref[...]
        first = pl.program_id(0) * tile
        ids = first + lax.broadcasted_iota(jnp.int32, (tile, slots), 0)
        o_ref[...] = jnp.zeros((tile, Q), jnp.float32) if base is None else refs[-2][...]
        for k in range(pieces):

            def chunk(i, carry, k=k):
                at = pl.ds(pl.multiple_of(i * slots, slots), slots)
                logits = lax.dot_general(
                    table, rows[k][at, :], (((1,), (1,)), ((), ())), preferred_element_type=jnp.float32
                )
                place = k * count + i
                grads = jnp.exp(logits - log_ref[place]) - (ids == target_ref[place]).astype(jnp.float32)
                grads = (grads * scale_ref[place]).astype(jnp.bfloat16)
                o_ref[...] += jnp.dot(grads, columns[k][at, :], preferred_element_type=jnp.float32)
                return carry

            lax.fori_loop(0, count, chunk, 0)

    fixed = pl.Buffered(1)
    whole = lambda shape: pl.BlockSpec(shape, lambda t, head_ref: (0,) * len(shape), pipeline_mode=fixed)
    shaped = lambda value: value.reshape(pieces * count, 1, slots)
    extra = [] if base is None else [base]
    return pl.pallas_call(
        body,
        out_shape=jax.ShapeDtypeStruct((V, Q), jnp.float32),
        grid_spec=pltpu.PrefetchScalarGridSpec(
            num_scalar_prefetch=1,
            grid=(V // tile,),
            in_specs=[pl.BlockSpec((tile, D), lambda t, head_ref: (t, 0))]
            + [whole((R, D))] * pieces
            + [pl.BlockSpec((R, Q), lambda t, head_ref: (0, head_ref[0]), pipeline_mode=fixed)] * pieces
            + [whole((pieces * count, 1, slots))] * 3
            + [pl.BlockSpec((tile, Q), lambda t, head_ref: (t, 0))] * len(extra),
            out_specs=pl.BlockSpec((tile, Q), lambda t, head_ref: (t, 0)),
        ),
        compiler_params=pltpu.CompilerParams(vmem_limit_bytes=56 * 2**20),
        cost_estimate=pl.CostEstimate(
            flops=2 * V * pieces * R * (D + Q), bytes_accessed=V * D * 2 + V * Q * 4 + pieces * R * D * 2, transcendentals=V * pieces * R
        ),
        name="table_grad",
    )(head.reshape(1), embedding, *finals, *finals, shaped(logs), shaped(targets), shaped(scales), *extra)


KD = 256
VD = 512
STEP = 10

NORM_EPS = 1e-05
BETA_ONE = 0.9
BETA_TWO = 0.999
ADAM_EPS = 1e-08
DECAY_WT = 0.01
LEARN_RATE = 0.2
TRUST_EPSILON = 1e-06


def contract_dims(left_side, right_side, left_dim, right_dim):
    return lax.dot_general(
        left_side,
        right_side,
        (((left_dim,), (right_dim,)), ((), ())),
        preferred_element_type=jnp.float32,
    )


def matmul(left_side, right_side):
    return jnp.dot(left_side, right_side, preferred_element_type=jnp.float32)


def centre(values):
    centred = values - jnp.mean(values, axis=-1, keepdims=True)
    return centred * lax.rsqrt(jnp.mean(centred * centred, axis=-1, keepdims=True) + NORM_EPS)


def row_scale(values):
    centred = values - jnp.mean(values, axis=-1, keepdims=True)
    return lax.rsqrt(jnp.mean(centred * centred, axis=-1, keepdims=True) + NORM_EPS)


def norm_back(values, gain_row, grad):
    hat, scale = centre(values), row_scale(values)
    scaled = grad * gain_row
    mean_one = jnp.mean(scaled, axis=-1, keepdims=True)
    mean_two = jnp.mean(scaled * hat, axis=-1, keepdims=True)
    return scale * (scaled - mean_one - hat * mean_two), jnp.sum(grad * hat, axis=0)


def rotary_tables(positions):
    halfway = KD // 2
    frequency = jnp.exp(-jnp.log(10000.0) * jnp.arange(halfway).astype(jnp.float32) / halfway)
    phases = positions.astype(jnp.float32)[:, None] * frequency[None, :]
    return (jnp.cos(phases), jnp.sin(phases))


def rotate(values, cosines, sines):
    halfway = values.shape[-1] // 2
    leading = values[..., :halfway]
    trailing = values[..., halfway:]
    return jnp.concatenate(
        [leading * cosines - trailing * sines, leading * sines + trailing * cosines], axis=-1
    )


def rotate_back(grads, cosines, sines):
    return rotate(grads, cosines, -sines)


def gate_norm(gate_pre, retained):
    scaled = retained * lax.rsqrt(jnp.mean(retained * retained, axis=-1, keepdims=True) + NORM_EPS)
    return gate_pre * jax.nn.sigmoid(gate_pre) * scaled


def gelu_gate(gate_part, up_part):
    return jax.nn.gelu(gate_part) * up_part


def lamb_parts(weight, moment, second, grad):
    new_moment = BETA_ONE * moment + (1.0 - BETA_ONE) * grad
    new_second = BETA_TWO * second + (1.0 - BETA_TWO) * grad * grad
    moment_hat = new_moment / (1.0 - BETA_ONE**STEP)
    second_hat = new_second / (1.0 - BETA_TWO**STEP)
    ratio = moment_hat / (jnp.sqrt(second_hat) + ADAM_EPS) + DECAY_WT * weight
    return (new_moment, new_second, ratio)


def shift(value, axis, by):
    count = lax.axis_size(axis)
    return lax.ppermute(value, axis, [(i, (i + by) % count) for i in range(count)])


def head_gather(value):
    return jnp.concatenate([value] + [shift(value, "head", k) for k in range(1, lax.axis_size("head"))])


def head_sum(value):
    count = lax.axis_size("head")
    rows = value.shape[0] // count
    total = value[:rows].astype(jnp.float32)
    for k in range(1, count):
        at = (count - k) * rows
        total = total + shift(value[at : at + rows].astype(jnp.bfloat16), "head", k).astype(jnp.float32)
    return total


def local(
    token_ids,
    completion,
    decay_rate,
    w_mixer,
    w_output,
    w_expand,
    w_contract,
    norm_gains,
    embedding,
    mom_mixer,
    var_mixer,
    mom_output,
    var_output,
    mom_expand,
    var_expand,
    mom_contract,
    var_contract,
    mom_gains,
    var_gains,
    mom_embed,
    var_embed,
):
    bf, f32 = jnp.bfloat16, jnp.float32
    s, h = lax.axis_index("seq"), lax.axis_index("head")
    S, H = lax.axis_size("seq"), lax.axis_size("head")
    total_tokens = token_ids.shape[0]
    span = total_tokens // S
    vocab_part, width = embedding.shape
    quarter = width // H
    cap = span // 2
    own = cap // H
    rows_own = span // H
    assert w_mixer.shape[0] == 1
    token_start = s * span
    vocab_start = s * vocab_part

    def run(cid, name, *tasks):
        return [results[0] for results in fused(cid, S, H, tasks, name)]

    def flat(blocks):
        return blocks.reshape((-1,) + blocks.shape[2:])

    mixer = lax.all_gather(w_mixer[0], "seq", axis=0, tiled=True)
    output = lax.all_gather(w_output[0], "seq", axis=1, tiled=True)
    expand = lax.all_gather(w_expand[0], "seq", axis=0, tiled=True)
    contract = lax.all_gather(w_contract[0], "seq", axis=1, tiled=True)
    small = jnp.concatenate([norm_gains.astype(f32), mom_gains, var_gains], axis=0)
    small = jnp.concatenate([small, jnp.zeros((16 - small.shape[0], small.shape[1]), f32)], axis=0)

    ids_grid = token_ids.reshape(S, H, rows_own)
    ids_own = lax.dynamic_index_in_dim(ids_grid, h, 1, keepdims=False)
    chosen = ids_own.reshape(-1) - vocab_start
    inside = (chosen >= 0) & (chosen < vocab_part)
    found = jnp.take(embedding, jnp.clip(chosen, 0, vocab_part - 1), axis=0)
    found = jnp.where(inside[:, None], found, jnp.zeros((), bf))
    rows, small_all = run(
        1,
        "enter",
        sum_seq(found.reshape(S, rows_own, width), S),
        gather_seq(small, S),
    )
    rows = rows.astype(bf)
    x0 = jnp.zeros((span, width), bf)
    for k in range(H):
        at = lax.rem(h - k + H, H) * rows_own
        x0 = lax.dynamic_update_slice_in_dim(x0, shift(rows, "head", k) if k else rows, at, 0)
    small_all = small_all.transpose(1, 0, 2).reshape(16, width)
    gains, mom_gains_all, var_gains_all = small_all[:3], small_all[3:6], small_all[6:9]

    mask_own = lax.dynamic_slice_in_dim(completion, token_start, span)
    slot_of = jnp.where(mask_own == 1, jnp.cumsum(mask_own) - 1, -1)
    in_turn = jnp.arange(cap)
    in_turn = lax.rem(h - in_turn // own + H, H) * own + lax.rem(in_turn, own)
    at_slot = slot_of[None, :] == in_turn[:, None]
    picker = at_slot.astype(bf)
    place = jnp.sum(jnp.where(at_slot, jnp.arange(span)[None, :], 0), axis=1)
    mask_grid = completion.reshape(S, span)
    next_ids = jnp.roll(token_ids, -1).reshape(S, span)
    live = (completion * (jnp.arange(total_tokens) < total_tokens - 1)).reshape(S, span)
    slot_grid = jnp.where(mask_grid == 1, jnp.cumsum(mask_grid, axis=1) - 1, -1)
    matches = slot_grid[:, None, :] == jnp.arange(cap)[None, :, None]
    targets = jnp.sum(jnp.where(matches, next_ids[:, None, :], 0), axis=-1)
    row_weights = jnp.sum(jnp.where(matches, live[:, None, :], 0), axis=-1).astype(f32)
    count_live = jnp.sum(live).astype(f32)

    def of_quarter(grid, head):
        return lax.dynamic_index_in_dim(grid.reshape(S, H, own), head, 1, keepdims=False).reshape(-1)

    rate = decay_rate[0, 0]
    steps_in = jnp.arange(span).astype(f32)
    offsets = place[:, None].astype(f32) - steps_in[None, :]
    within = jnp.where(offsets >= 0, jnp.exp(-rate * jnp.maximum(offsets, 0.0)), 0.0)
    tail_decay = jnp.exp(-rate * (span - 1.0 - steps_in))[:, None]
    lead_decay = jnp.exp(-rate * (place.astype(f32) + 1.0))[:, None]
    cosines, sines = rotary_tables(token_start + jnp.arange(span))
    cosines_q, sines_q = rotary_tables(token_start + place)

    def state_sum(everyone, backward):
        position = jnp.arange(S)
        gap = position - s - 1 if backward else s - 1 - position
        factor = jnp.where(gap >= 0, jnp.exp(-rate * span * jnp.maximum(gap, 0).astype(f32)), 0.0)
        return jnp.sum(everyone.astype(f32) * factor[:, None, None], axis=0).astype(bf)

    hat0 = centre(x0.astype(f32))
    normed = (hat0 * gains[0]).astype(bf)
    proj_kv = matmul(normed, mixer[:, KD : 2 * KD + VD])
    keys = (rotate(proj_kv[:, :KD], cosines, sines) * KD ** (-0.5)).astype(bf)
    values = proj_kv[:, KD:].astype(bf)
    weighted = (keys.astype(f32) * tail_decay).astype(bf)
    update = contract_dims(weighted, values, 0, 0)
    state = state_sum(run(2, "states", gather_seq(update.astype(bf), S))[0], False)
    normed_q = matmul(picker, normed).astype(bf)
    query = rotate(matmul(normed_q, mixer[:, :KD]), cosines_q, sines_q).astype(bf)
    gate_pre = matmul(normed_q, mixer[:, 2 * KD + VD :])
    scores = contract_dims(query, keys, 1, 1)
    weights_blk = (scores * within).astype(bf)
    inner_part = matmul(weights_blk, values)
    retained = inner_part + lead_decay * matmul(query, state)
    gated = gate_norm(gate_pre, retained).astype(bf)

    x1 = matmul(picker[:own], x0) + head_sum(matmul(gated, output))
    normed_b_own = (centre(x1) * gains[1]).astype(bf)
    normed_b = head_gather(normed_b_own)
    gate_up = matmul(normed_b, expand)
    width_ff = gate_up.shape[1] // 2
    hidden = gelu_gate(gate_up[:, :width_ff], gate_up[:, width_ff:]).astype(bf)
    x2 = x1 + head_sum(matmul(hidden, contract))
    final_own = (centre(x2) * gains[2]).astype(bf)

    final_rows = flat(run(6, "final", gather_seq(final_own, S))[0])
    final_rows, final_own = lax.optimization_barrier((final_rows, final_own))
    pieces = jnp.concatenate([shift(final_own, "head", k) for k in range(1, H)])
    logits = contract_dims(final_rows, embedding, 1, 1)
    peak = jnp.max(logits, axis=-1)
    exp_total = jnp.sum(jnp.exp(logits - peak[:, None]), axis=-1)
    stats = run(7, "stats", gather_seq(jnp.stack([peak, exp_total]).reshape(-1, 128), S))[0].reshape(S, 2, S * own)
    peak_all = jnp.max(stats[:, 0], axis=0)
    total_all = jnp.sum(stats[:, 1] * jnp.exp(stats[:, 0] - peak_all), axis=0)
    log_total = peak_all + jnp.log(total_all)

    def logits_grad(logits, log_total, head):
        scale = of_quarter(row_weights, head) / count_live
        local_target = of_quarter(targets, head) - vocab_start
        hit = jnp.arange(vocab_part)[None, :] == local_target[:, None]
        grads = jnp.exp(logits - log_total[:, None]) - hit.astype(f32)
        return (grads * scale[:, None]).astype(bf), hit, scale

    grad_logits, hit, scale_row = logits_grad(logits, log_total, h)
    target_logit = jnp.sum(jnp.where(hit, logits, 0.0), axis=-1)
    loss_lanes = scale_row * (log_total * (s == 0).astype(f32) - target_logit)
    loss_lanes = jnp.sum(loss_lanes.reshape(-1, 128), axis=0)[None]
    grad_rows = matmul(grad_logits, embedding).astype(bf)
    grad_rows, pieces = lax.optimization_barrier((grad_rows, pieces))
    grad_final = run(8, "logits_back", sum_seq(grad_rows.reshape(S, own, width), S))[0]
    grad_x2, grad_gain_final = norm_back(x2, gains[2], grad_final)

    pieces, grad_final = lax.optimization_barrier((pieces, grad_final))
    pieces = jnp.stack([pieces] + [shift(pieces, "seq", 2 * k) for k in range(1, S // 2)])
    chips = 2 * jnp.arange(S // 2)
    from_seq = jnp.concatenate([lax.rem(s - chips + S, S), lax.rem(s + 1 - 2 * lax.rem(s, 2) - chips + S, S)])

    back = lax.rem(h - jnp.arange(H) + H, H)
    numbers = jnp.stack([targets.astype(f32), row_weights]).reshape(2, S, H, own).transpose(2, 0, 1, 3)
    numbers = jnp.take(numbers, back, axis=0)

    def of_pieces(numbers, logs):
        rows = numbers[:, 0].reshape(logs.shape).astype(jnp.int32)
        return logs, rows - vocab_start, numbers[:, 1].reshape(logs.shape) / count_live

    sent = grad_x2.astype(bf)
    sent, log_total, final_rows = lax.optimization_barrier((sent, log_total, final_rows))
    parts = [sent] + [shift(sent, "head", k) for k in range(1, H)]
    grad_table = table_grad(embedding, [final_rows], *of_pieces(numbers[:1], log_total[None]), h, H)
    parts, grad_table = lax.optimization_barrier((parts, grad_table))
    grad_branch = jnp.concatenate(parts)
    logs = jnp.stack([shift(log_total.reshape(-1, 128), "head", k) for k in range(1, H)]).reshape(H - 1, S, own)
    grad_hidden = contract_dims(grad_branch, contract, 1, 1)
    grad_contract = contract_dims(hidden, grad_branch, 0, 0)
    _, gelu_back = jax.vjp(gelu_gate, gate_up[:, :width_ff], gate_up[:, width_ff:])
    grad_gate_up = jnp.concatenate(gelu_back(grad_hidden), axis=1).astype(bf)
    grad_expand = contract_dims(normed_b, grad_gate_up, 0, 0)
    grad_normed_b = head_sum(contract_dims(grad_gate_up, expand, 1, 1))
    grad_normed_b, pieces = lax.optimization_barrier((grad_normed_b, pieces))
    other_pieces = lax.ppermute(pieces, "seq", [(i, i ^ 1) for i in range(S)])
    grad_x1, grad_gain_b = norm_back(x1, gains[1], grad_normed_b)
    grad_x1 = grad_x1 + grad_x2
    grad_attn = head_gather(grad_x1.astype(bf))
    grad_attn, other_pieces = lax.optimization_barrier((grad_attn, other_pieces))
    pieces = jnp.concatenate([pieces, other_pieces])
    pieces = pieces.reshape(S, H - 1, own, width).transpose(1, 0, 2, 3).reshape(H - 1, S * own, width)
    grad_gated = contract_dims(grad_attn, output, 1, 1)
    grad_output = contract_dims(gated, grad_attn, 0, 0)
    _, gate_back = jax.vjp(gate_norm, gate_pre, retained)
    grad_gate_pre, grad_ret = gate_back(grad_gated)
    grad_cross = (lead_decay * grad_ret).astype(bf)
    grad_ret = grad_ret.astype(bf)
    grad_state = contract_dims(query, grad_cross, 0, 0)
    grad_update = state_sum(run(12, "states_back", gather_seq(grad_state.astype(bf), S))[0], True)
    grad_weights = contract_dims(grad_ret, values, 1, 1)
    grad_scores = (grad_weights * within).astype(bf)
    grad_query = matmul(grad_scores, keys) + contract_dims(grad_cross, state, 1, 1)
    grad_keys = contract_dims(grad_scores, query, 0, 0)
    grad_values = contract_dims(weights_blk, grad_ret, 0, 0) + matmul(weighted, grad_update)
    grad_keys = grad_keys + contract_dims(values, grad_update, 1, 1) * tail_decay
    grad_q_pre = rotate_back(grad_query, cosines_q, sines_q).astype(bf)
    grad_k_pre = rotate_back(grad_keys * KD ** (-0.5), cosines, sines).astype(bf)
    grad_qg = contract_dims(
        picker, jnp.concatenate([grad_q_pre, grad_gate_pre.astype(bf)], axis=1), 0, 0
    ).astype(bf)
    grad_proj = jnp.concatenate(
        [grad_qg[:, :KD], grad_k_pre, grad_values.astype(bf), grad_qg[:, KD:]], axis=1
    )
    grad_normed = contract_dims(grad_proj, mixer, 1, 1)
    grad_mixer = contract_dims(normed, grad_proj, 0, 0)

    def own_columns(value):
        return lax.dynamic_slice_in_dim(value, h * quarter, quarter, 1)

    scaled = grad_normed * gains[0]
    row_sums = jnp.stack([jnp.sum(scaled, axis=1), jnp.sum(scaled * hat0, axis=1)]).reshape(-1, 128)
    numbers = jnp.take(jnp.concatenate([numbers[1:], logs[:, None]], axis=1), from_seq, axis=2)
    logs, aims, scales = of_pieces(numbers, numbers[:, 2].reshape(H - 1, S * own))
    sent = grad_normed.astype(bf)
    sent, row_sums, logs = lax.optimization_barrier((sent, row_sums, logs))
    column_parts, sum_parts = [own_columns(sent)], [row_sums]
    for k in range(1, H):
        part = lax.dynamic_slice_in_dim(sent, lax.rem(h + k, H) * quarter, quarter, 1)
        column_parts.append(shift(part, "head", k))
        sum_parts.append(shift(row_sums, "head", k))
    grad_table = table_grad(
        embedding, [pieces[k] for k in range(H - 1)], logs, aims, scales, h, H, grad_table
    )
    column_parts, sum_parts, grad_table = lax.optimization_barrier((column_parts, sum_parts, grad_table))
    columns = sum(part.astype(f32) for part in column_parts)
    row_sums = sum(sum_parts).reshape(2, span, 1) / width
    hat_cols = own_columns(hat0)
    gain_cols = lax.dynamic_slice_in_dim(gains[0], h * quarter, quarter, 0)
    grad_gain_a = jnp.sum(columns * hat_cols, axis=0)
    grad_in = row_scale(x0.astype(f32)) * (columns * gain_cols - row_sums[0] - hat_cols * row_sums[1])
    grad_in = grad_in + contract_dims(picker, own_columns(grad_attn), 0, 0)
    ids = (token_ids - vocab_start).reshape(S, span)
    grad_table = run(14, "rows", scatter_seq(grad_in.astype(bf), grad_table, ids, S))[0]
    def scattered(value, dim):
        return lax.psum_scatter(value.astype(bf), "seq", scatter_dimension=dim, tiled=True).astype(f32)[None]

    grad_contract, _ = lax.optimization_barrier((scattered(grad_contract, 1), grad_update))
    grad_expand = scattered(grad_expand, 0)
    grad_output = scattered(grad_output, 1)
    grad_mixer = scattered(grad_mixer, 0)
    grad_gains = jnp.stack(
        [lax.dynamic_update_slice_in_dim(jnp.zeros((width,), f32), grad_gain_a, h * quarter, 0), grad_gain_b, grad_gain_final]
    )

    mixer_f = w_mixer.astype(f32)
    output_f = w_output.astype(f32)
    expand_f = w_expand.astype(f32)
    contract_f = w_contract.astype(f32)
    table_own = own_columns(embedding).astype(f32)
    parts = [
        lamb_parts(mixer_f, mom_mixer, var_mixer, grad_mixer),
        lamb_parts(output_f, mom_output, var_output, grad_output),
        lamb_parts(expand_f, mom_expand, var_expand, grad_expand),
        lamb_parts(contract_f, mom_contract, var_contract, grad_contract),
        lamb_parts(table_own, mom_embed, var_embed, grad_table),
    ]
    held = [mixer_f, output_f, expand_f, contract_f, table_own]
    def lanes(value):
        total = jnp.sum((value * value).reshape(-1, value.shape[-1]), axis=0)
        return jnp.pad(total, (0, -total.shape[0] % 128)).reshape(-1, 128).sum(axis=0)[None]

    sums = [lanes(w) for w in held] + [lanes(p[2]) for p in parts]
    loss, squares, trust, moment_gains, second_gains, new_gains = finish(
        sums + [loss_lanes], grad_gains.reshape(-1, 128), jnp.stack([gains, mom_gains_all, var_gains_all]).reshape(3, -1, 128), S, H, 15
    )
    new_w = [w - LEARN_RATE * trust[i, 0] * parts[i][2] for i, w in enumerate(held)]

    def own_gains(value):
        if value.shape[0] == 3:
            return value
        return lax.dynamic_slice_in_dim(value.reshape(3, width), s * (width // S), width // S, 1)

    return (
        loss[0, 0],
        squares[:, :2],
        parts[0][0],
        parts[0][1],
        new_w[0],
        parts[1][0],
        parts[1][1],
        new_w[1],
        parts[2][0],
        parts[2][1],
        new_w[2],
        parts[3][0],
        parts[3][1],
        new_w[3],
        own_gains(moment_gains),
        own_gains(second_gains),
        own_gains(new_gains),
        parts[4][0],
        parts[4][1],
        new_w[4],
    )


def solution(mesh):
    placed = (
        P(),
        P(),
        P(None, "head"),
        P(None, "seq", "head"),
        P(None, "head", "seq"),
        P(None, "seq", "head"),
        P(None, "head", "seq"),
        P(None, "seq"),
        P("seq", None),
        P(None, "seq", "head"),
        P(None, "seq", "head"),
        P(None, "head", "seq"),
        P(None, "head", "seq"),
        P(None, "seq", "head"),
        P(None, "seq", "head"),
        P(None, "head", "seq"),
        P(None, "head", "seq"),
        P(None, "seq"),
        P(None, "seq"),
        P("seq", "head"),
        P("seq", "head"),
    )
    return jax.shard_map(
        local,
        mesh=mesh,
        in_specs=placed,
        out_specs=(P(), P()) + placed[3:4] * 3 + placed[4:5] * 3 + placed[3:4] * 3 + placed[4:5] * 3 + placed[7:8] * 3 + placed[19:20] * 3,
        check_vma=False,
    )
```
